128 devices in a mesh: leaf: 128 (over z, x, y, core).
Axes of the slice: x: 4, y: 4, z: 4, core: 2. Of those that a mesh axis runs over, the one named last changes fastest.
Arguments:
- coords: float32 [3, 1048576], P(None, 'leaf'), may hold values from 0 to 1
- charges: bfloat16 [1048576, 128], P('leaf'), may hold values from -6 to 6
- near_leaves: int32 [8192, 27], P('leaf'), may hold values from 0 to 191
- leaf_basis: bfloat16 [8192, 4096], P('leaf'), may hold values from -1 to 1
- leaf_transfer: bfloat16 [8192, 1024], P('leaf'), may hold values from -0.75 to 0.75
- mid_transfer: bfloat16 [1024, 1024], P('leaf'), may hold values from -0.75 to 0.75
- base_transfer: bfloat16 [128, 1024], P('leaf'), may hold values from -0.75 to 0.75
- base_coupling: bfloat16 [24192, 1024], P('leaf'), may hold values from -0.01953125 to 0.01953125
- base_target: int32 [24192, 1], P('leaf'), may hold values from 0 to 127; in each aligned block of 189 rows (0 to 188, 189 to 377, ...) at most 2 rows name the same one
- base_source: int32 [24192], P('leaf'), may hold values from 0 to 127
- top_coupling: bfloat16 [1024, 1024], P('leaf'), may hold values from -0.015625 to 0.015625
- top_target: int32 [1024], P('leaf'), may hold values from 0 to 15
- top_source: int32 [1024], P('leaf'), may hold values from 0 to 15
Outputs:
- potential: bfloat16 [1048576, 128], P('leaf')
The draws below stay inside these ranges and needn't reach their ends.
Inputs may be any that keep to these rules, and one draw needn't show every extreme that they name: `near_leaves`: entry j of leaf l names leaf 64 * (l // 64 - 1) + j: a leaf of the device before in Morton order, of the row's own device, or of the device after; repeats may occur. `base_target`: among the 189 blocks of one device no base cluster is the target more than 2 times; that count is reached.
All inputs are finite; a program needn't handle non-finite values.
Results may differ from the reference program's by a relative error of at most 0.01.
Values may be sent and summed in bfloat16 or wider, within the bound.
A program may use at most 128 MiB of HBM per device.

```python
import math
import jax
import jax.numpy as jnp
import numpy as np
from jax import lax

K = 32
RHS = 128
M = 128
NNEAR = 27
NB = 189
TOPB_DEV = 8
LEAF_DEV = 64
BASE_DEV = 1
LEAVES = 8192
NPTS = 1048576
MIDS = 1024
NBASE = 128
NTOP = 16
BLK_DEV = 189
NBLK = 24192
NTBLK = 1024
CAPC = 2
N_LEAF = 128


def set_ends(drawn, stream_key, smallest, top_value):
    shape = drawn.shape
    spot = [jax.random.randint(jax.random.fold_in(stream_key, axis), (), 0, shape[axis]) for axis in range(len(shape))]
    drawn = drawn.at[tuple(spot)].set(smallest)
    longest = shape.index(max(shape))
    spot[longest] = (spot[longest] + 1) % shape[longest]
    return drawn.at[tuple(spot)].set(top_value)


def shard_levels(rng, dims, pieces, smallest, high):
    loudness, own = 1.0, jax.random.fold_in(rng, 6)
    for position, blocks in pieces:
        draws = jnp.exp(jax.random.uniform(jax.random.fold_in(own, position), (blocks,), jnp.float32, smallest / len(pieces), high / len(pieces)))
        loudness = loudness * jnp.repeat(draws, dims[position] // blocks).reshape([-1 if axis == position else 1 for axis in range(len(dims))])
    return loudness


def shared_out(rng, own, number, rows, amount, top, bound, slope):
    ranking = jax.random.permutation(rng, amount)
    heavy_load, ordinary = shares(amount, rows * top, bound, slope, True), shares(amount, rows * top, bound, slope, False)
    places = jnp.arange(amount)

    def named(lengths, offset_by):
        used = int((lengths > 0).sum())
        fixed = max(1, used // 4)
        passed = fixed + (places - fixed + offset_by * (used - fixed)) % max(1, amount - fixed)
        return jnp.zeros((amount,), jnp.int32).at[ranking[jnp.where(places < fixed, places, passed)]].set(jnp.asarray(lengths, jnp.int32))

    lengths = jnp.where(number % 4 == 0, named(heavy_load, number // 4), named(ordinary, number - number // 4 - 1))
    mixed = jax.random.permutation(jax.random.fold_in(own, 3), amount)
    source_of, taker = mixed[0:amount // 2 * 2:2], mixed[1:amount // 2 * 2:2]
    margin = jnp.minimum(lengths[source_of] - 1, bound - lengths[taker]) // 2
    margin = jnp.where((source_of == ranking[0]) | (taker == ranking[0]) | (lengths[taker] == 0), 0, jnp.maximum(margin, 0))
    passed = jax.random.randint(jax.random.fold_in(own, 4), (amount // 2,), 0, 1 << 20) % (margin + 1)
    lengths = lengths.at[source_of].add(-passed).at[taker].add(passed)
    labels = jnp.searchsorted(jnp.cumsum(lengths), jnp.arange(rows * top), side="right").astype(jnp.int32)
    listing = labels.reshape(top, rows).T
    listing = listing[jax.random.permutation(jax.random.fold_in(own, 1), rows)]
    offset_by = jax.random.randint(jax.random.fold_in(own, 2), (rows, 1), 0, top)
    return jnp.take_along_axis(listing, (jnp.arange(top)[None, :] + offset_by) % top, axis=1)


def shares(count, total, bound, lean, full):
    weights = [(1 << 20) // math.isqrt(grade ** lean) + 1 for grade in range(1, count + 1)]
    largest = bound if full else min(bound, max(-(-total // count), total * weights[0] // sum(weights)))
    least = 1 if total - largest >= count - 1 else 0
    counts, spare = [largest] + [least] * (count - 1), total - largest - least * (count - 1)
    while spare > 0:
        movable = [i for i in range(1, count) if counts[i] < largest] or [i for i in range(1, count) if counts[i] < bound]
        whole, remaining = sum([weights[i] for i in movable]), spare
        for i in movable:
            more = min(bound - counts[i], max(1, remaining * weights[i] // whole), spare)
            counts[i] = counts[i] + more
            spare = spare - more
    return np.array(counts)


def centred(key, dims, spread, bound, pieces=(), kind=jnp.bfloat16):
    result = spread * jax.random.normal(key, dims, jnp.float32)
    if pieces:
        result = result * shard_levels(key, dims, pieces, -0.22, 0.18)
    return jnp.clip(result, -bound, bound).astype(kind)


def setup_inputs(seed: int = 0) -> dict:
    arg_keys = jax.random.split(jax.random.key(seed), 14)
    coords = jnp.clip(1.0 * jax.random.uniform(arg_keys[0], (3, NPTS), jnp.float32) ** shard_levels(arg_keys[0], (3, NPTS), ((1, 128),), -0.2, 0.2), 0.0, 1.0)
    charges = centred(arg_keys[1], (NPTS, RHS), 1.0, 6.0, ((0, 128),))
    near_leaves = set_ends(jax.random.randint(arg_keys[2], (LEAVES, NNEAR), 0, 3 * LEAF_DEV), jax.random.fold_in(arg_keys[2], 1), 0, (3 * LEAF_DEV) - 1).astype(jnp.int32)
    leaf_basis = centred(arg_keys[3], (LEAVES, K * M), K ** -0.5, 1.0, ((0, 128),))
    leaf_transfer = centred(arg_keys[4], (LEAVES, K * K), (2 * K) ** -0.5, 0.75, ((0, 128),))
    mid_transfer = centred(arg_keys[5], (MIDS, K * K), (2 * K) ** -0.5, 0.75, ((0, 128),))
    base_transfer = centred(arg_keys[6], (NBASE, K * K), (2 * K) ** -0.5, 0.75, ((0, 128),))
    base_coupling = centred(arg_keys[7], (NBLK, K * K), (16 * K * NB) ** -0.5, 0.01953125, ((0, 128),))
    base_target_keys = jax.random.split(jax.random.fold_in(arg_keys[8], 1), NBLK // BLK_DEV)
    base_target_turns = jax.random.permutation(jax.random.fold_in(arg_keys[8], 3), NBLK // BLK_DEV)
    base_target = jax.vmap(lambda own, number: shared_out(jax.random.fold_in(arg_keys[8], 2), own, number, BLK_DEV, NBASE, 1, CAPC, 1))(base_target_keys, base_target_turns).reshape((NBLK, 1))
    base_source = set_ends(jax.random.randint(arg_keys[9], (NBLK,), 0, NBASE), jax.random.fold_in(arg_keys[9], 1), 0, NBASE - 1).astype(jnp.int32)
    top_coupling = centred(arg_keys[10], (NTBLK, K * K), (512 * K * TOPB_DEV // BASE_DEV) ** -0.5, 0.015625, ((0, 128),))
    top_target = set_ends(jax.random.randint(arg_keys[11], (NTBLK,), 0, NTOP), jax.random.fold_in(arg_keys[11], 1), 0, NTOP - 1).astype(jnp.int32)
    top_source = set_ends(jax.random.randint(arg_keys[12], (NTBLK,), 0, NTOP), jax.random.fold_in(arg_keys[12], 1), 0, NTOP - 1).astype(jnp.int32)
    return {"coords": coords, "charges": charges, "near_leaves": near_leaves, "leaf_basis": leaf_basis, "leaf_transfer": leaf_transfer, "mid_transfer": mid_transfer, "base_transfer": base_transfer, "base_coupling": base_coupling, "base_target": base_target, "base_source": base_source, "top_coupling": top_coupling, "top_target": top_target, "top_source": top_source}


delta_sq = 0.0025

def rounded_values(values):
    return lax.optimization_barrier(values.astype(jnp.bfloat16))

def near_block(points, pool_points, pool_charges, columns):
    near_scale = 1.0 / math.sqrt(columns.shape[1] * points.shape[2])

    def near_step(running, column):
        other_points = jnp.take(pool_points, column, axis=1)
        other_charges = jnp.take(pool_charges, column, axis=0)
        squares = lax.optimization_barrier(jnp.sum((points[:, :, :, None] - other_points[:, :, None, :]) ** 2, axis=0))
        kernel = rounded_values(near_scale / jnp.sqrt(squares + delta_sq))
        update = jnp.einsum('lab,lbr->lar', kernel.astype(jnp.float32), other_charges.astype(jnp.float32))
        return (running + update, None)
    initial = jnp.zeros((points.shape[1], points.shape[2], pool_charges.shape[2]), jnp.float32)
    running, unused = lax.scan(near_step, initial, columns.T)
    return running

def reference(coords, charges, near_leaves, leaf_basis, leaf_transfer, mid_transfer, base_transfer, base_coupling, base_target, base_source, top_coupling, top_target, top_source):
    single_precision = jnp.float32
    charge_row_block = charges.reshape(LEAVES, M, RHS)
    basis_matrix = leaf_basis.reshape(LEAVES, K, M)
    leaf_coefficients = rounded_values(jnp.einsum('xpt,xtu->xpu', basis_matrix.astype(single_precision), charge_row_block.astype(single_precision)))
    mid_coeffs = rounded_values(jnp.einsum('mckp,mckr->mpr', leaf_transfer.reshape(MIDS, 8, K, K).astype(single_precision), leaf_coefficients.reshape(MIDS, 8, K, RHS).astype(single_precision)))
    base_coeffs = rounded_values(jnp.einsum('mckp,mckr->mpr', mid_transfer.reshape(NBASE, 8, K, K).astype(single_precision), mid_coeffs.reshape(NBASE, 8, K, RHS).astype(single_precision)))
    base_lift = base_transfer.reshape(NBASE, K, K)
    lifted = rounded_values(jnp.einsum('bkp,bkr->bpr', base_lift.astype(single_precision), base_coeffs.astype(single_precision)))
    top_coeffs = rounded_values(lax.optimization_barrier(jnp.sum(lifted.reshape(NTOP, 8, K, RHS).astype(single_precision), axis=1)))

    def add_portion(running, portion):
        blocks, targets, sources = portion
        products = jnp.einsum('bts,bsr->btr', blocks.reshape(-1, K, K).astype(single_precision), jnp.take(base_coeffs, sources, axis=0).astype(single_precision))
        return (running + jax.ops.segment_sum(products, targets, num_segments=NBASE), None)
    portions = (base_coupling.reshape(N_LEAF, BLK_DEV, K * K), base_target.reshape(N_LEAF, BLK_DEV), base_source.reshape(N_LEAF, BLK_DEV))
    coupled, unused = lax.scan(add_portion, jnp.zeros((NBASE, K, RHS), single_precision), portions)
    top_products = jnp.einsum('bts,bsr->btr', top_coupling.reshape(NTBLK, K, K).astype(single_precision), jnp.take(top_coeffs, top_source, axis=0).astype(single_precision))
    top_field = rounded_values(jax.ops.segment_sum(top_products, top_target, num_segments=NTOP))
    base_field = rounded_values(coupled + jnp.einsum('bkp,bpr->bkr', base_lift.astype(single_precision), jnp.repeat(top_field, 8, axis=0).astype(single_precision)))
    mid_field = rounded_values(jnp.einsum('mkp,mpr->mkr', mid_transfer.reshape(MIDS, K, K).astype(single_precision), jnp.repeat(base_field, 8, axis=0).astype(single_precision)))
    leaf_potential = rounded_values(jnp.einsum('lkp,lpr->lkr', leaf_transfer.reshape(LEAVES, K, K).astype(single_precision), jnp.repeat(mid_field, 8, axis=0).astype(single_precision)))
    all_points = coords.reshape(3, LEAVES, M)
    padded_points = jnp.pad(all_points, ((0, 0), (LEAF_DEV, LEAF_DEV), (0, 0)))
    padded_charges = jnp.pad(charge_row_block, ((LEAF_DEV, LEAF_DEV), (0, 0), (0, 0)))
    device_ids = jnp.arange(N_LEAF, dtype=jnp.int32)

    def device_block(portion):
        device, columns, local_expansion_basis, local_potential = portion
        first = (device * LEAF_DEV).astype(jnp.int32)
        points = lax.dynamic_slice_in_dim(all_points, first, LEAF_DEV, 1)
        pool_points = lax.dynamic_slice_in_dim(padded_points, first, 3 * LEAF_DEV, 1)
        pool_charges = lax.dynamic_slice_in_dim(padded_charges, first, 3 * LEAF_DEV, 0)
        near_field = near_block(points, pool_points, pool_charges, columns)
        distant_field = jnp.einsum('cbz,cbw->czw', local_expansion_basis.astype(single_precision), local_potential.astype(single_precision))
        return (near_field + distant_field).astype(jnp.bfloat16)
    inputs = (device_ids, near_leaves.reshape(N_LEAF, LEAF_DEV, NNEAR), basis_matrix.reshape(N_LEAF, LEAF_DEV, K, M), leaf_potential.reshape(N_LEAF, LEAF_DEV, K, RHS))
    potential = lax.map(device_block, inputs)
    return potential.reshape(NPTS, RHS)
```

```python
import functools
import math

import jax
import jax.numpy as jnp
from jax import lax
from jax.experimental import pallas as pl
from jax.experimental.pallas import tpu as pltpu
from jax.sharding import PartitionSpec as P

K = 32
RHS = 128
M = 128
N = 128
LEAVES = 64
POOL = 3 * LEAVES
NNEAR = 27
PAIRS = (NNEAR + 1) // 2
GROUP = 8
DELTA_SQ = 0.0025
AXIS = "leaf"
MESH = pl.DeviceIdType.MESH
bf16 = jnp.bfloat16
f32 = jnp.float32


def dot(a, b):
    return jnp.dot(a, b, preferred_element_type=f32)


def dot_t(a, b):
    return lax.dot_general(a, b, (((0,), (0,)), ((), ())), preferred_element_type=f32)


def vmem(*shape):
    return pl.BlockSpec(shape, lambda *_: (0,) * len(shape))


def split3(v):
    high = v.astype(bf16).astype(f32)
    rest = v - high
    mid = rest.astype(bf16).astype(f32)
    return high, mid, rest - mid


def features(scale, points, target):
    centred = [(p - 0.5) * scale for p in points]
    norm = centred[0] * centred[0] + centred[1] * centred[1] + centred[2] * centred[2]
    one = jnp.ones_like(norm)
    rows = []
    for c in centred:
        h, m, l = split3(c)
        if target:
            h, m, l = -2.0 * h, -2.0 * m, -2.0 * l
            rows += [h, h, m, m, h, l]
        else:
            rows += [h, m, h, m, l, h]
    if target:
        rows += [*split3(norm + scale * scale * DELTA_SQ), one, one, one]
    else:
        rows += [one, one, one, *split3(norm)]
    return rows + [jnp.zeros_like(norm)] * (K - len(rows))


def feature_kernel(scale, points, source, target, lines):
    count = points.shape[1]
    for r, row in enumerate(features(scale, [points[i] for i in range(3)], False)):
        lines[pl.ds(r, count, stride=K), :] = row

    def put(l, c):
        source[l] = lines[pl.ds(pl.multiple_of(l * K, K), K), :].astype(bf16)
        return c

    lax.fori_loop(0, count, put, 0, unroll=4)
    own = [points[i, LEAVES : 2 * LEAVES] for i in range(3)]
    for r, row in enumerate(features(scale, own, True)):
        lines[pl.ds(r, LEAVES, stride=K), :] = row

    def turn(l, c):
        target[l] = lines[pl.ds(pl.multiple_of(l * K, K), K), :].T.astype(bf16)
        return c

    lax.fori_loop(0, LEAVES, turn, 0, unroll=4)


def feature_call(points):
    count = points.shape[1]
    return pl.pallas_call(
        functools.partial(feature_kernel, math.sqrt(NNEAR * M)),
        out_shape=(
            jax.ShapeDtypeStruct((count, K, M), bf16),
            jax.ShapeDtypeStruct((LEAVES, M, K), bf16),
        ),
        scratch_shapes=[pltpu.VMEM((count * K, M), f32)],
        cost_estimate=pl.CostEstimate(flops=10**8, bytes_accessed=10**6, transcendentals=0),
        name="features",
    )(points)


def upward_kernel(charges, basis, leaf_t, mid_t, base_t, out, mids):
    step = pl.program_id(0)
    parts = []
    for c in range(GROUP):
        parts.append(dot(basis[c], charges[c]).astype(bf16))
    rows = jnp.concatenate(parts, axis=0)
    mids[pl.ds(pl.multiple_of(step * K, K), K), :] = dot_t(leaf_t[...], rows).astype(bf16)

    @pl.when(step == GROUP - 1)
    def _():
        base = dot_t(mid_t[...], mids[...]).astype(bf16)
        out[0] = base
        out[1] = dot_t(base_t[...], base).astype(bf16)


def upward_call(charges, basis, leaf_t, mid_t, base_t):
    return pl.pallas_call(
        upward_kernel,
        grid=(GROUP,),
        in_specs=[
            pl.BlockSpec((GROUP, M, RHS), lambda i: (i, 0, 0)),
            pl.BlockSpec((GROUP, K, M), lambda i: (i, 0, 0)),
            pl.BlockSpec((GROUP * K, K), lambda i: (i, 0)),
            vmem(GROUP * K, K),
            vmem(K, K),
        ],
        out_specs=vmem(2, K, RHS),
        out_shape=jax.ShapeDtypeStruct((2, K, RHS), bf16),
        scratch_shapes=[pltpu.VMEM((GROUP * K, RHS), bf16)],
        cost_estimate=pl.CostEstimate(flops=10**8, bytes_accessed=3 * 10**6, transcendentals=0),
        name="upward",
    )(charges, basis, leaf_t, mid_t, base_t)


def blocks_kernel(blk, blk_src, top, top_idx, r_blk, r_src, r_top, r_idx, send, recv, local):
    me = lax.axis_index(AXIS)
    plane, place = me // GROUP, me % GROUP
    barrier = pltpu.get_barrier_semaphore()

    def hello(o, c):
        pl.semaphore_signal(
            barrier, inc=1, device_id=(lax.rem(me + o, N),), device_id_type=MESH
        )
        return c

    lax.fori_loop(1, N, hello, 0)
    pl.semaphore_wait(barrier, N - 1)

    def remote(src, dst, k, to):
        return pltpu.make_async_remote_copy(
            src_ref=src,
            dst_ref=dst,
            send_sem=send.at[k],
            recv_sem=recv.at[k],
            device_id=(to,),
            device_id_type=MESH,
        )

    def give(o, c):
        to = lax.rem(me + o, N)
        remote(blk.at[to], r_blk.at[me], 0, to).start()
        remote(blk_src.at[to], r_src.at[me], 1, to).start()
        return c

    lax.fori_loop(1, N, give, 0)

    def give_top(o, c):
        to = lax.rem(plane + o, 16) * GROUP + place
        remote(top, r_top.at[plane], 2, to).start()
        remote(top_idx, r_idx.at[plane], 3, to).start()
        return c

    lax.fori_loop(1, 16, give_top, 0)
    own = [
        pltpu.make_async_copy(blk.at[me], r_blk.at[me], local.at[0]),
        pltpu.make_async_copy(blk_src.at[me], r_src.at[me], local.at[1]),
        pltpu.make_async_copy(top, r_top.at[plane], local.at[2]),
        pltpu.make_async_copy(top_idx, r_idx.at[plane], local.at[3]),
    ]
    for copy in own:
        copy.start()
    for copy in own:
        copy.wait()
    for k, (ref, count) in enumerate(((r_blk, N), (r_src, N), (r_top, 16), (r_idx, 16))):
        part = ref.at[pl.ds(0, count - 1)]
        whole = remote(part, part, k, me)
        whole.wait_send()
        whole.wait_recv()


def blocks_call(blk, blk_src, top, top_idx):
    return pl.pallas_call(
        blocks_kernel,
        out_shape=(
            jax.ShapeDtypeStruct(blk.shape, blk.dtype),
            jax.ShapeDtypeStruct(blk_src.shape, blk_src.dtype),
            jax.ShapeDtypeStruct((16, *top.shape), top.dtype),
            jax.ShapeDtypeStruct((16, *top_idx.shape), top_idx.dtype),
        ),
        in_specs=[pl.BlockSpec(memory_space=pltpu.VMEM)] * 4,
        out_specs=(pl.BlockSpec(memory_space=pltpu.VMEM),) * 4,
        scratch_shapes=[
            pltpu.SemaphoreType.DMA((4,)),
            pltpu.SemaphoreType.DMA((4,)),
            pltpu.SemaphoreType.DMA((4,)),
        ],
        compiler_params=pltpu.CompilerParams(collective_id=0, has_side_effects=True),
        cost_estimate=pl.CostEstimate(flops=10**8, bytes_accessed=10**6, transcendentals=0),
        name="blocks",
    )(blk, blk_src, top, top_idx)


def field_kernel(
    coeffs, top_part, a_high, a_low, base_t, out, every, lifted, tops, mine, top_all, send, recv, local
):
    me = lax.axis_index(AXIS)
    plane, place = me // GROUP, me % GROUP
    core, y = place % 2, place // 2
    barrier = pltpu.get_barrier_semaphore()
    for o in range(1, GROUP):
        to = plane * GROUP + lax.rem(place + o, GROUP)
        pl.semaphore_signal(barrier, inc=1, device_id=(to,), device_id_type=MESH)
    for o in range(1, 16):
        to = lax.rem(plane + o, 16) * GROUP + place
        pl.semaphore_signal(barrier, inc=1, device_id=(to,), device_id_type=MESH)
    pl.semaphore_wait(barrier, GROUP + 14)

    def remote(src, dst, k, to):
        return pltpu.make_async_remote_copy(
            src_ref=src,
            dst_ref=dst,
            send_sem=send.at[k],
            recv_sem=recv.at[k],
            device_id=(to,),
            device_id_type=MESH,
        )

    def finish(part, k):
        whole = remote(part, part, k, me)
        whole.wait_send()
        whole.wait_recv()

    for o in range(1, 4):
        to = plane * GROUP + lax.rem(y + o, 4) * 2 + core
        remote(coeffs.at[0], every.at[core, plane, y], 0, to).start()
    for o in range(1, GROUP):
        to = plane * GROUP + lax.rem(place + o, GROUP)
        remote(coeffs.at[1], lifted.at[place], 1, to).start()
    for o in range(1, GROUP):
        to = plane * GROUP + lax.rem(place + o, GROUP)
        remote(top_part, tops.at[place], 2, to).start()
    own = [
        pltpu.make_async_copy(coeffs.at[0], every.at[core, plane, y], local.at[0]),
        pltpu.make_async_copy(coeffs.at[1], lifted.at[place], local.at[1]),
        pltpu.make_async_copy(top_part, tops.at[place], local.at[2]),
    ]
    for copy in own:
        copy.start()
    for copy in own:
        copy.wait()
    finish(lifted.at[pl.ds(0, 3)], 0)
    for o in range(1, 16):
        to = lax.rem(plane + o, 16) * GROUP + place
        remote(every.at[core, plane], every.at[core, plane], 3, to).start()
    finish(lifted.at[pl.ds(0, GROUP - 1)], 1)
    mine[...] = jnp.sum(lifted[...].astype(f32), axis=0).astype(bf16)
    for o in range(1, 16):
        to = lax.rem(plane + o, 16) * GROUP + place
        remote(mine, top_all.at[plane], 4, to).start()
    own_top = pltpu.make_async_copy(mine, top_all.at[plane], local.at[3])
    own_top.start()
    own_top.wait()
    finish(every.at[0, pl.ds(0, 15)], 3)
    partner = me + 1 - 2 * core
    across = remote(every.at[core], every.at[core], 5, partner)
    across.start()
    finish(tops.at[pl.ds(0, GROUP - 1)], 2)
    finish(top_all.at[pl.ds(0, 15)], 4)
    top = jnp.sum(tops[...].astype(f32), axis=0)
    top_high = top.astype(bf16)
    top_low = (top - top_high.astype(f32)).astype(bf16)
    coeff_tops = top_all[...].reshape(16 * K, RHS)
    top_field = (dot(top_high, coeff_tops) + dot(top_low, coeff_tops)).astype(bf16)
    total = dot(base_t[...], top_field)
    across.wait()
    rows = every[...].reshape(N * K, RHS)
    total = total + (dot(a_high[...], rows) + dot(a_low[...], rows))
    out[...] = total.astype(bf16)


def field_call(coeffs, top_part, a_high, a_low, base_t):
    return pl.pallas_call(
        field_kernel,
        out_shape=jax.ShapeDtypeStruct((K, RHS), bf16),
        in_specs=[pl.BlockSpec(memory_space=pltpu.VMEM)] * 5,
        out_specs=pl.BlockSpec(memory_space=pltpu.VMEM),
        scratch_shapes=[
            pltpu.VMEM((2, 16, 4, K, RHS), bf16),
            pltpu.VMEM((GROUP, K, RHS), bf16),
            pltpu.VMEM((GROUP, K, 16 * K), bf16),
            pltpu.VMEM((K, RHS), bf16),
            pltpu.VMEM((16, K, RHS), bf16),
            pltpu.SemaphoreType.DMA((6,)),
            pltpu.SemaphoreType.DMA((6,)),
            pltpu.SemaphoreType.DMA((4,)),
        ],
        compiler_params=pltpu.CompilerParams(collective_id=1, has_side_effects=True),
        cost_estimate=pl.CostEstimate(flops=10**8, bytes_accessed=10**6, transcendentals=0),
        name="field",
    )(coeffs, top_part, a_high, a_low, base_t)


def near_kernel(
    near, source, target, before, here, after, base, mid_t, leaf_t, basis, out, pool, kern, gathered, sems
):
    step = pl.program_id(0)

    @pl.when(step == 0)
    def _():
        copies = [
            pltpu.make_async_copy(ref, pool.at[pl.ds(LEAVES * i, LEAVES)], sems.at[i])
            for i, ref in enumerate((before, here, after))
        ]
        for copy in copies:
            copy.start()
        pool[POOL] = jnp.zeros((M, RHS), bf16)
        for copy in copies:
            copy.wait()

    mid = dot(mid_t[...], base[...]).astype(bf16)
    fields = dot(leaf_t[...], mid).astype(bf16)
    for b in range(GROUP):
        leaf = step * GROUP + b
        mine = target[b]
        for j in range(PAIRS):
            one = near[leaf * 2 * PAIRS + 2 * j]
            two = near[leaf * 2 * PAIRS + 2 * j + 1]
            others = jnp.concatenate([source[one], source[two]], axis=1)
            squares = dot(mine, others)
            kern[b, :, 2 * M * j : 2 * M * (j + 1)] = lax.rsqrt(squares.astype(bf16))
            gathered[b, 2 * M * j : 2 * M * j + M] = pool[one]
            gathered[b, 2 * M * j + M : 2 * M * (j + 1)] = pool[two]
        far = dot_t(basis[b], fields[b * K : (b + 1) * K])
        total = dot(kern[b], gathered[b]) + far
        out[pl.ds(b * M, M), :] = total.astype(bf16)


def near_call(near, source, target, before, here, after, base, mid_t, leaf_t, basis):
    count = source.shape[0]
    grid_spec = pltpu.PrefetchScalarGridSpec(
        num_scalar_prefetch=1,
        grid=(LEAVES // GROUP,),
        in_specs=[
            vmem(count, K, M),
            pl.BlockSpec((GROUP, M, K), lambda i, _: (i, 0, 0)),
            pl.BlockSpec(memory_space=pl.ANY),
            pl.BlockSpec(memory_space=pl.ANY),
            pl.BlockSpec(memory_space=pl.ANY),
            vmem(K, RHS),
            pl.BlockSpec((K, K), lambda i, _: (i, 0)),
            pl.BlockSpec((GROUP * K, K), lambda i, _: (i, 0)),
            pl.BlockSpec((GROUP, K, M), lambda i, _: (i, 0, 0)),
        ],
        out_specs=pl.BlockSpec((GROUP * M, RHS), lambda i, _: (i, 0)),
        scratch_shapes=[
            pltpu.VMEM((POOL + 1, M, RHS), bf16),
            pltpu.VMEM((GROUP, M, 2 * M * PAIRS), bf16),
            pltpu.VMEM((GROUP, 2 * M * PAIRS, RHS), bf16),
            pltpu.SemaphoreType.DMA((3,)),
        ],
    )
    return pl.pallas_call(
        near_kernel,
        grid_spec=grid_spec,
        out_shape=jax.ShapeDtypeStruct((LEAVES * M, RHS), bf16),
        compiler_params=pltpu.CompilerParams(
            vmem_limit_bytes=48 * 1024 * 1024, dimension_semantics=("arbitrary",)
        ),
        cost_estimate=pl.CostEstimate(
            flops=10**10, bytes_accessed=10**7, transcendentals=3 * 10**7
        ),
        name="near",
    )(near, source, target, before, here, after, base, mid_t, leaf_t, basis)


def high_low(v):
    high = v.astype(bf16)
    return high, (v - high.astype(f32)).astype(bf16)


def per_device(
    coords,
    charges,
    near_leaves,
    leaf_basis,
    leaf_transfer,
    mid_transfer,
    base_transfer,
    base_coupling,
    base_target,
    base_source,
    top_coupling,
    top_target,
    top_source,
):
    me = lax.axis_index(AXIS)
    up = [(i, i + 1) for i in range(N - 1)]
    down = [(i + 1, i) for i in range(N - 1)]
    rows = charges.reshape(LEAVES, M, RHS)
    before = lax.ppermute(rows, AXIS, up)
    after = lax.ppermute(rows, AXIS, down)
    points = coords.reshape(3, LEAVES, M)
    points = jnp.concatenate(
        [
            lax.ppermute(points, AXIS, up),
            points,
            lax.ppermute(points, AXIS, down),
            jnp.zeros((3, 8, M), f32),
        ],
        axis=1,
    )
    source, target = feature_call(points)

    targets = base_target[:, 0]
    count = targets.shape[0]
    earlier = jnp.arange(count)[:, None] > jnp.arange(count)[None, :]
    rank = jnp.sum((targets[:, None] == targets[None, :]) & earlier, axis=1)
    slots = jnp.arange(2 * N)
    chosen = (slots[:, None] == (2 * targets + rank)[None, :]).astype(bf16)
    blk = dot(chosen, base_coupling).astype(bf16).reshape(N, 16, 128)
    order = (base_source % 2) * 64 + (base_source // 8) * 4 + (base_source // 2) % 4
    slot_source = jnp.sum(chosen.astype(jnp.int32) * (order + 1)[None, :], axis=1) - 1
    blk_src = jnp.pad(slot_source.reshape(N, 1, 2), ((0, 0), (0, 0), (0, 126)))
    top_idx = jnp.pad(top_target * 16 + top_source, (0, 120)).reshape(1, 128)
    r_blk, r_src, r_top, r_idx = blocks_call(
        blk, blk_src, top_coupling.reshape(64, 128), top_idx
    )
    by_source = (jnp.arange(N)[:, None] == r_src[:, 0, :2].reshape(1, 2 * N)).astype(bf16)
    a = dot(by_source, r_blk.reshape(2 * N, K * K))
    a = a.reshape(N, K, K).transpose(1, 0, 2).reshape(K, N * K)
    a_high, a_low = high_low(a)
    wanted = (me // GROUP) * 16 + jnp.arange(16)
    by_top = (wanted[:, None] == r_idx[:, 0, :8].reshape(1, N)).astype(bf16)
    top_part = dot(by_top, r_top.reshape(N, K * K)).astype(bf16)
    top_part = top_part.reshape(16, K, K).transpose(1, 0, 2).reshape(K, 16 * K)

    basis = leaf_basis.reshape(LEAVES, K, M)
    leaf_t = leaf_transfer.reshape(LEAVES * K, K)
    mid_t = mid_transfer.reshape(GROUP * K, K)
    base_t = base_transfer.reshape(K, K)
    coeffs = upward_call(rows, basis, leaf_t, mid_t, base_t)
    base = field_call(coeffs, top_part, a_high, a_low, base_t)

    near = jnp.pad(near_leaves, ((0, 0), (0, 1)), constant_values=POOL).reshape(-1)
    return near_call(near, source, target, before, rows, after, base, mid_t, leaf_t, basis)


def solution(mesh):
    lead = P(AXIS, None)
    in_specs = (
        P(None, AXIS),
        lead,
        lead,
        lead,
        lead,
        lead,
        lead,
        lead,
        lead,
        P(AXIS),
        lead,
        P(AXIS),
        P(AXIS),
    )
    return jax.shard_map(
        per_device, mesh=mesh, in_specs=in_specs, out_specs=lead, check_vma=False
    )
```

```python
import functools
import math

import jax
import jax.numpy as jnp
from jax import lax
from jax.experimental import pallas as pl
from jax.experimental.pallas import tpu as pltpu
from jax.sharding import PartitionSpec as P

K = 32
RHS = 128
M = 128
N = 128
LEAVES = 64
POOL = 3 * LEAVES
NNEAR = 27
PAIRS = (NNEAR + 1) // 2
GROUP = 8
DELTA_SQ = 0.0025
AXIS = "leaf"
MESH = pl.DeviceIdType.MESH
bf16 = jnp.bfloat16
f32 = jnp.float32


def dot(a, b):
    return jnp.dot(a, b, preferred_element_type=f32)


def dot_t(a, b):
    return lax.dot_general(a, b, (((0,), (0,)), ((), ())), preferred_element_type=f32)


def vmem(*shape):
    return pl.BlockSpec(shape, lambda *_: (0,) * len(shape))


def split3(v):
    high = v.astype(bf16).astype(f32)
    rest = v - high
    mid = rest.astype(bf16).astype(f32)
    return high, mid, rest - mid


def features(scale, points, target):
    centred = [(p - 0.5) * scale for p in points]
    norm = centred[0] * centred[0] + centred[1] * centred[1] + centred[2] * centred[2]
    one = jnp.ones_like(norm)
    rows = []
    for c in centred:
        h, m, l = split3(c)
        if target:
            h, m, l = -2.0 * h, -2.0 * m, -2.0 * l
            rows += [h, h, m, m, h, l]
        else:
            rows += [h, m, h, m, l, h]
    if target:
        rows += [*split3(norm + scale * scale * DELTA_SQ), one, one, one]
    else:
        rows += [one, one, one, *split3(norm)]
    return rows + [jnp.zeros_like(norm)] * (K - len(rows))


def exchange_kernel(
    scale,
    blk,
    blk_src,
    top,
    top_idx,
    points,
    charges,
    basis,
    leaf_t,
    mid_t,
    base_t,
    r_blk,
    r_src,
    every,
    top_all,
    tops,
    source,
    target,
    held,
    r_top,
    r_idx,
    lifted,
    coeffs,
    mine,
    mids,
    part,
    others,
    lines,
    send,
    recv,
    local,
):
    me = lax.axis_index(AXIS)
    plane, place = me // GROUP, me % GROUP
    core, y = place % 2, place // 2
    fetch = pltpu.make_async_copy(charges, held, local.at[0])
    fetch.start()
    barrier = pltpu.get_barrier_semaphore()

    def hello(o, c):
        pl.semaphore_signal(
            barrier, inc=1, device_id=(lax.rem(me + o, N),), device_id_type=MESH
        )
        return c

    lax.fori_loop(1, N, hello, 0)
    pl.semaphore_wait(barrier, N - 1)

    def remote(src, dst, k, to):
        return pltpu.make_async_remote_copy(
            src_ref=src,
            dst_ref=dst,
            send_sem=send.at[k],
            recv_sem=recv.at[k],
            device_id=(to,),
            device_id_type=MESH,
        )

    def finish(ref, k):
        whole = remote(ref, ref, k, me)
        whole.wait_send()
        whole.wait_recv()

    right, left = lax.rem(me + 1, N), lax.rem(me + N - 1, N)
    to_right = remote(points, others.at[0], 0, right)
    to_left = remote(points, others.at[1], 1, left)
    to_right.start()
    to_left.start()

    def give_top(o, c):
        to = lax.rem(plane + o, 16) * GROUP + place
        remote(top, r_top.at[plane], 2, to).start()
        remote(top_idx, r_idx.at[plane], 3, to).start()
        return c

    lax.fori_loop(1, 16, give_top, 0)

    def give(o, c):
        to = lax.rem(me + o, N)
        remote(blk.at[to], r_blk.at[me], 4, to).start()
        remote(blk_src.at[to], r_src.at[me], 5, to).start()
        return c

    lax.fori_loop(1, N, give, 0)
    own = [
        pltpu.make_async_copy(blk.at[me], r_blk.at[me], local.at[1]),
        pltpu.make_async_copy(blk_src.at[me], r_src.at[me], local.at[2]),
        pltpu.make_async_copy(top, r_top.at[plane], local.at[3]),
        pltpu.make_async_copy(top_idx, r_idx.at[plane], local.at[4]),
    ]
    for copy in own:
        copy.start()

    fetch.wait()

    def one_mid(m, c):
        rows = []
        for b in range(GROUP):
            rows.append(dot(basis[m * GROUP + b], held[m * GROUP + b]).astype(bf16))
        first = pl.multiple_of(m * GROUP * K, GROUP * K)
        rows = dot_t(leaf_t[pl.ds(first, GROUP * K), :], jnp.concatenate(rows, axis=0))
        mids[pl.ds(pl.multiple_of(m * K, K), K), :] = rows.astype(bf16)
        return c

    lax.fori_loop(0, GROUP, one_mid, 0)
    base = dot_t(mid_t[...], mids[...]).astype(bf16)
    coeffs[0] = base
    coeffs[1] = dot_t(base_t[...], base).astype(bf16)
    for o in range(1, 4):
        to = plane * GROUP + lax.rem(y + o, 4) * 2 + core
        remote(coeffs.at[0], every.at[core, plane, y], 6, to).start()
    for o in range(1, GROUP):
        to = plane * GROUP + lax.rem(place + o, GROUP)
        remote(coeffs.at[1], lifted.at[place], 7, to).start()
    own += [
        pltpu.make_async_copy(coeffs.at[0], every.at[core, plane, y], local.at[5]),
        pltpu.make_async_copy(coeffs.at[1], lifted.at[place], local.at[6]),
    ]
    for copy in own[4:]:
        copy.start()

    def side(rows, put, count):
        for r, row in enumerate(rows):
            lines[pl.ds(r, LEAVES, stride=K), :] = row
        lax.fori_loop(0, count, put, 0, unroll=4)

    def line(l):
        return lines[pl.ds(pl.multiple_of(l * K, K), K), :]

    def put_target(l, c):
        target[l] = line(l).T.astype(bf16)
        return c

    def put_source(block):
        def put(l, c):
            source[block * LEAVES + l] = line(l).astype(bf16)
            return c

        return put

    here = [points[i] for i in range(3)]
    side(features(scale, here, True), put_target, LEAVES)
    for copy in own:
        copy.wait()
    finish(lifted.at[pl.ds(0, 3)], 6)
    for o in range(1, 16):
        to = lax.rem(plane + o, 16) * GROUP + place
        remote(every.at[core, plane], every.at[core, plane], 8, to).start()
    finish(lifted.at[pl.ds(0, GROUP - 1)], 7)
    mine[...] = jnp.sum(lifted[...].astype(f32), axis=0).astype(bf16)
    for o in range(1, 16):
        to = lax.rem(plane + o, 16) * GROUP + place
        remote(mine, top_all.at[plane], 9, to).start()
    own_top = pltpu.make_async_copy(mine, top_all.at[plane], local.at[0])
    own_top.start()
    side(features(scale, here, False), put_source(1), LEAVES)
    own_top.wait()

    finish(r_top.at[pl.ds(0, 15)], 2)
    finish(r_idx.at[pl.ds(0, 15)], 3)
    named = jnp.sum(r_idx[...], axis=0)
    wanted = plane * 16 + lax.broadcasted_iota(jnp.int32, (16, N), 0)
    chosen = jnp.where(wanted == named, 1.0, 0.0).astype(bf16)
    part[...] = dot(chosen, r_top[...].reshape(N, K * K)).astype(bf16)
    for o in range(1, GROUP):
        to = plane * GROUP + lax.rem(place + o, GROUP)
        remote(part, tops.at[place], 10, to).start()
    own_part = pltpu.make_async_copy(part, tops.at[place], local.at[0])
    own_part.start()
    to_right.wait()
    to_left.wait()
    spare = source[LEAVES]
    for l in range(8):
        source[POOL + l] = spare
    side(features(scale, [others[0, i] for i in range(3)], False), put_source(0), LEAVES)
    finish(every.at[0, pl.ds(0, 15)], 8)
    across = remote(every.at[core], every.at[core], 11, me + 1 - 2 * core)
    across.start()
    side(features(scale, [others[1, i] for i in range(3)], False), put_source(2), LEAVES)
    finish(top_all.at[pl.ds(0, 15)], 9)
    own_part.wait()
    finish(tops.at[pl.ds(0, GROUP - 1)], 10)
    across.wait()
    finish(r_blk.at[pl.ds(0, N - 1)], 4)
    finish(r_src.at[pl.ds(0, N - 1)], 5)


def exchange_call(blk, blk_src, top, top_idx, points, charges, basis, leaf_t, mid_t, base_t):
    inside = pl.BlockSpec(memory_space=pltpu.VMEM)
    shape = jax.ShapeDtypeStruct
    return pl.pallas_call(
        functools.partial(exchange_kernel, math.sqrt(NNEAR * M)),
        out_shape=(
            shape(blk.shape, bf16),
            shape(blk_src.shape, jnp.int32),
            shape((2, 16, 4, K, RHS), bf16),
            shape((16, K, RHS), bf16),
            shape((GROUP, 16, K * K), bf16),
            shape((POOL + 8, K, M), bf16),
            shape((LEAVES, M, K), bf16),
        ),
        in_specs=[inside] * 5 + [pl.BlockSpec(memory_space=pl.ANY)] + [inside] * 4,
        out_specs=(inside,) * 7,
        scratch_shapes=[
            pltpu.VMEM((LEAVES, M, RHS), bf16),
            pltpu.VMEM((16, 8, K * K), bf16),
            pltpu.VMEM((16, 1, N), jnp.int32),
            pltpu.VMEM((GROUP, K, RHS), bf16),
            pltpu.VMEM((2, K, RHS), bf16),
            pltpu.VMEM((K, RHS), bf16),
            pltpu.VMEM((GROUP * K, RHS), bf16),
            pltpu.VMEM((16, K * K), bf16),
            pltpu.VMEM((2, 3, LEAVES, M), f32),
            pltpu.VMEM((LEAVES * K, M), f32),
            pltpu.SemaphoreType.DMA((12,)),
            pltpu.SemaphoreType.DMA((12,)),
            pltpu.SemaphoreType.DMA((7,)),
        ],
        compiler_params=pltpu.CompilerParams(
            collective_id=0, has_side_effects=True, vmem_limit_bytes=40 * 1024 * 1024
        ),
        cost_estimate=pl.CostEstimate(flops=10**9, bytes_accessed=10**7, transcendentals=0),
        name="exchange",
    )(blk, blk_src, top, top_idx, points, charges, basis, leaf_t, mid_t, base_t)


def near_kernel(
    near,
    source,
    target,
    before,
    here,
    after,
    a_high,
    a_low,
    every,
    t_high,
    t_low,
    top_all,
    base_t,
    mid_t,
    leaf_t,
    basis,
    out,
    pool,
    kern,
    gathered,
    base,
    sems,
):
    step = pl.program_id(0)

    @pl.when(step == 0)
    def _():
        copies = [
            pltpu.make_async_copy(ref, pool.at[pl.ds(LEAVES * i, LEAVES)], sems.at[i])
            for i, ref in enumerate((before, here, after))
        ]
        for copy in copies:
            copy.start()
        pool[POOL] = jnp.zeros((M, RHS), bf16)
        top_field = (dot(t_high[...], top_all[...]) + dot(t_low[...], top_all[...])).astype(bf16)
        coupled = dot(a_high[...], every[...]) + dot(a_low[...], every[...])
        base[...] = (coupled + dot(base_t[...], top_field)).astype(bf16)
        for copy in copies:
            copy.wait()

    mid = dot(mid_t[...], base[...]).astype(bf16)
    fields = dot(leaf_t[...], mid).astype(bf16)
    for b in range(GROUP):
        leaf = step * GROUP + b
        mine = target[b]
        for j in range(PAIRS):
            one = near[leaf * 2 * PAIRS + 2 * j]
            two = near[leaf * 2 * PAIRS + 2 * j + 1]
            others = jnp.concatenate([source[one], source[two]], axis=1)
            squares = dot(mine, others)
            kern[b, :, 2 * M * j : 2 * M * (j + 1)] = lax.rsqrt(squares.astype(bf16))
            gathered[b, 2 * M * j : 2 * M * j + M] = pool[one]
            gathered[b, 2 * M * j + M : 2 * M * (j + 1)] = pool[two]
        far = dot_t(basis[b], fields[b * K : (b + 1) * K])
        total = dot(kern[b], gathered[b]) + far
        out[pl.ds(b * M, M), :] = total.astype(bf16)


def near_call(near, source, target, before, here, after, far, mid_t, leaf_t, basis):
    count = source.shape[0]
    grid_spec = pltpu.PrefetchScalarGridSpec(
        num_scalar_prefetch=1,
        grid=(LEAVES // GROUP,),
        in_specs=[
            vmem(count, K, M),
            pl.BlockSpec((GROUP, M, K), lambda i, _: (i, 0, 0)),
            pl.BlockSpec(memory_space=pl.ANY),
            pl.BlockSpec(memory_space=pl.ANY),
            pl.BlockSpec(memory_space=pl.ANY),
            *[vmem(*v.shape) for v in far],
            pl.BlockSpec((K, K), lambda i, _: (i, 0)),
            pl.BlockSpec((GROUP * K, K), lambda i, _: (i, 0)),
            pl.BlockSpec((GROUP, K, M), lambda i, _: (i, 0, 0)),
        ],
        out_specs=pl.BlockSpec((GROUP * M, RHS), lambda i, _: (i, 0)),
        scratch_shapes=[
            pltpu.VMEM((POOL + 1, M, RHS), bf16),
            pltpu.VMEM((GROUP, M, 2 * M * PAIRS), bf16),
            pltpu.VMEM((GROUP, 2 * M * PAIRS, RHS), bf16),
            pltpu.VMEM((K, RHS), bf16),
            pltpu.SemaphoreType.DMA((3,)),
        ],
    )
    return pl.pallas_call(
        near_kernel,
        grid_spec=grid_spec,
        out_shape=jax.ShapeDtypeStruct((LEAVES * M, RHS), bf16),
        compiler_params=pltpu.CompilerParams(
            vmem_limit_bytes=48 * 1024 * 1024, dimension_semantics=("arbitrary",)
        ),
        cost_estimate=pl.CostEstimate(
            flops=10**10, bytes_accessed=10**7, transcendentals=3 * 10**7
        ),
        name="near",
    )(near, source, target, before, here, after, *far, mid_t, leaf_t, basis)


def high_low(v):
    high = v.astype(bf16)
    return high, (v - high.astype(f32)).astype(bf16)


def per_device(
    coords,
    charges,
    near_leaves,
    leaf_basis,
    leaf_transfer,
    mid_transfer,
    base_transfer,
    base_coupling,
    base_target,
    base_source,
    top_coupling,
    top_target,
    top_source,
):
    me = lax.axis_index(AXIS)
    up = [(i, i + 1) for i in range(N - 1)]
    down = [(i + 1, i) for i in range(N - 1)]
    rows = charges.reshape(LEAVES, M, RHS)
    before = lax.ppermute(rows, AXIS, up)
    after = lax.ppermute(rows, AXIS, down)
    points = coords.reshape(3, LEAVES, M)

    targets = base_target[:, 0]
    count = targets.shape[0]
    earlier = jnp.arange(count)[:, None] > jnp.arange(count)[None, :]
    rank = jnp.sum((targets[:, None] == targets[None, :]) & earlier, axis=1)
    slots = jnp.arange(2 * N)
    chosen = (slots[:, None] == (2 * targets + rank)[None, :]).astype(bf16)
    blk = dot(chosen, base_coupling).astype(bf16).reshape(N, 16, 128)
    order = (base_source % 2) * 64 + (base_source // 8) * 4 + (base_source // 2) % 4
    slot_source = jnp.sum(chosen.astype(jnp.int32) * (order + 1)[None, :], axis=1) - 1
    blk_src = jnp.pad(slot_source.reshape(N, 1, 2), ((0, 0), (0, 0), (0, 126)))
    lane = jnp.arange(N)
    top_idx = jnp.tile(top_target * 16 + top_source, 16)
    top_idx = jnp.where(lane // 8 == me // GROUP, top_idx, 0).reshape(1, N)

    basis = leaf_basis.reshape(LEAVES, K, M)
    leaf_t = leaf_transfer.reshape(LEAVES * K, K)
    mid_t = mid_transfer.reshape(GROUP * K, K)
    base_t = base_transfer.reshape(K, K)
    r_blk, r_src, every, top_all, tops, source, target = exchange_call(
        blk, blk_src, top_coupling, top_idx, points, rows, basis, leaf_t, mid_t, base_t
    )
    by_source = (lane[:, None] == r_src[:, 0, :2].reshape(1, 2 * N)).astype(bf16)
    a = dot(by_source, r_blk.reshape(2 * N, K * K))
    a = a.reshape(N, K, K).transpose(1, 0, 2).reshape(K, N * K)
    t = jnp.sum(tops.astype(f32), axis=0)
    t = t.reshape(16, K, K).transpose(1, 0, 2).reshape(K, 16 * K)
    far = (
        *high_low(a),
        every.reshape(N * K, RHS),
        *high_low(t),
        top_all.reshape(16 * K, RHS),
        base_t,
    )
    near = jnp.pad(near_leaves, ((0, 0), (0, 1)), constant_values=POOL).reshape(-1)
    return near_call(near, source, target, before, rows, after, far, mid_t, leaf_t, basis)


def solution(mesh):
    lead = P(AXIS, None)
    in_specs = (
        P(None, AXIS),
        lead,
        lead,
        lead,
        lead,
        lead,
        lead,
        lead,
        lead,
        P(AXIS),
        lead,
        P(AXIS),
        P(AXIS),
    )
    return jax.shard_map(
        per_device, mesh=mesh, in_specs=in_specs, out_specs=lead, check_vma=False
    )
```

```python
import functools
import math

import jax
import jax.numpy as jnp
from jax import lax
from jax.experimental import pallas as pl
from jax.experimental.pallas import tpu as pltpu
from jax.sharding import PartitionSpec as P

K = 32
RHS = 128
M = 128
N = 128
LEAVES = 64
POOL = 3 * LEAVES
NNEAR = 27
HALF = (NNEAR + 1) // 2
GROUP = 8
DELTA_SQ = 0.0025
AXIS = "leaf"
MESH = pl.DeviceIdType.MESH
bf16 = jnp.bfloat16
f32 = jnp.float32


def dot(a, b):
    return jnp.dot(a, b, preferred_element_type=f32)


def dot_t(a, b):
    return lax.dot_general(a, b, (((0,), (0,)), ((), ())), preferred_element_type=f32)


def vmem(*shape):
    return pl.BlockSpec(shape, lambda *_: (0,) * len(shape))


def split3(v):
    high = v.astype(bf16).astype(f32)
    rest = v - high
    mid = rest.astype(bf16).astype(f32)
    return high, mid, rest - mid


def features(scale, points, target):
    centred = [(p - 0.5) * scale for p in points]
    norm = centred[0] * centred[0] + centred[1] * centred[1] + centred[2] * centred[2]
    one = jnp.ones_like(norm)
    rows = []
    for c in centred:
        h, m, l = split3(c)
        if target:
            h, m, l = -2.0 * h, -2.0 * m, -2.0 * l
            rows += [h, h, m, m, h, l]
        else:
            rows += [h, m, h, m, l, h]
    if target:
        rows += [*split3(norm + scale * scale * DELTA_SQ), one, one, one]
    else:
        rows += [one, one, one, *split3(norm)]
    return rows + [jnp.zeros_like(norm)] * (K - len(rows))


def exchange_kernel(
    scale,
    blk,
    blk_src,
    top,
    top_idx,
    points,
    charges,
    basis,
    leaf_t,
    mid_t,
    base_t,
    r_blk,
    r_src,
    every,
    top_all,
    tops,
    source,
    target,
    partner,
    held,
    r_top,
    r_idx,
    lifted,
    coeffs,
    mine,
    mids,
    part,
    others,
    lines,
    send,
    recv,
    local,
):
    me = lax.axis_index(AXIS)
    plane, place = me // GROUP, me % GROUP
    core, y = place % 2, place // 2
    fetch = pltpu.make_async_copy(charges, held, local.at[0])
    fetch.start()
    barrier = pltpu.get_barrier_semaphore()

    def hello(o, c):
        pl.semaphore_signal(
            barrier, inc=1, device_id=(lax.rem(me + o, N),), device_id_type=MESH
        )
        return c

    lax.fori_loop(1, N, hello, 0)
    pl.semaphore_wait(barrier, N - 1)

    def remote(src, dst, k, to):
        return pltpu.make_async_remote_copy(
            src_ref=src,
            dst_ref=dst,
            send_sem=send.at[k],
            recv_sem=recv.at[k],
            device_id=(to,),
            device_id_type=MESH,
        )

    def finish(ref, k):
        whole = remote(ref, ref, k, me)
        whole.wait_send()
        whole.wait_recv()

    to_partner = remote(points, others.at[0], 0, me + 1 - 2 * core)
    to_other = remote(points, others.at[1], 1, lax.rem(me - 1 + 2 * core + N, N))
    to_partner.start()
    to_other.start()

    def give_top(o, c):
        to = lax.rem(plane + o, 16) * GROUP + place
        remote(top, r_top.at[plane], 2, to).start()
        remote(top_idx, r_idx.at[plane], 3, to).start()
        return c

    lax.fori_loop(1, 16, give_top, 0)

    def give(o, c):
        to = lax.rem(me + o, N)
        remote(blk.at[to], r_blk.at[me], 4, to).start()
        remote(blk_src.at[to], r_src.at[me], 5, to).start()
        return c

    lax.fori_loop(1, N, give, 0)
    own = [
        pltpu.make_async_copy(blk.at[me], r_blk.at[me], local.at[1]),
        pltpu.make_async_copy(blk_src.at[me], r_src.at[me], local.at[2]),
        pltpu.make_async_copy(top, r_top.at[plane], local.at[3]),
        pltpu.make_async_copy(top_idx, r_idx.at[plane], local.at[4]),
    ]
    for copy in own:
        copy.start()

    fetch.wait()
    swap = remote(held, partner, 12, me + 1 - 2 * core)
    swap.start()

    def one_mid(m, c):
        rows = []
        for b in range(GROUP):
            rows.append(dot(basis[m * GROUP + b], held[m * GROUP + b]).astype(bf16))
        first = pl.multiple_of(m * GROUP * K, GROUP * K)
        rows = dot_t(leaf_t[pl.ds(first, GROUP * K), :], jnp.concatenate(rows, axis=0))
        mids[pl.ds(pl.multiple_of(m * K, K), K), :] = rows.astype(bf16)
        return c

    lax.fori_loop(0, GROUP, one_mid, 0)
    base = dot_t(mid_t[...], mids[...]).astype(bf16)
    coeffs[0] = base
    coeffs[1] = dot_t(base_t[...], base).astype(bf16)
    for o in range(1, 4):
        to = plane * GROUP + lax.rem(y + o, 4) * 2 + core
        remote(coeffs.at[0], every.at[core, plane, y], 6, to).start()
    for o in range(1, GROUP):
        to = plane * GROUP + lax.rem(place + o, GROUP)
        remote(coeffs.at[1], lifted.at[place], 7, to).start()
    own += [
        pltpu.make_async_copy(coeffs.at[0], every.at[core, plane, y], local.at[5]),
        pltpu.make_async_copy(coeffs.at[1], lifted.at[place], local.at[6]),
    ]
    for copy in own[4:]:
        copy.start()

    def side(rows, put, count):
        for r, row in enumerate(rows):
            lines[pl.ds(r, LEAVES, stride=K), :] = row
        lax.fori_loop(0, count, put, 0, unroll=4)

    def line(l):
        return lines[pl.ds(pl.multiple_of(l * K, K), K), :]

    def put_target(l, c):
        target[l] = line(l).T.astype(bf16)
        return c

    def put_source(block):
        def put(l, c):
            source[block * LEAVES + l] = line(l).astype(bf16)
            return c

        return put

    here = [points[i] for i in range(3)]
    side(features(scale, here, True), put_target, LEAVES)
    for copy in own:
        copy.wait()
    finish(lifted.at[pl.ds(0, 3)], 6)
    for o in range(1, 16):
        to = lax.rem(plane + o, 16) * GROUP + place
        remote(every.at[core, plane], every.at[core, plane], 8, to).start()
    finish(lifted.at[pl.ds(0, GROUP - 1)], 7)
    mine[...] = jnp.sum(lifted[...].astype(f32), axis=0).astype(bf16)
    for o in range(1, 16):
        to = lax.rem(plane + o, 16) * GROUP + place
        remote(mine, top_all.at[plane], 9, to).start()
    own_top = pltpu.make_async_copy(mine, top_all.at[plane], local.at[0])
    own_top.start()
    side(features(scale, here, False), put_source(0), LEAVES)
    own_top.wait()

    finish(r_top.at[pl.ds(0, 15)], 2)
    finish(r_idx.at[pl.ds(0, 15)], 3)
    named = jnp.sum(r_idx[...], axis=0)
    wanted = plane * 16 + lax.broadcasted_iota(jnp.int32, (16, N), 0)
    chosen = jnp.where(wanted == named, 1.0, 0.0).astype(bf16)
    part[...] = dot(chosen, r_top[...].reshape(N, K * K)).astype(bf16)
    for o in range(1, GROUP):
        to = plane * GROUP + lax.rem(place + o, GROUP)
        remote(part, tops.at[place], 10, to).start()
    own_part = pltpu.make_async_copy(part, tops.at[place], local.at[0])
    own_part.start()
    to_partner.wait()
    to_other.wait()
    spare = source[0]
    for l in range(8):
        source[POOL + l] = spare
    side(features(scale, [others[0, i] for i in range(3)], False), put_source(1), LEAVES)
    finish(every.at[0, pl.ds(0, 15)], 8)
    across = remote(every.at[core], every.at[core], 11, me + 1 - 2 * core)
    across.start()
    side(features(scale, [others[1, i] for i in range(3)], False), put_source(2), LEAVES)
    finish(top_all.at[pl.ds(0, 15)], 9)
    own_part.wait()
    finish(tops.at[pl.ds(0, GROUP - 1)], 10)
    across.wait()
    swap.wait()
    finish(r_blk.at[pl.ds(0, N - 1)], 4)
    finish(r_src.at[pl.ds(0, N - 1)], 5)


def exchange_call(blk, blk_src, top, top_idx, points, charges, basis, leaf_t, mid_t, base_t):
    inside = pl.BlockSpec(memory_space=pltpu.VMEM)
    shape = jax.ShapeDtypeStruct
    return pl.pallas_call(
        functools.partial(exchange_kernel, math.sqrt(NNEAR * M)),
        out_shape=(
            shape(blk.shape, bf16),
            shape(blk_src.shape, jnp.int32),
            shape((2, 16, 4, K, RHS), bf16),
            shape((16, K, RHS), bf16),
            shape((GROUP, 16, K * K), bf16),
            shape((POOL + 8, K, M), bf16),
            shape((LEAVES, M, K), bf16),
            shape((LEAVES, M, RHS), bf16),
        ),
        in_specs=[inside] * 5 + [pl.BlockSpec(memory_space=pl.ANY)] + [inside] * 4,
        out_specs=(*(inside,) * 7, pl.BlockSpec(memory_space=pl.ANY)),
        scratch_shapes=[
            pltpu.VMEM((LEAVES, M, RHS), bf16),
            pltpu.VMEM((16, 8, K * K), bf16),
            pltpu.VMEM((16, 1, N), jnp.int32),
            pltpu.VMEM((GROUP, K, RHS), bf16),
            pltpu.VMEM((2, K, RHS), bf16),
            pltpu.VMEM((K, RHS), bf16),
            pltpu.VMEM((GROUP * K, RHS), bf16),
            pltpu.VMEM((16, K * K), bf16),
            pltpu.VMEM((2, 3, LEAVES, M), f32),
            pltpu.VMEM((LEAVES * K, M), f32),
            pltpu.SemaphoreType.DMA((13,)),
            pltpu.SemaphoreType.DMA((13,)),
            pltpu.SemaphoreType.DMA((7,)),
        ],
        compiler_params=pltpu.CompilerParams(
            collective_id=0, has_side_effects=True, vmem_limit_bytes=63 * 1024 * 1024
        ),
        cost_estimate=pl.CostEstimate(flops=10**9, bytes_accessed=10**7, transcendentals=0),
        name="exchange",
    )(blk, blk_src, top, top_idx, points, charges, basis, leaf_t, mid_t, base_t)


def pair_rows(slot, mine, one, two, j, source, pool, kern, gathered):
    squares = dot(mine, jnp.concatenate([source[one], source[two]], axis=1))
    kern[slot, :, 2 * M * j : 2 * M * (j + 1)] = lax.rsqrt(squares.astype(bf16))
    gathered[slot, 2 * M * j : 2 * M * j + M] = pool[one]
    gathered[slot, 2 * M * j + M : 2 * M * (j + 1)] = pool[two]


def load_pool(refs, pool, sems):
    copies = [
        pltpu.make_async_copy(ref, pool.at[pl.ds(LEAVES * i, LEAVES)], sems.at[i])
        for i, ref in enumerate(refs)
    ]
    for copy in copies:
        copy.start()
    pool[POOL] = jnp.zeros((M, RHS), bf16)
    return copies


def close_kernel(near, source, target, here, partner, out, pool, kern, gathered, sems):
    step = pl.program_id(0)

    @pl.when(step == 0)
    def _():
        for copy in load_pool((here, partner), pool, sems):
            copy.wait()

    for b in range(GROUP):
        first = (step * GROUP + b) * HALF
        for j in range(HALF // 2):
            one, two = near[first + 2 * j], near[first + 2 * j + 1]
            pair_rows(b, target[b], one, two, j, source, pool, kern, gathered)
        out[b] = dot(kern[b], gathered[b])


def near_kernel(
    near,
    source,
    target,
    here,
    partner,
    other,
    partial,
    a_high,
    a_low,
    every,
    t_high,
    t_low,
    top_all,
    base_t,
    mid_t,
    leaf_t,
    basis,
    out,
    pool,
    kern,
    gathered,
    base,
    extra,
    sems,
):
    step = pl.program_id(0)

    @pl.when(step == 0)
    def _():
        copies = load_pool((here, partner, other), pool, sems)
        extra[...] = jnp.zeros_like(extra)
        top_field = (dot(t_high[...], top_all[...]) + dot(t_low[...], top_all[...])).astype(bf16)
        coupled = dot(a_high[...], every[...]) + dot(a_low[...], every[...])
        base[...] = (coupled + dot(base_t[...], top_field)).astype(bf16)
        for copy in copies:
            copy.wait()

    late = near[2 * LEAVES * HALF + LEAVES + step]

    @pl.when(late > 0)
    def _():
        def one_leaf(b, c):
            leaf = step * GROUP + b

            def one_entry(e, total):
                g = near[(LEAVES + leaf) * HALF + e]
                squares = dot(target[b], source[g])
                return total + dot(lax.rsqrt(squares.astype(bf16)), pool[g])

            extra[b] = lax.fori_loop(
                near[2 * LEAVES * HALF + leaf], HALF, one_entry, jnp.zeros((M, RHS), f32)
            )
            return c

        lax.fori_loop(0, GROUP, one_leaf, 0)

    mid = dot(mid_t[...], base[...]).astype(bf16)
    fields = dot(leaf_t[...], mid).astype(bf16)
    for b in range(GROUP):
        first = (step * GROUP + b) * HALF
        for j in range(HALF // 2):
            one, two = near[first + 2 * j], near[first + 2 * j + 1]
            pair_rows(b, target[b], one, two, j, source, pool, kern, gathered)
        far = dot_t(basis[b], fields[b * K : (b + 1) * K])
        total = dot(kern[b], gathered[b]) + far + (partial[b] + extra[b])
        out[pl.ds(b * M, M), :] = total.astype(bf16)

    @pl.when(late > 0)
    def _():
        extra[...] = jnp.zeros_like(extra)


def near_scratch():
    return [
        pltpu.VMEM((POOL + 1, M, RHS), bf16),
        pltpu.VMEM((GROUP, M, M * HALF), bf16),
        pltpu.VMEM((GROUP, M * HALF, RHS), bf16),
    ]


NEAR_PARAMS = dict(
    compiler_params=pltpu.CompilerParams(
        vmem_limit_bytes=63 * 1024 * 1024, dimension_semantics=("arbitrary",)
    ),
    cost_estimate=pl.CostEstimate(
        flops=5 * 10**9, bytes_accessed=10**7, transcendentals=10**7
    ),
)


def close_call(near, source, target, here, partner):
    anywhere = pl.BlockSpec(memory_space=pl.ANY)
    grid_spec = pltpu.PrefetchScalarGridSpec(
        num_scalar_prefetch=1,
        grid=(LEAVES // GROUP,),
        in_specs=[
            vmem(*source.shape),
            pl.BlockSpec((GROUP, M, K), lambda i, _: (i, 0, 0)),
            anywhere,
            anywhere,
        ],
        out_specs=pl.BlockSpec((GROUP, M, RHS), lambda i, _: (i, 0, 0)),
        scratch_shapes=[*near_scratch(), pltpu.SemaphoreType.DMA((2,))],
    )
    return pl.pallas_call(
        close_kernel,
        grid_spec=grid_spec,
        out_shape=jax.ShapeDtypeStruct((LEAVES, M, RHS), f32),
        name="close",
        **NEAR_PARAMS,
    )(near, source, target, here, partner)


def near_call(near, source, target, here, partner, other, partial, far, mid_t, leaf_t, basis):
    anywhere = pl.BlockSpec(memory_space=pl.ANY)
    grid_spec = pltpu.PrefetchScalarGridSpec(
        num_scalar_prefetch=1,
        grid=(LEAVES // GROUP,),
        in_specs=[
            vmem(*source.shape),
            pl.BlockSpec((GROUP, M, K), lambda i, _: (i, 0, 0)),
            anywhere,
            anywhere,
            anywhere,
            pl.BlockSpec((GROUP, M, RHS), lambda i, _: (i, 0, 0)),
            *[vmem(*v.shape) for v in far],
            pl.BlockSpec((K, K), lambda i, _: (i, 0)),
            pl.BlockSpec((GROUP * K, K), lambda i, _: (i, 0)),
            pl.BlockSpec((GROUP, K, M), lambda i, _: (i, 0, 0)),
        ],
        out_specs=pl.BlockSpec((GROUP * M, RHS), lambda i, _: (i, 0)),
        scratch_shapes=[
            *near_scratch(),
            pltpu.VMEM((K, RHS), bf16),
            pltpu.VMEM((GROUP, M, RHS), f32),
            pltpu.SemaphoreType.DMA((3,)),
        ],
    )
    return pl.pallas_call(
        near_kernel,
        grid_spec=grid_spec,
        out_shape=jax.ShapeDtypeStruct((LEAVES * M, RHS), bf16),
        name="near",
        **NEAR_PARAMS,
    )(near, source, target, here, partner, other, partial, *far, mid_t, leaf_t, basis)


def near_lists(near_leaves, core):
    block, inside = near_leaves // LEAVES, near_leaves % LEAVES
    moved = jnp.where(block == 1, 0, jnp.where((block == 0) == (core == 0), 2, 1))
    place = moved * LEAVES + inside
    away = place >= 2 * LEAVES
    column = jnp.arange(NNEAR)
    key = jnp.where(away, NNEAR, 0) + column
    rank = jnp.sum(key[:, None, :] < key[:, :, None], axis=2)
    ordered = jnp.sum(
        jnp.where(rank[:, :, None] == jnp.arange(2 * HALF), place[:, :, None] + 1, 0), axis=1
    )
    ordered = jnp.where(ordered == 0, POOL, ordered - 1)
    early = ordered[:, :HALF]
    close = jnp.where(early >= 2 * LEAVES, POOL, early).reshape(-1)
    ready = jnp.minimum(NNEAR - jnp.sum(away, axis=1), HALF)
    late = jnp.sum((HALF - ready).reshape(GROUP, GROUP), axis=1)
    rest = jnp.concatenate([ordered[:, HALF:].reshape(-1), early.reshape(-1), ready, late])
    return close.astype(jnp.int32), rest.astype(jnp.int32)


def high_low(v):
    high = v.astype(bf16)
    return high, (v - high.astype(f32)).astype(bf16)


def per_device(
    coords,
    charges,
    near_leaves,
    leaf_basis,
    leaf_transfer,
    mid_transfer,
    base_transfer,
    base_coupling,
    base_target,
    base_source,
    top_coupling,
    top_target,
    top_source,
):
    me = lax.axis_index(AXIS)
    rows = charges.reshape(LEAVES, M, RHS)
    points = coords.reshape(3, LEAVES, M)

    targets = base_target[:, 0]
    count = targets.shape[0]
    earlier = jnp.arange(count)[:, None] > jnp.arange(count)[None, :]
    rank = jnp.sum((targets[:, None] == targets[None, :]) & earlier, axis=1)
    slots = jnp.arange(2 * N)
    chosen = (slots[:, None] == (2 * targets + rank)[None, :]).astype(bf16)
    blk = dot(chosen, base_coupling).astype(bf16).reshape(N, 16, 128)
    order = (base_source % 2) * 64 + (base_source // 8) * 4 + (base_source // 2) % 4
    slot_source = jnp.sum(chosen.astype(jnp.int32) * (order + 1)[None, :], axis=1) - 1
    blk_src = jnp.pad(slot_source.reshape(N, 1, 2), ((0, 0), (0, 0), (0, 126)))
    lane = jnp.arange(N)
    top_idx = jnp.tile(top_target * 16 + top_source, 16)
    top_idx = jnp.where(lane // 8 == me // GROUP, top_idx, 0).reshape(1, N)

    basis = leaf_basis.reshape(LEAVES, K, M)
    leaf_t = leaf_transfer.reshape(LEAVES * K, K)
    mid_t = mid_transfer.reshape(GROUP * K, K)
    base_t = base_transfer.reshape(K, K)
    r_blk, r_src, every, top_all, tops, source, target, partner = exchange_call(
        blk, blk_src, top_coupling, top_idx, points, rows, basis, leaf_t, mid_t, base_t
    )
    outward = [(i, i + 1) for i in range(1, N - 1, 2)] + [(i, i - 1) for i in range(2, N, 2)]
    sent, partner = lax.optimization_barrier((rows, partner))
    other = lax.ppermute(sent, AXIS, outward)
    close_list, near_list = near_lists(near_leaves, me % 2)
    partial = close_call(close_list, source, target, rows, partner)
    by_source = (lane[:, None] == r_src[:, 0, :2].reshape(1, 2 * N)).astype(bf16)
    a = dot(by_source, r_blk.reshape(2 * N, K * K))
    a = a.reshape(N, K, K).transpose(1, 0, 2).reshape(K, N * K)
    t = jnp.sum(tops.astype(f32), axis=0)
    t = t.reshape(16, K, K).transpose(1, 0, 2).reshape(K, 16 * K)
    far = (
        *high_low(a),
        every.reshape(N * K, RHS),
        *high_low(t),
        top_all.reshape(16 * K, RHS),
        base_t,
    )
    return near_call(
        near_list, source, target, rows, partner, other, partial, far, mid_t, leaf_t, basis
    )


def solution(mesh):
    lead = P(AXIS, None)
    in_specs = (
        P(None, AXIS),
        lead,
        lead,
        lead,
        lead,
        lead,
        lead,
        lead,
        lead,
        P(AXIS),
        lead,
        P(AXIS),
        P(AXIS),
    )
    return jax.shard_map(
        per_device, mesh=mesh, in_specs=in_specs, out_specs=lead, check_vma=False
    )
```

```python
import functools
import math

import jax
import jax.numpy as jnp
from jax import lax
from jax.experimental import pallas as pl
from jax.experimental.pallas import tpu as pltpu
from jax.sharding import PartitionSpec as P

K = 32
RHS = 128
M = 128
N = 128
LEAVES = 64
POOL = 3 * LEAVES
NNEAR = 27
HALF = (NNEAR + 1) // 2
GROUP = 8
DELTA_SQ = 0.0025
AXIS = "leaf"
MESH = pl.DeviceIdType.MESH
bf16 = jnp.bfloat16
f32 = jnp.float32


def dot(a, b):
    return jnp.dot(a, b, preferred_element_type=f32)


def dot_t(a, b):
    return lax.dot_general(a, b, (((0,), (0,)), ((), ())), preferred_element_type=f32)


def vmem(*shape):
    return pl.BlockSpec(shape, lambda *_: (0,) * len(shape))


def split3(v):
    high = v.astype(bf16).astype(f32)
    rest = v - high
    mid = rest.astype(bf16).astype(f32)
    return high, mid, rest - mid


def features(scale, points, target):
    centred = [(p - 0.5) * scale for p in points]
    norm = centred[0] * centred[0] + centred[1] * centred[1] + centred[2] * centred[2]
    one = jnp.ones_like(norm)
    rows = []
    for c in centred:
        h, m, l = split3(c)
        if target:
            h, m, l = -2.0 * h, -2.0 * m, -2.0 * l
            rows += [h, h, m, m, h, l]
        else:
            rows += [h, m, h, m, l, h]
    if target:
        rows += [*split3(norm + scale * scale * DELTA_SQ), one, one, one]
    else:
        rows += [one, one, one, *split3(norm)]
    return rows + [jnp.zeros_like(norm)] * (K - len(rows))


def exchange_kernel(
    scale,
    near,
    blk,
    blk_src,
    top,
    top_idx,
    coords,
    charges,
    basis,
    transfers,
    r_blk,
    r_src,
    every,
    top_all,
    top_sum,
    source,
    target,
    partner,
    other,
    partial,
    pool,
    kern,
    gathered,
    sums,
    points,
    tops,
    r_top,
    r_idx,
    lifted,
    coeffs,
    mine,
    mids,
    part,
    others,
    lines,
    send,
    recv,
    local,
    leave,
):
    me = lax.axis_index(AXIS)
    plane, place = me // GROUP, me % GROUP
    core, y = place % 2, place // 2
    held = pool.at[pl.ds(0, LEAVES)]
    fetch = pltpu.make_async_copy(charges, held, local.at[0])
    fetch.start()
    barrier = pltpu.get_barrier_semaphore()

    def hello(o, c):
        pl.semaphore_signal(
            barrier, inc=1, device_id=(lax.rem(me + o, N),), device_id_type=MESH
        )
        return c

    lax.fori_loop(1, N, hello, 0)
    for i in range(3):
        for l in range(LEAVES):
            points[i, l : l + 1, :] = coords[i : i + 1, l * M : (l + 1) * M]
    pool[2 * LEAVES] = jnp.zeros((M, RHS), bf16)

    fetch.wait()

    def one_mid(m, c):
        rows = []
        for b in range(GROUP):
            rows.append(dot(basis[m * GROUP + b], pool[m * GROUP + b]).astype(bf16))
        first = pl.multiple_of(m * GROUP * K, GROUP * K)
        rows = dot_t(transfers[pl.ds(first, GROUP * K), :], jnp.concatenate(rows, axis=0))
        mids[pl.ds(pl.multiple_of(m * K, K), K), :] = rows.astype(bf16)
        return c

    lax.fori_loop(0, GROUP, one_mid, 0)
    base = dot_t(transfers[LEAVES * K : LEAVES * K + GROUP * K, :], mids[...]).astype(bf16)
    coeffs[0] = base
    coeffs[1] = dot_t(transfers[LEAVES * K + GROUP * K :, :], base).astype(bf16)
    pl.semaphore_wait(barrier, N - 1)

    def remote(src, dst, k, to):
        return pltpu.make_async_remote_copy(
            src_ref=src,
            dst_ref=dst,
            send_sem=send.at[k],
            recv_sem=recv.at[k],
            device_id=(to,),
            device_id_type=MESH,
        )

    def finish(ref, k):
        whole = remote(ref, ref, k, me)
        whole.wait_send()
        whole.wait_recv()

    across_chip, next_chip = me + 1 - 2 * core, lax.rem(me - 1 + 2 * core + N, N)
    for o in range(1, 4):
        to = plane * GROUP + lax.rem(y + o, 4) * 2 + core
        remote(coeffs.at[0], every.at[core, plane, y], 6, to).start()
    for o in range(1, GROUP):
        to = plane * GROUP + lax.rem(place + o, GROUP)
        remote(coeffs.at[1], lifted.at[place], 7, to).start()
    to_partner = remote(points, others.at[0], 0, across_chip)
    to_other = remote(points, others.at[1], 1, next_chip)
    to_partner.start()
    to_other.start()
    swap = remote(held, pool.at[pl.ds(LEAVES, LEAVES)], 12, across_chip)
    swap.start()

    def give_top(o, c):
        to = lax.rem(plane + o, 16) * GROUP + place
        remote(top, r_top.at[plane], 2, to).start()
        remote(top_idx, r_idx.at[plane], 3, to).start()
        return c

    lax.fori_loop(1, 16, give_top, 0)

    def give(o, c):
        to = lax.rem(me + o, N)
        remote(blk.at[to], r_blk.at[me], 4, to).start()
        remote(blk_src.at[to], r_src.at[me], 5, to).start()
        return c

    lax.fori_loop(1, N, give, 0)
    outward = remote(held, other, 13, next_chip)
    outward.start()
    own = [
        pltpu.make_async_copy(blk.at[me], r_blk.at[me], local.at[1]),
        pltpu.make_async_copy(blk_src.at[me], r_src.at[me], local.at[2]),
        pltpu.make_async_copy(top, r_top.at[plane], local.at[3]),
        pltpu.make_async_copy(top_idx, r_idx.at[plane], local.at[4]),
        pltpu.make_async_copy(coeffs.at[0], every.at[core, plane, y], local.at[5]),
        pltpu.make_async_copy(coeffs.at[1], lifted.at[place], local.at[6]),
    ]
    for copy in own:
        copy.start()

    def side(rows, put, count):
        for r, row in enumerate(rows):
            lines[pl.ds(r, LEAVES, stride=K), :] = row
        lax.fori_loop(0, count, put, 0, unroll=4)

    def line(l):
        return lines[pl.ds(pl.multiple_of(l * K, K), K), :]

    def put_target(l, c):
        target[l] = line(l).T.astype(bf16)
        return c

    def put_source(block):
        def put(l, c):
            source[block * LEAVES + l] = line(l).astype(bf16)
            return c

        return put

    here = [points[i] for i in range(3)]
    side(features(scale, here, True), put_target, LEAVES)
    for copy in own:
        copy.wait()
    finish(lifted.at[pl.ds(0, 3)], 6)
    for o in range(1, 16):
        to = lax.rem(plane + o, 16) * GROUP + place
        remote(every.at[core, plane], every.at[core, plane], 8, to).start()
    finish(lifted.at[pl.ds(0, GROUP - 1)], 7)
    mine[...] = jnp.sum(lifted[...].astype(f32), axis=0).astype(bf16)
    for o in range(1, 16):
        to = lax.rem(plane + o, 16) * GROUP + place
        remote(mine, top_all.at[plane], 9, to).start()
    own_top = pltpu.make_async_copy(mine, top_all.at[plane], local.at[0])
    own_top.start()
    side(features(scale, here, False), put_source(0), LEAVES)
    own_top.wait()
    to_partner.wait()
    to_other.wait()
    spare = source[0]
    for l in range(8):
        source[POOL + l] = spare
    for i in range(2):
        side(features(scale, [others[i, j] for j in range(3)], False), put_source(i + 1), LEAVES)

    finish(r_top.at[pl.ds(0, 15)], 2)
    finish(r_idx.at[pl.ds(0, 15)], 3)
    named = jnp.sum(r_idx[...], axis=0)
    wanted = plane * 16 + lax.broadcasted_iota(jnp.int32, (16, N), 0)
    chosen = jnp.where(wanted == named, 1.0, 0.0).astype(bf16)
    part[...] = dot(chosen, r_top[...].reshape(N, K * K)).astype(bf16)
    for o in range(1, GROUP):
        to = plane * GROUP + lax.rem(place + o, GROUP)
        remote(part, tops.at[place], 10, to).start()
    own_part = pltpu.make_async_copy(part, tops.at[place], local.at[0])
    own_part.start()

    swap.wait()
    keep = pltpu.make_async_copy(pool.at[pl.ds(LEAVES, LEAVES)], partner, local.at[1])
    keep.start()

    def close_group(group, c):
        for b in range(GROUP):
            leaf = group * GROUP + b
            for j in range(HALF // 2):
                one, two = near[leaf, 2 * j], near[leaf, 2 * j + 1]
                pair_rows(
                    b, target[leaf], one, two, j, source, pool, kern, gathered, 2 * LEAVES
                )
            sums[leaf] = dot(kern[b], gathered[b])
        return c

    lax.fori_loop(0, 2, close_group, 0)
    finish(every.at[0, pl.ds(0, 15)], 8)
    across = remote(every.at[core], every.at[core], 11, across_chip)
    across.start()
    lax.fori_loop(2, 4, close_group, 0)
    own_part.wait()
    finish(tops.at[pl.ds(0, GROUP - 1)], 10)
    top_sum[...] = jnp.sum(tops[...].astype(f32), axis=0)
    lax.fori_loop(4, GROUP, close_group, 0)
    away = pltpu.make_async_copy(sums, partial, leave)
    away.start()
    finish(top_all.at[pl.ds(0, 15)], 9)
    across.wait()
    finish(r_blk.at[pl.ds(0, N - 1)], 4)
    finish(r_src.at[pl.ds(0, N - 1)], 5)
    keep.wait()
    away.wait()
    outward.wait()


def exchange_call(near, blk, blk_src, top, top_idx, coords, charges, basis, transfers):
    inside = pl.BlockSpec(memory_space=pltpu.VMEM)
    anywhere = pl.BlockSpec(memory_space=pl.ANY)
    shape = jax.ShapeDtypeStruct
    return pl.pallas_call(
        functools.partial(exchange_kernel, math.sqrt(NNEAR * M)),
        out_shape=(
            shape(blk.shape, bf16),
            shape(blk_src.shape, jnp.int32),
            shape((2, 16, 4, K, RHS), bf16),
            shape((16, K, RHS), bf16),
            shape((16, K * K), f32),
            shape((POOL + 8, K, M), bf16),
            shape((LEAVES, M, K), bf16),
            shape((LEAVES, M, RHS), bf16),
            shape((LEAVES, M, RHS), bf16),
            shape((LEAVES, M, RHS), f32),
        ),
        in_specs=[
            pl.BlockSpec(memory_space=pltpu.SMEM),
            *[inside] * 5,
            anywhere,
            inside,
            inside,
        ],
        out_specs=(*[inside] * 7, *[anywhere] * 3),
        scratch_shapes=[
            pltpu.VMEM((2 * LEAVES + 1, M, RHS), bf16),
            pltpu.VMEM((GROUP, M, M * HALF), bf16),
            pltpu.VMEM((GROUP, M * HALF, RHS), bf16),
            pltpu.VMEM((LEAVES, M, RHS), f32),
            pltpu.VMEM((3, LEAVES, M), f32),
            pltpu.VMEM((GROUP, 16, K * K), bf16),
            pltpu.VMEM((16, 8, K * K), bf16),
            pltpu.VMEM((16, 1, N), jnp.int32),
            pltpu.VMEM((GROUP, K, RHS), bf16),
            pltpu.VMEM((2, K, RHS), bf16),
            pltpu.VMEM((K, RHS), bf16),
            pltpu.VMEM((GROUP * K, RHS), bf16),
            pltpu.VMEM((16, K * K), bf16),
            pltpu.VMEM((2, 3, LEAVES, M), f32),
            pltpu.VMEM((LEAVES * K, M), f32),
            pltpu.SemaphoreType.DMA((14,)),
            pltpu.SemaphoreType.DMA((14,)),
            pltpu.SemaphoreType.DMA((7,)),
            pltpu.SemaphoreType.DMA,
        ],
        compiler_params=pltpu.CompilerParams(
            collective_id=0, has_side_effects=True, vmem_limit_bytes=63 * 1024 * 1024
        ),
        cost_estimate=pl.CostEstimate(flops=10**9, bytes_accessed=10**7, transcendentals=0),
        name="exchange",
    )(near, blk, blk_src, top, top_idx, coords, charges, basis, transfers)


def pair_rows(slot, mine, one, two, j, source, pool, kern, gathered, last):
    squares = dot(mine, jnp.concatenate([source[one], source[two]], axis=1))
    kern[slot, :, 2 * M * j : 2 * M * (j + 1)] = lax.rsqrt(squares.astype(bf16))
    gathered[slot, 2 * M * j : 2 * M * j + M] = pool[jnp.minimum(one, last)]
    gathered[slot, 2 * M * j + M : 2 * M * (j + 1)] = pool[jnp.minimum(two, last)]


def load_pool(refs, pool, sems):
    copies = [
        pltpu.make_async_copy(ref, pool.at[pl.ds(LEAVES * i, LEAVES)], sems.at[i])
        for i, ref in enumerate(refs)
    ]
    for copy in copies:
        copy.start()
    pool[POOL] = jnp.zeros((M, RHS), bf16)
    return copies


def near_kernel(
    near,
    source,
    target,
    here,
    partner,
    other,
    partial,
    a_high,
    a_low,
    every,
    t_high,
    t_low,
    top_all,
    transfers,
    basis,
    out,
    pool,
    kern,
    gathered,
    base,
    extra,
    sems,
):
    step = pl.program_id(0)

    @pl.when(step == 0)
    def _():
        copies = load_pool((here, partner, other), pool, sems)
        extra[...] = jnp.zeros_like(extra)
        top_field = (dot(t_high[...], top_all[...]) + dot(t_low[...], top_all[...])).astype(bf16)
        coupled = dot(a_high[...], every[...]) + dot(a_low[...], every[...])
        base[...] = (coupled + dot(transfers[(LEAVES + GROUP) * K :, :], top_field)).astype(bf16)
        for copy in copies:
            copy.wait()

        @pl.when(near[0, 2 * HALF + 1] > 0)
        def _():
            pool[pl.ds(2 * LEAVES, LEAVES)] = jnp.zeros((LEAVES, M, RHS), bf16)

    late = jnp.int32(0)
    for b in range(GROUP):
        late += HALF - near[step * GROUP + b, 2 * HALF]

    @pl.when(late > 0)
    def _():
        def one_leaf(b, c):
            leaf = step * GROUP + b

            def one_entry(e, total):
                g = near[leaf, e]
                squares = dot(target[b], source[g])
                return total + dot(lax.rsqrt(squares.astype(bf16)), pool[g])

            extra[b] = lax.fori_loop(
                near[leaf, 2 * HALF], HALF, one_entry, jnp.zeros((M, RHS), f32)
            )
            return c

        lax.fori_loop(0, GROUP, one_leaf, 0)

    down = transfers[pl.ds(pl.multiple_of((LEAVES + step) * K, K), K), :]
    mid = dot(down, base[...]).astype(bf16)
    down = transfers[pl.ds(pl.multiple_of(step * GROUP * K, GROUP * K), GROUP * K), :]
    fields = dot(down, mid).astype(bf16)
    for b in range(GROUP):
        leaf = step * GROUP + b
        for j in range(HALF // 2):
            one, two = near[leaf, HALF + 2 * j], near[leaf, HALF + 2 * j + 1]
            pair_rows(b, target[b], one, two, j, source, pool, kern, gathered, POOL)
        far = dot_t(basis[b], fields[b * K : (b + 1) * K])
        total = dot(kern[b], gathered[b]) + far + (partial[b] + extra[b])
        out[pl.ds(b * M, M), :] = total.astype(bf16)

    @pl.when(late > 0)
    def _():
        extra[...] = jnp.zeros_like(extra)


def near_scratch():
    return [
        pltpu.VMEM((POOL + 1, M, RHS), bf16),
        pltpu.VMEM((GROUP, M, M * HALF), bf16),
        pltpu.VMEM((GROUP, M * HALF, RHS), bf16),
    ]


NEAR_PARAMS = dict(
    compiler_params=pltpu.CompilerParams(
        vmem_limit_bytes=63 * 1024 * 1024, dimension_semantics=("arbitrary",)
    ),
    cost_estimate=pl.CostEstimate(
        flops=5 * 10**9, bytes_accessed=10**7, transcendentals=10**7
    ),
)


def near_call(near, source, target, here, partner, other, partial, far, transfers, basis):
    anywhere = pl.BlockSpec(memory_space=pl.ANY)
    grid_spec = pltpu.PrefetchScalarGridSpec(
        num_scalar_prefetch=1,
        grid=(LEAVES // GROUP,),
        in_specs=[
            vmem(*source.shape),
            pl.BlockSpec((GROUP, M, K), lambda i, _: (i, 0, 0)),
            anywhere,
            anywhere,
            anywhere,
            pl.BlockSpec((GROUP, M, RHS), lambda i, _: (i, 0, 0)),
            *[vmem(*v.shape) for v in far],
            vmem(*transfers.shape),
            pl.BlockSpec((GROUP, K, M), lambda i, _: (i, 0, 0)),
        ],
        out_specs=pl.BlockSpec((GROUP * M, RHS), lambda i, _: (i, 0)),
        scratch_shapes=[
            *near_scratch(),
            pltpu.VMEM((K, RHS), bf16),
            pltpu.VMEM((GROUP, M, RHS), f32),
            pltpu.SemaphoreType.DMA((3,)),
        ],
    )
    return pl.pallas_call(
        near_kernel,
        grid_spec=grid_spec,
        out_shape=jax.ShapeDtypeStruct((LEAVES * M, RHS), bf16),
        name="near",
        **NEAR_PARAMS,
    )(near, source, target, here, partner, other, partial, *far, transfers, basis)


def near_lists(near_leaves, core, edge):
    block, inside = near_leaves // LEAVES, near_leaves % LEAVES
    moved = jnp.where(block == 1, 0, jnp.where((block == 0) == (core == 0), 2, 1))
    place = moved * LEAVES + inside
    away = place >= 2 * LEAVES
    column = jnp.arange(NNEAR)
    key = jnp.where(away, NNEAR, 0) + column
    rank = jnp.sum(key[:, None, :] < key[:, :, None], axis=2)
    ordered = jnp.sum(
        jnp.where(rank[:, :, None] == jnp.arange(2 * HALF), place[:, :, None] + 1, 0), axis=1
    )
    ordered = jnp.where(ordered == 0, POOL, ordered - 1)
    ready = jnp.minimum(NNEAR - jnp.sum(away, axis=1, keepdims=True), HALF)
    return jnp.concatenate([ordered, ready, jnp.full_like(ready, edge)], axis=1)


def high_low(v):
    high = v.astype(bf16)
    return high, (v - high.astype(f32)).astype(bf16)


def per_device(
    coords,
    charges,
    near_leaves,
    leaf_basis,
    leaf_transfer,
    mid_transfer,
    base_transfer,
    base_coupling,
    base_target,
    base_source,
    top_coupling,
    top_target,
    top_source,
):
    me = lax.axis_index(AXIS)
    rows = charges.reshape(LEAVES, M, RHS)
    targets = base_target[:, 0]
    count = targets.shape[0]
    earlier = jnp.arange(count)[:, None] > jnp.arange(count)[None, :]
    rank = jnp.sum((targets[:, None] == targets[None, :]) & earlier, axis=1)
    slots = jnp.arange(2 * N)
    chosen = (slots[:, None] == (2 * targets + rank)[None, :]).astype(bf16)
    blk = dot(chosen, base_coupling).astype(bf16).reshape(N, 16, 128)
    order = (base_source % 2) * 64 + (base_source // 8) * 4 + (base_source // 2) % 4
    slot_source = jnp.sum(chosen.astype(jnp.int32) * (order + 1)[None, :], axis=1) - 1
    blk_src = jnp.pad(slot_source.reshape(N, 1, 2), ((0, 0), (0, 0), (0, 126)))
    lane = jnp.arange(N)
    top_idx = jnp.tile(top_target * 16 + top_source, 16)
    top_idx = jnp.where(lane // 8 == me // GROUP, top_idx, 0).reshape(1, N)

    basis = leaf_basis.reshape(LEAVES, K, M)
    transfers = jnp.concatenate([leaf_transfer, mid_transfer, base_transfer], axis=0)
    transfers = transfers.reshape((LEAVES + GROUP + 1) * K, K)
    edge = ((me == 0) | (me == N - 1)).astype(jnp.int32)
    near = near_lists(near_leaves, me % 2, edge)
    r_blk, r_src, every, top_all, t, source, target, partner, other, partial = exchange_call(
        near, blk, blk_src, top_coupling, top_idx, coords, rows, basis, transfers
    )
    by_source = (lane[:, None] == r_src[:, 0, :2].reshape(1, 2 * N)).astype(bf16)
    a = dot(by_source, r_blk.reshape(2 * N, K * K))
    a = a.reshape(N, K, K).transpose(1, 0, 2).reshape(K, N * K)
    t = t.reshape(16, K, K).transpose(1, 0, 2).reshape(K, 16 * K)
    far = (
        *high_low(a),
        every.reshape(N * K, RHS),
        *high_low(t),
        top_all.reshape(16 * K, RHS),
    )
    return near_call(
        near, source, target, rows, partner, other, partial, far, transfers, basis
    )


def solution(mesh):
    lead = P(AXIS, None)
    in_specs = (
        P(None, AXIS),
        lead,
        lead,
        lead,
        lead,
        lead,
        lead,
        lead,
        lead,
        P(AXIS),
        lead,
        P(AXIS),
        P(AXIS),
    )
    return jax.shard_map(
        per_device, mesh=mesh, in_specs=in_specs, out_specs=lead, check_vma=False
    )
```

```python
import functools
import math

import jax
import jax.numpy as jnp
from jax import lax
from jax.experimental import pallas as pl
from jax.experimental.pallas import tpu as pltpu
from jax.sharding import PartitionSpec as P

K = 32
RHS = 128
M = 128
N = 128
LEAVES = 64
POOL = 3 * LEAVES
NNEAR = 27
HALF = (NNEAR + 1) // 2
GROUP = 8
DELTA_SQ = 0.0025
AXIS = "leaf"
MESH = pl.DeviceIdType.MESH
bf16 = jnp.bfloat16
f32 = jnp.float32


def dot(a, b):
    return jnp.dot(a, b, preferred_element_type=f32)


def dot_t(a, b):
    return lax.dot_general(a, b, (((0,), (0,)), ((), ())), preferred_element_type=f32)


def vmem(*shape):
    return pl.BlockSpec(shape, lambda *_: (0,) * len(shape))


def split3(v):
    high = v.astype(bf16).astype(f32)
    rest = v - high
    mid = rest.astype(bf16).astype(f32)
    return high, mid, rest - mid


def features(scale, points, target):
    centred = [(p - 0.5) * scale for p in points]
    norm = centred[0] * centred[0] + centred[1] * centred[1] + centred[2] * centred[2]
    one = jnp.ones_like(norm)
    rows = []
    for c in centred:
        h, m, l = split3(c)
        if target:
            h, m, l = -2.0 * h, -2.0 * m, -2.0 * l
            rows += [h, h, m, m, h, l]
        else:
            rows += [h, m, h, m, l, h]
    if target:
        rows += [*split3(norm + scale * scale * DELTA_SQ), one, one, one]
    else:
        rows += [one, one, one, *split3(norm)]
    return rows + [jnp.zeros_like(norm)] * (K - len(rows))


def exchange_kernel(
    scale,
    near,
    blk,
    blk_src,
    top,
    top_idx,
    coords,
    charges,
    basis,
    transfers,
    r_blk,
    r_src,
    every,
    top_all,
    top_sum,
    source,
    target,
    partner,
    other,
    partial,
    pool,
    kern,
    gathered,
    sums,
    points,
    half,
    half_src,
    tops,
    r_top,
    r_idx,
    lifted,
    coeffs,
    mine,
    mids,
    part,
    others,
    lines,
    send,
    recv,
    local,
    leave,
):
    me = lax.axis_index(AXIS)
    plane, place = me // GROUP, me % GROUP
    core, y = place % 2, place // 2
    held = pool.at[pl.ds(0, LEAVES)]
    fetch = pltpu.make_async_copy(charges, held, local.at[0])
    fetch.start()
    barrier = pltpu.get_barrier_semaphore()

    across_chip, next_chip = me + 1 - 2 * core, lax.rem(me - 1 + 2 * core + N, N)
    peers = [plane * GROUP + lax.rem(place + o, GROUP) for o in range(1, GROUP)]
    planes = [lax.rem(plane + o, 16) for o in range(1, 16)]
    greeted = [*peers, *[p * GROUP + place for p in planes], next_chip]
    for to in greeted:
        pl.semaphore_signal(barrier, inc=1, device_id=(to,), device_id_type=MESH)
    for i in range(3):
        for l in range(LEAVES):
            points[i, l : l + 1, :] = coords[i : i + 1, l * M : (l + 1) * M]
    pool[2 * LEAVES] = jnp.zeros((M, RHS), bf16)

    fetch.wait()

    def one_mid(m, c):
        rows = []
        for b in range(GROUP):
            rows.append(dot(basis[m * GROUP + b], pool[m * GROUP + b]).astype(bf16))
        first = pl.multiple_of(m * GROUP * K, GROUP * K)
        rows = dot_t(transfers[pl.ds(first, GROUP * K), :], jnp.concatenate(rows, axis=0))
        mids[pl.ds(pl.multiple_of(m * K, K), K), :] = rows.astype(bf16)
        return c

    lax.fori_loop(0, GROUP, one_mid, 0)
    base = dot_t(transfers[LEAVES * K : LEAVES * K + GROUP * K, :], mids[...]).astype(bf16)
    coeffs[0] = base
    coeffs[1] = dot_t(transfers[LEAVES * K + GROUP * K :, :], base).astype(bf16)
    pl.semaphore_wait(barrier, len(greeted))

    def remote(src, dst, k, to):
        return pltpu.make_async_remote_copy(
            src_ref=src,
            dst_ref=dst,
            send_sem=send.at[k],
            recv_sem=recv.at[k],
            device_id=(to,),
            device_id_type=MESH,
        )

    def finish(ref, k):
        whole = remote(ref, ref, k, me)
        whole.wait_send()
        whole.wait_recv()

    for o in range(1, 4):
        to = plane * GROUP + lax.rem(y + o, 4) * 2 + core
        remote(coeffs.at[0], every.at[core, plane, y], 6, to).start()
    for to in peers:
        remote(coeffs.at[1], lifted.at[place], 7, to).start()
    for to in peers:
        remote(blk.at[to % GROUP], half.at[place], 4, to).start()
        remote(blk_src.at[to % GROUP], half_src.at[place], 5, to).start()
    to_partner = remote(points, others.at[0], 0, across_chip)
    to_other = remote(points, others.at[1], 1, next_chip)
    to_partner.start()
    to_other.start()
    swap = remote(held, pool.at[pl.ds(LEAVES, LEAVES)], 12, across_chip)
    swap.start()
    for p in planes:
        to = p * GROUP + place
        remote(top, r_top.at[plane], 2, to).start()
        remote(top_idx, r_idx.at[plane], 3, to).start()
    outward = remote(held, other, 13, next_chip)
    outward.start()
    own = [
        pltpu.make_async_copy(blk.at[place], half.at[place], local.at[1]),
        pltpu.make_async_copy(blk_src.at[place], half_src.at[place], local.at[2]),
        pltpu.make_async_copy(top, r_top.at[plane], local.at[3]),
        pltpu.make_async_copy(top_idx, r_idx.at[plane], local.at[4]),
        pltpu.make_async_copy(coeffs.at[0], every.at[core, plane, y], local.at[5]),
        pltpu.make_async_copy(coeffs.at[1], lifted.at[place], local.at[6]),
    ]
    for copy in own:
        copy.start()

    def side(rows, put, count):
        for r, row in enumerate(rows):
            lines[pl.ds(r, LEAVES, stride=K), :] = row
        lax.fori_loop(0, count, put, 0, unroll=4)

    def line(l):
        return lines[pl.ds(pl.multiple_of(l * K, K), K), :]

    def put_target(l, c):
        target[l] = line(l).T.astype(bf16)
        return c

    def put_source(block):
        def put(l, c):
            source[block * LEAVES + l] = line(l).astype(bf16)
            return c

        return put

    here = [points[i] for i in range(3)]
    side(features(scale, here, True), put_target, LEAVES)
    for copy in own:
        copy.wait()
    finish(lifted.at[pl.ds(0, 3)], 6)
    for p in planes:
        to = p * GROUP + place
        remote(every.at[core, plane], every.at[core, plane], 8, to).start()
    finish(lifted.at[pl.ds(0, GROUP - 1)], 7)
    mine[...] = jnp.sum(lifted[...].astype(f32), axis=0).astype(bf16)
    for p in planes:
        remote(mine, top_all.at[plane], 9, p * GROUP + place).start()
    own_top = pltpu.make_async_copy(mine, top_all.at[plane], local.at[0])
    own_top.start()
    side(features(scale, here, False), put_source(0), LEAVES)
    own_top.wait()

    finish(half.at[pl.ds(0, GROUP - 1)], 4)
    finish(half_src.at[pl.ds(0, GROUP - 1)], 5)
    for p in planes:
        to = p * GROUP + place
        remote(half.at[:, p], r_blk.at[plane], 14, to).start()
        remote(half_src.at[:, p], r_src.at[plane], 15, to).start()
    own = [
        pltpu.make_async_copy(half.at[:, plane], r_blk.at[plane], local.at[2]),
        pltpu.make_async_copy(half_src.at[:, plane], r_src.at[plane], local.at[3]),
    ]
    for copy in own:
        copy.start()
    to_partner.wait()
    to_other.wait()
    spare = source[0]
    for l in range(8):
        source[POOL + l] = spare
    for i in range(2):
        side(features(scale, [others[i, j] for j in range(3)], False), put_source(i + 1), LEAVES)

    swap.wait()
    keep = pltpu.make_async_copy(pool.at[pl.ds(LEAVES, LEAVES)], partner, local.at[1])
    keep.start()

    def close_group(group, c):
        for b in range(GROUP):
            leaf = group * GROUP + b
            for j in range(HALF // 2):
                one, two = near[leaf, 2 * j], near[leaf, 2 * j + 1]
                pair_rows(
                    b, target[leaf], one, two, j, source, pool, kern, gathered, 2 * LEAVES
                )
            sums[leaf] = dot(kern[b], gathered[b])
        return c

    lax.fori_loop(0, 2, close_group, 0)

    finish(r_top.at[pl.ds(0, 15)], 2)
    finish(r_idx.at[pl.ds(0, 15)], 3)
    named = jnp.sum(r_idx[...], axis=0)
    wanted = plane * 16 + lax.broadcasted_iota(jnp.int32, (16, N), 0)
    chosen = jnp.where(wanted == named, 1.0, 0.0).astype(bf16)
    part[...] = dot(chosen, r_top[...].reshape(N, K * K)).astype(bf16)
    for to in peers:
        remote(part, tops.at[place], 10, to).start()
    own_part = pltpu.make_async_copy(part, tops.at[place], local.at[0])
    own_part.start()

    lax.fori_loop(2, 4, close_group, 0)
    finish(every.at[0, pl.ds(0, 15)], 8)
    across = remote(every.at[core], every.at[core], 11, across_chip)
    across.start()
    lax.fori_loop(4, 6, close_group, 0)
    own_part.wait()
    finish(tops.at[pl.ds(0, GROUP - 1)], 10)
    top_sum[...] = jnp.sum(tops[...].astype(f32), axis=0)
    lax.fori_loop(6, GROUP, close_group, 0)
    away = pltpu.make_async_copy(sums, partial, leave)
    away.start()
    finish(top_all.at[pl.ds(0, 15)], 9)
    across.wait()
    for copy in own:
        copy.wait()
    finish(r_blk.at[pl.ds(0, 15)], 14)
    finish(r_src.at[pl.ds(0, 15)], 15)
    keep.wait()
    away.wait()
    outward.wait()


def exchange_call(near, blk, blk_src, top, top_idx, coords, charges, basis, transfers):
    inside = pl.BlockSpec(memory_space=pltpu.VMEM)
    anywhere = pl.BlockSpec(memory_space=pl.ANY)
    shape = jax.ShapeDtypeStruct
    return pl.pallas_call(
        functools.partial(exchange_kernel, math.sqrt(NNEAR * M)),
        out_shape=(
            shape((16, GROUP, *blk.shape[2:]), bf16),
            shape((16, GROUP, *blk_src.shape[2:]), jnp.int32),
            shape((2, 16, 4, K, RHS), bf16),
            shape((16, K, RHS), bf16),
            shape((16, K * K), f32),
            shape((POOL + 8, K, M), bf16),
            shape((LEAVES, M, K), bf16),
            shape((LEAVES, M, RHS), bf16),
            shape((LEAVES, M, RHS), bf16),
            shape((LEAVES, M, RHS), f32),
        ),
        in_specs=[
            pl.BlockSpec(memory_space=pltpu.SMEM),
            *[inside] * 5,
            anywhere,
            inside,
            inside,
        ],
        out_specs=(*[inside] * 7, *[anywhere] * 3),
        scratch_shapes=[
            pltpu.VMEM((2 * LEAVES + 1, M, RHS), bf16),
            pltpu.VMEM((GROUP, M, M * HALF), bf16),
            pltpu.VMEM((GROUP, M * HALF, RHS), bf16),
            pltpu.VMEM((LEAVES, M, RHS), f32),
            pltpu.VMEM((3, LEAVES, M), f32),
            pltpu.VMEM(blk.shape, bf16),
            pltpu.VMEM(blk_src.shape, jnp.int32),
            pltpu.VMEM((GROUP, 16, K * K), bf16),
            pltpu.VMEM((16, 8, K * K), bf16),
            pltpu.VMEM((16, 1, N), jnp.int32),
            pltpu.VMEM((GROUP, K, RHS), bf16),
            pltpu.VMEM((2, K, RHS), bf16),
            pltpu.VMEM((K, RHS), bf16),
            pltpu.VMEM((GROUP * K, RHS), bf16),
            pltpu.VMEM((16, K * K), bf16),
            pltpu.VMEM((2, 3, LEAVES, M), f32),
            pltpu.VMEM((LEAVES * K, M), f32),
            pltpu.SemaphoreType.DMA((16,)),
            pltpu.SemaphoreType.DMA((16,)),
            pltpu.SemaphoreType.DMA((7,)),
            pltpu.SemaphoreType.DMA,
        ],
        compiler_params=pltpu.CompilerParams(
            collective_id=0, has_side_effects=True, vmem_limit_bytes=63 * 1024 * 1024
        ),
        cost_estimate=pl.CostEstimate(flops=10**9, bytes_accessed=10**7, transcendentals=0),
        name="exchange",
    )(near, blk, blk_src, top, top_idx, coords, charges, basis, transfers)


def pair_rows(slot, mine, one, two, j, source, pool, kern, gathered, last):
    squares = dot(mine, jnp.concatenate([source[one], source[two]], axis=1))
    kern[slot, :, 2 * M * j : 2 * M * (j + 1)] = lax.rsqrt(squares.astype(bf16))
    gathered[slot, 2 * M * j : 2 * M * j + M] = pool[jnp.minimum(one, last)]
    gathered[slot, 2 * M * j + M : 2 * M * (j + 1)] = pool[jnp.minimum(two, last)]


def load_pool(refs, pool, sems):
    copies = [
        pltpu.make_async_copy(ref, pool.at[pl.ds(LEAVES * i, LEAVES)], sems.at[i])
        for i, ref in enumerate(refs)
    ]
    for copy in copies:
        copy.start()
    pool[POOL] = jnp.zeros((M, RHS), bf16)
    return copies


def near_kernel(
    near,
    source,
    target,
    here,
    partner,
    other,
    partial,
    a_high,
    a_low,
    every,
    t_high,
    t_low,
    top_all,
    transfers,
    basis,
    out,
    pool,
    kern,
    gathered,
    base,
    extra,
    sems,
):
    step = pl.program_id(0)

    @pl.when(step == 0)
    def _():
        copies = load_pool((here, partner, other), pool, sems)
        extra[...] = jnp.zeros_like(extra)
        top_field = (dot(t_high[...], top_all[...]) + dot(t_low[...], top_all[...])).astype(bf16)
        coupled = dot(a_high[...], every[...]) + dot(a_low[...], every[...])
        base[...] = (coupled + dot(transfers[(LEAVES + GROUP) * K :, :], top_field)).astype(bf16)
        for copy in copies:
            copy.wait()

        @pl.when(near[0, 2 * HALF + 1] > 0)
        def _():
            pool[pl.ds(2 * LEAVES, LEAVES)] = jnp.zeros((LEAVES, M, RHS), bf16)

    late = jnp.int32(0)
    for b in range(GROUP):
        late += HALF - near[step * GROUP + b, 2 * HALF]

    @pl.when(late > 0)
    def _():
        def one_leaf(b, c):
            leaf = step * GROUP + b

            def one_entry(e, total):
                g = near[leaf, e]
                squares = dot(target[b], source[g])
                return total + dot(lax.rsqrt(squares.astype(bf16)), pool[g])

            extra[b] = lax.fori_loop(
                near[leaf, 2 * HALF], HALF, one_entry, jnp.zeros((M, RHS), f32)
            )
            return c

        lax.fori_loop(0, GROUP, one_leaf, 0)

    down = transfers[pl.ds(pl.multiple_of((LEAVES + step) * K, K), K), :]
    mid = dot(down, base[...]).astype(bf16)
    down = transfers[pl.ds(pl.multiple_of(step * GROUP * K, GROUP * K), GROUP * K), :]
    fields = dot(down, mid).astype(bf16)
    for b in range(GROUP):
        leaf = step * GROUP + b
        for j in range(HALF // 2):
            one, two = near[leaf, HALF + 2 * j], near[leaf, HALF + 2 * j + 1]
            pair_rows(b, target[b], one, two, j, source, pool, kern, gathered, POOL)
        far = dot_t(basis[b], fields[b * K : (b + 1) * K])
        total = dot(kern[b], gathered[b]) + far + (partial[b] + extra[b])
        out[pl.ds(b * M, M), :] = total.astype(bf16)

    @pl.when(late > 0)
    def _():
        extra[...] = jnp.zeros_like(extra)


def near_scratch():
    return [
        pltpu.VMEM((POOL + 1, M, RHS), bf16),
        pltpu.VMEM((GROUP, M, M * HALF), bf16),
        pltpu.VMEM((GROUP, M * HALF, RHS), bf16),
    ]


NEAR_PARAMS = dict(
    compiler_params=pltpu.CompilerParams(
        vmem_limit_bytes=63 * 1024 * 1024, dimension_semantics=("arbitrary",)
    ),
    cost_estimate=pl.CostEstimate(
        flops=5 * 10**9, bytes_accessed=10**7, transcendentals=10**7
    ),
)


def near_call(near, source, target, here, partner, other, partial, far, transfers, basis):
    anywhere = pl.BlockSpec(memory_space=pl.ANY)
    grid_spec = pltpu.PrefetchScalarGridSpec(
        num_scalar_prefetch=1,
        grid=(LEAVES // GROUP,),
        in_specs=[
            vmem(*source.shape),
            pl.BlockSpec((GROUP, M, K), lambda i, _: (i, 0, 0)),
            anywhere,
            anywhere,
            anywhere,
            pl.BlockSpec((GROUP, M, RHS), lambda i, _: (i, 0, 0)),
            *[vmem(*v.shape) for v in far],
            vmem(*transfers.shape),
            pl.BlockSpec((GROUP, K, M), lambda i, _: (i, 0, 0)),
        ],
        out_specs=pl.BlockSpec((GROUP * M, RHS), lambda i, _: (i, 0)),
        scratch_shapes=[
            *near_scratch(),
            pltpu.VMEM((K, RHS), bf16),
            pltpu.VMEM((GROUP, M, RHS), f32),
            pltpu.SemaphoreType.DMA((3,)),
        ],
    )
    return pl.pallas_call(
        near_kernel,
        grid_spec=grid_spec,
        out_shape=jax.ShapeDtypeStruct((LEAVES * M, RHS), bf16),
        name="near",
        **NEAR_PARAMS,
    )(near, source, target, here, partner, other, partial, *far, transfers, basis)


def near_lists(near_leaves, core, edge):
    block, inside = near_leaves // LEAVES, near_leaves % LEAVES
    moved = jnp.where(block == 1, 0, jnp.where((block == 0) == (core == 0), 2, 1))
    place = moved * LEAVES + inside
    away = place >= 2 * LEAVES
    column = jnp.arange(NNEAR)
    key = jnp.where(away, NNEAR, 0) + column
    rank = jnp.sum(key[:, None, :] < key[:, :, None], axis=2)
    ordered = jnp.sum(
        jnp.where(rank[:, :, None] == jnp.arange(2 * HALF), place[:, :, None] + 1, 0), axis=1
    )
    ordered = jnp.where(ordered == 0, POOL, ordered - 1)
    ready = jnp.minimum(NNEAR - jnp.sum(away, axis=1, keepdims=True), HALF)
    return jnp.concatenate([ordered, ready, jnp.full_like(ready, edge)], axis=1)


def high_low(v):
    high = v.astype(bf16)
    return high, (v - high.astype(f32)).astype(bf16)


def per_device(
    coords,
    charges,
    near_leaves,
    leaf_basis,
    leaf_transfer,
    mid_transfer,
    base_transfer,
    base_coupling,
    base_target,
    base_source,
    top_coupling,
    top_target,
    top_source,
):
    me = lax.axis_index(AXIS)
    rows = charges.reshape(LEAVES, M, RHS)
    targets = base_target[:, 0]
    count = targets.shape[0]
    earlier = jnp.arange(count)[:, None] > jnp.arange(count)[None, :]
    rank = jnp.sum((targets[:, None] == targets[None, :]) & earlier, axis=1)
    slots = jnp.arange(2 * N)
    places = (targets % GROUP) * 16 + targets // GROUP
    chosen = (slots[:, None] == (2 * places + rank)[None, :]).astype(bf16)
    blk = dot(chosen, base_coupling).astype(bf16).reshape(GROUP, 16, 16, 128)
    order = (base_source % 2) * 64 + (base_source // 8) * 4 + (base_source // 2) % 4
    slot_source = jnp.sum(chosen.astype(jnp.int32) * (order + 1)[None, :], axis=1) - 1
    blk_src = jnp.pad(slot_source.reshape(GROUP, 16, 1, 2), ((0, 0),) * 3 + ((0, 126),))
    lane = jnp.arange(N)
    top_idx = jnp.tile(top_target * 16 + top_source, 16)
    top_idx = jnp.where(lane // 8 == me // GROUP, top_idx, 0).reshape(1, N)

    basis = leaf_basis.reshape(LEAVES, K, M)
    transfers = jnp.concatenate([leaf_transfer, mid_transfer, base_transfer], axis=0)
    transfers = transfers.reshape((LEAVES + GROUP + 1) * K, K)
    edge = ((me == 0) | (me == N - 1)).astype(jnp.int32)
    near = near_lists(near_leaves, me % 2, edge)
    r_blk, r_src, every, top_all, t, source, target, partner, other, partial = exchange_call(
        near, blk, blk_src, top_coupling, top_idx, coords, rows, basis, transfers
    )
    by_source = (lane[:, None] == r_src[:, :, 0, :2].reshape(1, 2 * N)).astype(bf16)
    a = dot(by_source, r_blk.reshape(2 * N, K * K))
    a = a.reshape(N, K, K).transpose(1, 0, 2).reshape(K, N * K)
    t = t.reshape(16, K, K).transpose(1, 0, 2).reshape(K, 16 * K)
    far = (
        *high_low(a),
        every.reshape(N * K, RHS),
        *high_low(t),
        top_all.reshape(16 * K, RHS),
    )
    return near_call(
        near, source, target, rows, partner, other, partial, far, transfers, basis
    )


def solution(mesh):
    lead = P(AXIS, None)
    in_specs = (
        P(None, AXIS),
        lead,
        lead,
        lead,
        lead,
        lead,
        lead,
        lead,
        lead,
        P(AXIS),
        lead,
        P(AXIS),
        P(AXIS),
    )
    return jax.shard_map(
        per_device, mesh=mesh, in_specs=in_specs, out_specs=lead, check_vma=False
    )
```

```python
import functools
import math

import jax
import jax.numpy as jnp
from jax import lax
from jax.experimental import pallas as pl
from jax.experimental.pallas import tpu as pltpu
from jax.sharding import PartitionSpec as P

K = 32
RHS = 128
M = 128
N = 128
LEAVES = 64
POOL = 3 * LEAVES
NNEAR = 27
HALF = (NNEAR + 1) // 2
GROUP = 8
DELTA_SQ = 0.0025
AXIS = "leaf"
MESH = pl.DeviceIdType.MESH
bf16 = jnp.bfloat16
f32 = jnp.float32


def dot(a, b):
    return jnp.dot(a, b, preferred_element_type=f32)


def dot_t(a, b):
    return lax.dot_general(a, b, (((0,), (0,)), ((), ())), preferred_element_type=f32)


def vmem(*shape):
    return pl.BlockSpec(shape, lambda *_: (0,) * len(shape))


def split3(v):
    high = v.astype(bf16).astype(f32)
    rest = v - high
    mid = rest.astype(bf16).astype(f32)
    return high, mid, rest - mid


def features(scale, points, target):
    centred = [(p - 0.5) * scale for p in points]
    norm = centred[0] * centred[0] + centred[1] * centred[1] + centred[2] * centred[2]
    one = jnp.ones_like(norm)
    rows = []
    for c in centred:
        h, m, l = split3(c)
        if target:
            h, m, l = -2.0 * h, -2.0 * m, -2.0 * l
            rows += [h, h, m, m, h, l]
        else:
            rows += [h, m, h, m, l, h]
    if target:
        rows += [*split3(norm + scale * scale * DELTA_SQ), one, one, one]
    else:
        rows += [one, one, one, *split3(norm)]
    return rows + [jnp.zeros_like(norm)] * (K - len(rows))


def exchange_kernel(
    scale,
    near,
    blk,
    blk_src,
    top,
    top_idx,
    coords,
    charges,
    basis,
    transfers,
    r_blk,
    r_src,
    every,
    top_all,
    top_sum,
    source,
    target,
    partner,
    other,
    partial,
    pool,
    kern,
    gathered,
    sums,
    points,
    half,
    half_src,
    tops,
    r_top,
    r_idx,
    lifted,
    coeffs,
    mine,
    mids,
    part,
    others,
    lines,
    send,
    recv,
    local,
    leave,
):
    me = lax.axis_index(AXIS)
    plane, place = me // GROUP, me % GROUP
    core, y = place % 2, place // 2
    held = pool.at[pl.ds(0, LEAVES)]
    fetch = pltpu.make_async_copy(charges, held, local.at[0])
    fetch.start()
    barrier = pltpu.get_barrier_semaphore()

    across_chip, next_chip = me + 1 - 2 * core, lax.rem(me - 1 + 2 * core + N, N)
    peers = [plane * GROUP + lax.rem(place + o, GROUP) for o in range(1, GROUP)]
    planes = [lax.rem(plane + o, 16) for o in range(1, 16)]
    greeted = [*peers, *[p * GROUP + place for p in planes], next_chip]
    for to in greeted:
        pl.semaphore_signal(barrier, inc=1, device_id=(to,), device_id_type=MESH)
    for i in range(3):
        for l in range(LEAVES):
            points[i, l : l + 1, :] = coords[i : i + 1, l * M : (l + 1) * M]
    pool[2 * LEAVES] = jnp.zeros((M, RHS), bf16)

    pl.semaphore_wait(barrier, len(greeted))

    def remote(src, dst, k, to):
        return pltpu.make_async_remote_copy(
            src_ref=src,
            dst_ref=dst,
            send_sem=send.at[k],
            recv_sem=recv.at[k],
            device_id=(to,),
            device_id_type=MESH,
        )

    def finish(ref, k):
        whole = remote(ref, ref, k, me)
        whole.wait_send()
        whole.wait_recv()

    for to in peers:
        remote(blk.at[to % GROUP], half.at[place], 4, to).start()
        remote(blk_src.at[to % GROUP], half_src.at[place], 5, to).start()
    to_partner = remote(points, others.at[0], 0, across_chip)
    to_other = remote(points, others.at[1], 1, next_chip)
    to_partner.start()
    to_other.start()
    swap = remote(charges, pool.at[pl.ds(LEAVES, LEAVES)], 12, across_chip)
    swap.start()
    for p in planes:
        to = p * GROUP + place
        remote(top, r_top.at[plane], 2, to).start()
        remote(top_idx, r_idx.at[plane], 3, to).start()
    piece = pl.ds(0, 16)
    remote(charges.at[piece], other.at[piece], 13, next_chip).start()

    fetch.wait()

    def one_mid(m, c):
        rows = []
        for b in range(GROUP):
            rows.append(dot(basis[m * GROUP + b], pool[m * GROUP + b]).astype(bf16))
        first = pl.multiple_of(m * GROUP * K, GROUP * K)
        rows = dot_t(transfers[pl.ds(first, GROUP * K), :], jnp.concatenate(rows, axis=0))
        mids[pl.ds(pl.multiple_of(m * K, K), K), :] = rows.astype(bf16)
        return c

    lax.fori_loop(0, GROUP, one_mid, 0)
    base = dot_t(transfers[LEAVES * K : LEAVES * K + GROUP * K, :], mids[...]).astype(bf16)
    coeffs[0] = base
    coeffs[1] = dot_t(transfers[LEAVES * K + GROUP * K :, :], base).astype(bf16)
    for o in range(1, 4):
        to = plane * GROUP + lax.rem(y + o, 4) * 2 + core
        remote(coeffs.at[0], every.at[core, plane, y], 6, to).start()
    for to in peers:
        remote(coeffs.at[1], lifted.at[place], 7, to).start()
    piece = pl.ds(16, LEAVES - 16)
    remote(charges.at[piece], other.at[piece], 13, next_chip).start()
    own = [
        pltpu.make_async_copy(blk.at[place], half.at[place], local.at[1]),
        pltpu.make_async_copy(blk_src.at[place], half_src.at[place], local.at[2]),
        pltpu.make_async_copy(top, r_top.at[plane], local.at[3]),
        pltpu.make_async_copy(top_idx, r_idx.at[plane], local.at[4]),
        pltpu.make_async_copy(coeffs.at[0], every.at[core, plane, y], local.at[5]),
        pltpu.make_async_copy(coeffs.at[1], lifted.at[place], local.at[6]),
    ]
    for copy in own:
        copy.start()

    def side(rows, put, count):
        for r, row in enumerate(rows):
            lines[pl.ds(r, LEAVES, stride=K), :] = row
        lax.fori_loop(0, count, put, 0, unroll=4)

    def line(l):
        return lines[pl.ds(pl.multiple_of(l * K, K), K), :]

    def put_target(l, c):
        target[l] = line(l).astype(bf16)
        return c

    def put_source(block):
        def put(l, c):
            source[block * LEAVES + l] = line(l).astype(bf16)
            return c

        return put

    here = [points[i] for i in range(3)]
    side(features(scale, here, True), put_target, LEAVES)
    for copy in own:
        copy.wait()
    finish(lifted.at[pl.ds(0, 3)], 6)
    for p in planes:
        to = p * GROUP + place
        remote(every.at[core, plane], every.at[core, plane], 8, to).start()
    finish(lifted.at[pl.ds(0, GROUP - 1)], 7)
    mine[...] = jnp.sum(lifted[...].astype(f32), axis=0).astype(bf16)
    for p in planes:
        remote(mine, top_all.at[plane], 9, p * GROUP + place).start()
    own_top = pltpu.make_async_copy(mine, top_all.at[plane], local.at[0])
    own_top.start()
    side(features(scale, here, False), put_source(0), LEAVES)
    own_top.wait()

    finish(half.at[pl.ds(0, GROUP - 1)], 4)
    finish(half_src.at[pl.ds(0, GROUP - 1)], 5)
    for p in planes:
        to = p * GROUP + place
        remote(half.at[:, p], r_blk.at[plane], 14, to).start()
        remote(half_src.at[:, p], r_src.at[plane], 15, to).start()
    own = [
        pltpu.make_async_copy(half.at[:, plane], r_blk.at[plane], local.at[2]),
        pltpu.make_async_copy(half_src.at[:, plane], r_src.at[plane], local.at[3]),
    ]
    for copy in own:
        copy.start()
    to_partner.wait()
    to_other.wait()
    spare = source[0]
    for l in range(8):
        source[POOL + l] = spare
    for i in range(2):
        side(features(scale, [others[i, j] for j in range(3)], False), put_source(i + 1), LEAVES)

    swap.wait()
    keep = pltpu.make_async_copy(pool.at[pl.ds(LEAVES, LEAVES)], partner, local.at[1])
    keep.start()

    def close_group(group, c):
        for b in range(GROUP):
            leaf = group * GROUP + b
            mine_t = target[leaf].T
            for j in range(HALF // 2):
                one, two = near[leaf, 2 * j], near[leaf, 2 * j + 1]
                kernel_rows(b, mine_t, one, two, j, source, kern)
                charge_rows(b, one, two, j, pool, gathered, 2 * LEAVES)
            sums[leaf] = dot(kern[b], gathered[b])
        return c

    def close_half(k):
        lax.fori_loop(2 * k, 2 * k + 2, close_group, 0)
        done = pl.ds(2 * k * GROUP, 2 * GROUP)
        pltpu.make_async_copy(sums.at[done], partial.at[done], leave).start()

    close_half(0)

    finish(r_top.at[pl.ds(0, 15)], 2)
    finish(r_idx.at[pl.ds(0, 15)], 3)
    named = jnp.sum(r_idx[...], axis=0)
    wanted = plane * 16 + lax.broadcasted_iota(jnp.int32, (16, N), 0)
    chosen = jnp.where(wanted == named, 1.0, 0.0).astype(bf16)
    part[...] = dot(chosen, r_top[...].reshape(N, K * K)).astype(bf16)
    for to in peers:
        remote(part, tops.at[place], 10, to).start()
    own_part = pltpu.make_async_copy(part, tops.at[place], local.at[0])
    own_part.start()

    close_half(1)
    finish(every.at[0, pl.ds(0, 15)], 8)
    across = remote(every.at[core], every.at[core], 11, across_chip)
    across.start()
    close_half(2)
    own_part.wait()
    finish(tops.at[pl.ds(0, GROUP - 1)], 10)
    top_sum[...] = jnp.sum(tops[...].astype(f32), axis=0)
    close_half(3)
    away = pltpu.make_async_copy(sums, partial, leave)
    finish(top_all.at[pl.ds(0, 15)], 9)
    across.wait()
    for copy in own:
        copy.wait()
    finish(r_blk.at[pl.ds(0, 15)], 14)
    finish(r_src.at[pl.ds(0, 15)], 15)
    keep.wait()
    away.wait()
    finish(other, 13)


def exchange_call(near, blk, blk_src, top, top_idx, coords, charges, basis, transfers):
    inside = pl.BlockSpec(memory_space=pltpu.VMEM)
    anywhere = pl.BlockSpec(memory_space=pl.ANY)
    shape = jax.ShapeDtypeStruct
    return pl.pallas_call(
        functools.partial(exchange_kernel, math.sqrt(NNEAR * M)),
        out_shape=(
            shape((16, GROUP, *blk.shape[2:]), bf16),
            shape((16, GROUP, *blk_src.shape[2:]), jnp.int32),
            shape((2, 16, 4, K, RHS), bf16),
            shape((16, K, RHS), bf16),
            shape((16, K * K), f32),
            shape((POOL + 8, K, M), bf16),
            shape((LEAVES, K, M), bf16),
            shape((LEAVES, M, RHS), bf16),
            shape((LEAVES, M, RHS), bf16),
            shape((LEAVES, M, RHS), f32),
        ),
        in_specs=[
            pl.BlockSpec(memory_space=pltpu.SMEM),
            *[inside] * 5,
            anywhere,
            inside,
            inside,
        ],
        out_specs=(*[inside] * 7, *[anywhere] * 3),
        scratch_shapes=[
            pltpu.VMEM((2 * LEAVES + 1, M, RHS), bf16),
            pltpu.VMEM((GROUP, M, M * HALF), bf16),
            pltpu.VMEM((GROUP, M * HALF, RHS), bf16),
            pltpu.VMEM((LEAVES, M, RHS), f32),
            pltpu.VMEM((3, LEAVES, M), f32),
            pltpu.VMEM(blk.shape, bf16),
            pltpu.VMEM(blk_src.shape, jnp.int32),
            pltpu.VMEM((GROUP, 16, K * K), bf16),
            pltpu.VMEM((16, 8, K * K), bf16),
            pltpu.VMEM((16, 1, N), jnp.int32),
            pltpu.VMEM((GROUP, K, RHS), bf16),
            pltpu.VMEM((2, K, RHS), bf16),
            pltpu.VMEM((K, RHS), bf16),
            pltpu.VMEM((GROUP * K, RHS), bf16),
            pltpu.VMEM((16, K * K), bf16),
            pltpu.VMEM((2, 3, LEAVES, M), f32),
            pltpu.VMEM((LEAVES * K, M), f32),
            pltpu.SemaphoreType.DMA((16,)),
            pltpu.SemaphoreType.DMA((16,)),
            pltpu.SemaphoreType.DMA((7,)),
            pltpu.SemaphoreType.DMA,
        ],
        compiler_params=pltpu.CompilerParams(
            collective_id=0, has_side_effects=True, vmem_limit_bytes=63 * 1024 * 1024
        ),
        cost_estimate=pl.CostEstimate(flops=10**9, bytes_accessed=10**7, transcendentals=0),
        name="exchange",
    )(near, blk, blk_src, top, top_idx, coords, charges, basis, transfers)


def kernel_rows(slot, mine, one, two, j, source, kern):
    squares = dot(mine, jnp.concatenate([source[one], source[two]], axis=1))
    kern[slot, :, 2 * M * j : 2 * M * (j + 1)] = lax.rsqrt(squares.astype(bf16))


def charge_rows(slot, one, two, j, pool, gathered, last):
    gathered[slot, 2 * M * j : 2 * M * j + M] = pool[jnp.minimum(one, last)]
    gathered[slot, 2 * M * j + M : 2 * M * (j + 1)] = pool[jnp.minimum(two, last)]


def load_pool(refs, pool, sems):
    copies = [
        pltpu.make_async_copy(ref, pool.at[pl.ds(LEAVES * i, LEAVES)], sems.at[i])
        for i, ref in enumerate(refs)
    ]
    for copy in copies:
        copy.start()
    pool[POOL] = jnp.zeros((M, RHS), bf16)
    return copies


def near_kernel(
    near,
    source,
    target,
    here,
    partner,
    other,
    partial,
    a_high,
    a_low,
    every,
    t_high,
    t_low,
    top_all,
    transfers,
    basis,
    out,
    pool,
    kern,
    gathered,
    base,
    extra,
    sems,
):
    step = pl.program_id(0)

    def entries(b):
        leaf = step * GROUP + b
        return [
            (near[leaf, HALF + 2 * j], near[leaf, HALF + 2 * j + 1], j)
            for j in range(HALF // 2)
        ]

    def fill(b):
        mine = target[b].T
        for one, two, j in entries(b):
            kernel_rows(b, mine, one, two, j, source, kern)

    @pl.when(step == 0)
    def _():
        copies = load_pool((here, partner, other), pool, sems)
        for b in range(GROUP):
            fill(b)
        extra[...] = jnp.zeros_like(extra)
        top_field = (dot(t_high[...], top_all[...]) + dot(t_low[...], top_all[...])).astype(bf16)
        coupled = dot(a_high[...], every[...]) + dot(a_low[...], every[...])
        base[...] = (coupled + dot(transfers[(LEAVES + GROUP) * K :, :], top_field)).astype(bf16)
        for copy in copies:
            copy.wait()

        @pl.when(near[0, 2 * HALF + 1] > 0)
        def _():
            pool[pl.ds(2 * LEAVES, LEAVES)] = jnp.zeros((LEAVES, M, RHS), bf16)

    late = jnp.int32(0)
    for b in range(GROUP):
        late += HALF - near[step * GROUP + b, 2 * HALF]

    @pl.when(late > 0)
    def _():
        def one_leaf(b, c):
            leaf = step * GROUP + b

            def one_entry(e, total):
                g = near[leaf, e]
                squares = dot_t(target[b], source[g])
                return total + dot(lax.rsqrt(squares.astype(bf16)), pool[g])

            extra[b] = lax.fori_loop(
                near[leaf, 2 * HALF], HALF, one_entry, jnp.zeros((M, RHS), f32)
            )
            return c

        lax.fori_loop(0, GROUP, one_leaf, 0)

    def group(filled):
        down = transfers[pl.ds(pl.multiple_of((LEAVES + step) * K, K), K), :]
        mid = dot(down, base[...]).astype(bf16)
        down = transfers[pl.ds(pl.multiple_of(step * GROUP * K, GROUP * K), GROUP * K), :]
        fields = dot(down, mid).astype(bf16)
        for b in range(GROUP):
            if not filled:
                fill(b)
            for one, two, j in entries(b):
                charge_rows(b, one, two, j, pool, gathered, POOL)
            far = dot_t(basis[b], fields[b * K : (b + 1) * K])
            total = dot(kern[b], gathered[b]) + far + (partial[b] + extra[b])
            out[pl.ds(b * M, M), :] = total.astype(bf16)

    pl.when(step == 0)(lambda: group(True))
    pl.when(step > 0)(lambda: group(False))

    @pl.when(late > 0)
    def _():
        extra[...] = jnp.zeros_like(extra)


def near_scratch():
    return [
        pltpu.VMEM((POOL + 1, M, RHS), bf16),
        pltpu.VMEM((GROUP, M, M * HALF), bf16),
        pltpu.VMEM((GROUP, M * HALF, RHS), bf16),
    ]


NEAR_PARAMS = dict(
    compiler_params=pltpu.CompilerParams(
        vmem_limit_bytes=63 * 1024 * 1024, dimension_semantics=("arbitrary",)
    ),
    cost_estimate=pl.CostEstimate(
        flops=5 * 10**9, bytes_accessed=10**7, transcendentals=10**7
    ),
)


def near_call(near, source, target, here, partner, other, partial, far, transfers, basis):
    anywhere = pl.BlockSpec(memory_space=pl.ANY)
    grid_spec = pltpu.PrefetchScalarGridSpec(
        num_scalar_prefetch=1,
        grid=(LEAVES // GROUP,),
        in_specs=[
            vmem(*source.shape),
            pl.BlockSpec((GROUP, K, M), lambda i, _: (i, 0, 0)),
            anywhere,
            anywhere,
            anywhere,
            pl.BlockSpec((GROUP, M, RHS), lambda i, _: (i, 0, 0)),
            *[vmem(*v.shape) for v in far],
            vmem(*transfers.shape),
            pl.BlockSpec((GROUP, K, M), lambda i, _: (i, 0, 0)),
        ],
        out_specs=pl.BlockSpec((GROUP * M, RHS), lambda i, _: (i, 0)),
        scratch_shapes=[
            *near_scratch(),
            pltpu.VMEM((K, RHS), bf16),
            pltpu.VMEM((GROUP, M, RHS), f32),
            pltpu.SemaphoreType.DMA((3,)),
        ],
    )
    return pl.pallas_call(
        near_kernel,
        grid_spec=grid_spec,
        out_shape=jax.ShapeDtypeStruct((LEAVES * M, RHS), bf16),
        name="near",
        **NEAR_PARAMS,
    )(near, source, target, here, partner, other, partial, *far, transfers, basis)


def near_lists(near_leaves, core, edge):
    block, inside = near_leaves // LEAVES, near_leaves % LEAVES
    moved = jnp.where(block == 1, 0, jnp.where((block == 0) == (core == 0), 2, 1))
    place = moved * LEAVES + inside
    away = place >= 2 * LEAVES
    column = jnp.arange(NNEAR)
    key = jnp.where(away, NNEAR, 0) + column
    rank = jnp.sum(key[:, None, :] < key[:, :, None], axis=2)
    ordered = jnp.sum(
        jnp.where(rank[:, :, None] == jnp.arange(2 * HALF), place[:, :, None] + 1, 0), axis=1
    )
    ordered = jnp.where(ordered == 0, POOL, ordered - 1)
    ready = jnp.minimum(NNEAR - jnp.sum(away, axis=1, keepdims=True), HALF)
    return jnp.concatenate([ordered, ready, jnp.full_like(ready, edge)], axis=1)


def high_low(v):
    high = v.astype(bf16)
    return high, (v - high.astype(f32)).astype(bf16)


def per_device(
    coords,
    charges,
    near_leaves,
    leaf_basis,
    leaf_transfer,
    mid_transfer,
    base_transfer,
    base_coupling,
    base_target,
    base_source,
    top_coupling,
    top_target,
    top_source,
):
    me = lax.axis_index(AXIS)
    rows = charges.reshape(LEAVES, M, RHS)
    targets = base_target[:, 0]
    count = targets.shape[0]
    earlier = jnp.arange(count)[:, None] > jnp.arange(count)[None, :]
    rank = jnp.sum((targets[:, None] == targets[None, :]) & earlier, axis=1)
    slots = jnp.arange(2 * N)
    places = (targets % GROUP) * 16 + targets // GROUP
    chosen = (slots[:, None] == (2 * places + rank)[None, :]).astype(bf16)
    blk = dot(chosen, base_coupling).astype(bf16).reshape(GROUP, 16, 16, 128)
    order = (base_source % 2) * 64 + (base_source // 8) * 4 + (base_source // 2) % 4
    slot_source = jnp.sum(chosen.astype(jnp.int32) * (order + 1)[None, :], axis=1) - 1
    blk_src = jnp.pad(slot_source.reshape(GROUP, 16, 1, 2), ((0, 0),) * 3 + ((0, 126),))
    lane = jnp.arange(N)
    top_idx = jnp.tile(top_target * 16 + top_source, 16)
    top_idx = jnp.where(lane // 8 == me // GROUP, top_idx, 0).reshape(1, N)

    basis = leaf_basis.reshape(LEAVES, K, M)
    transfers = jnp.concatenate([leaf_transfer, mid_transfer, base_transfer], axis=0)
    transfers = transfers.reshape((LEAVES + GROUP + 1) * K, K)
    edge = ((me == 0) | (me == N - 1)).astype(jnp.int32)
    near = near_lists(near_leaves, me % 2, edge)
    r_blk, r_src, every, top_all, t, source, target, partner, other, partial = exchange_call(
        near, blk, blk_src, top_coupling, top_idx, coords, rows, basis, transfers
    )
    by_source = (lane[:, None] == r_src[:, :, 0, :2].reshape(1, 2 * N)).astype(bf16)
    a = dot(by_source, r_blk.reshape(2 * N, K * K))
    a = a.reshape(N, K, K).transpose(1, 0, 2).reshape(K, N * K)
    t = t.reshape(16, K, K).transpose(1, 0, 2).reshape(K, 16 * K)
    far = (
        *high_low(a),
        every.reshape(N * K, RHS),
        *high_low(t),
        top_all.reshape(16 * K, RHS),
    )
    return near_call(
        near, source, target, rows, partner, other, partial, far, transfers, basis
    )


def solution(mesh):
    lead = P(AXIS, None)
    in_specs = (
        P(None, AXIS),
        lead,
        lead,
        lead,
        lead,
        lead,
        lead,
        lead,
        lead,
        P(AXIS),
        lead,
        P(AXIS),
        P(AXIS),
    )
    return jax.shard_map(
        per_device, mesh=mesh, in_specs=in_specs, out_specs=lead, check_vma=False
    )
```

```python
import functools
import math

import jax
import jax.numpy as jnp
from jax import lax
from jax.experimental import pallas as pl
from jax.experimental.pallas import tpu as pltpu
from jax.sharding import PartitionSpec as P

K = 32
RHS = 128
M = 128
N = 128
LEAVES = 64
POOL = 3 * LEAVES
NNEAR = 27
HALF = (NNEAR + 1) // 2
GROUP = 8
DELTA_SQ = 0.0025
AXIS = "leaf"
MESH = pl.DeviceIdType.MESH
bf16 = jnp.bfloat16
f32 = jnp.float32


def dot(a, b):
    return jnp.dot(a, b, preferred_element_type=f32)


def dot_t(a, b):
    return lax.dot_general(a, b, (((0,), (0,)), ((), ())), preferred_element_type=f32)


def vmem(*shape):
    return pl.BlockSpec(shape, lambda *_: (0,) * len(shape))


def split3(v):
    high = v.astype(bf16).astype(f32)
    rest = v - high
    mid = rest.astype(bf16).astype(f32)
    return high, mid, rest - mid


def features(scale, points, target):
    centred = [(p - 0.5) * scale for p in points]
    norm = centred[0] * centred[0] + centred[1] * centred[1] + centred[2] * centred[2]
    one = jnp.ones_like(norm)
    rows = []
    for c in centred:
        h, m, l = split3(c)
        if target:
            h, m, l = -2.0 * h, -2.0 * m, -2.0 * l
            rows += [h, h, m, m, h, l]
        else:
            rows += [h, m, h, m, l, h]
    if target:
        rows += [*split3(norm + scale * scale * DELTA_SQ), one, one, one]
    else:
        rows += [one, one, one, *split3(norm)]
    return rows + [jnp.zeros_like(norm)] * (K - len(rows))


def exchange_kernel(
    scale,
    blk,
    blk_src,
    top,
    top_idx,
    coords,
    charges,
    basis,
    transfers,
    r_blk,
    r_src,
    every,
    top_all,
    top_sum,
    source,
    target,
    partner,
    held,
    points,
    half,
    half_src,
    tops,
    r_top,
    r_idx,
    lifted,
    coeffs,
    mine,
    mids,
    part,
    others,
    lines,
    send,
    recv,
    local,
):
    me = lax.axis_index(AXIS)
    plane, place = me // GROUP, me % GROUP
    core, y = place % 2, place // 2
    fetch = pltpu.make_async_copy(charges, held, local.at[0])
    fetch.start()
    barrier = pltpu.get_barrier_semaphore()

    across_chip, next_chip = me + 1 - 2 * core, lax.rem(me - 1 + 2 * core + N, N)
    peers = [plane * GROUP + lax.rem(place + o, GROUP) for o in range(1, GROUP)]
    planes = [lax.rem(plane + o, 16) for o in range(1, 16)]
    greeted = [*peers, *[p * GROUP + place for p in planes], next_chip]
    for to in greeted:
        pl.semaphore_signal(barrier, inc=1, device_id=(to,), device_id_type=MESH)
    for i in range(3):
        for l in range(LEAVES):
            points[i, l : l + 1, :] = coords[i : i + 1, l * M : (l + 1) * M]

    fetch.wait()

    def one_mid(m, c):
        rows = []
        for b in range(GROUP):
            rows.append(dot(basis[m * GROUP + b], held[m * GROUP + b]).astype(bf16))
        first = pl.multiple_of(m * GROUP * K, GROUP * K)
        rows = dot_t(transfers[pl.ds(first, GROUP * K), :], jnp.concatenate(rows, axis=0))
        mids[pl.ds(pl.multiple_of(m * K, K), K), :] = rows.astype(bf16)
        return c

    lax.fori_loop(0, GROUP, one_mid, 0)
    base = dot_t(transfers[LEAVES * K : LEAVES * K + GROUP * K, :], mids[...]).astype(bf16)
    coeffs[0] = base
    coeffs[1] = dot_t(transfers[LEAVES * K + GROUP * K :, :], base).astype(bf16)
    pl.semaphore_wait(barrier, len(greeted))

    def remote(src, dst, k, to):
        return pltpu.make_async_remote_copy(
            src_ref=src,
            dst_ref=dst,
            send_sem=send.at[k],
            recv_sem=recv.at[k],
            device_id=(to,),
            device_id_type=MESH,
        )

    def finish(ref, k):
        whole = remote(ref, ref, k, me)
        whole.wait_send()
        whole.wait_recv()

    for o in range(1, 4):
        to = plane * GROUP + lax.rem(y + o, 4) * 2 + core
        remote(coeffs.at[0], every.at[core, plane, y], 6, to).start()
    for to in peers:
        remote(coeffs.at[1], lifted.at[place], 7, to).start()
    for to in peers:
        remote(blk.at[to % GROUP], half.at[place], 4, to).start()
        remote(blk_src.at[to % GROUP], half_src.at[place], 5, to).start()
    to_partner = remote(points, others.at[0], 0, across_chip)
    to_other = remote(points, others.at[1], 1, next_chip)
    to_partner.start()
    to_other.start()
    swap = remote(held, partner, 12, across_chip)
    swap.start()
    for p in planes:
        to = p * GROUP + place
        remote(top, r_top.at[plane], 2, to).start()
        remote(top_idx, r_idx.at[plane], 3, to).start()
    own = [
        pltpu.make_async_copy(blk.at[place], half.at[place], local.at[1]),
        pltpu.make_async_copy(blk_src.at[place], half_src.at[place], local.at[2]),
        pltpu.make_async_copy(top, r_top.at[plane], local.at[3]),
        pltpu.make_async_copy(top_idx, r_idx.at[plane], local.at[4]),
        pltpu.make_async_copy(coeffs.at[0], every.at[core, plane, y], local.at[5]),
        pltpu.make_async_copy(coeffs.at[1], lifted.at[place], local.at[6]),
    ]
    for copy in own:
        copy.start()

    def side(rows, put, count):
        for r, row in enumerate(rows):
            lines[pl.ds(r, LEAVES, stride=K), :] = row
        lax.fori_loop(0, count, put, 0, unroll=4)

    def line(l):
        return lines[pl.ds(pl.multiple_of(l * K, K), K), :]

    def put_target(l, c):
        target[l] = line(l).astype(bf16)
        return c

    def put_source(block):
        def put(l, c):
            source[block * LEAVES + l] = line(l).astype(bf16)
            return c

        return put

    here = [points[i] for i in range(3)]
    side(features(scale, here, True), put_target, LEAVES)
    for copy in own:
        copy.wait()
    finish(lifted.at[pl.ds(0, 3)], 6)
    for p in planes:
        to = p * GROUP + place
        remote(every.at[core, plane], every.at[core, plane], 8, to).start()
    finish(lifted.at[pl.ds(0, GROUP - 1)], 7)
    mine[...] = jnp.sum(lifted[...].astype(f32), axis=0).astype(bf16)
    for p in planes:
        remote(mine, top_all.at[plane], 9, p * GROUP + place).start()
    own_top = pltpu.make_async_copy(mine, top_all.at[plane], local.at[0])
    own_top.start()
    side(features(scale, here, False), put_source(0), LEAVES)
    own_top.wait()

    finish(half.at[pl.ds(0, GROUP - 1)], 4)
    finish(half_src.at[pl.ds(0, GROUP - 1)], 5)
    for p in planes:
        to = p * GROUP + place
        remote(half.at[:, p], r_blk.at[plane], 14, to).start()
        remote(half_src.at[:, p], r_src.at[plane], 15, to).start()
    own = [
        pltpu.make_async_copy(half.at[:, plane], r_blk.at[plane], local.at[2]),
        pltpu.make_async_copy(half_src.at[:, plane], r_src.at[plane], local.at[3]),
    ]
    for copy in own:
        copy.start()
    to_partner.wait()
    to_other.wait()
    spare = source[0]
    for l in range(8):
        source[POOL + l] = spare
    for i in range(2):
        side(features(scale, [others[i, j] for j in range(3)], False), put_source(i + 1), LEAVES)

    finish(r_top.at[pl.ds(0, 15)], 2)
    finish(r_idx.at[pl.ds(0, 15)], 3)
    named = jnp.sum(r_idx[...], axis=0)
    wanted = plane * 16 + lax.broadcasted_iota(jnp.int32, (16, N), 0)
    chosen = jnp.where(wanted == named, 1.0, 0.0).astype(bf16)
    part[...] = dot(chosen, r_top[...].reshape(N, K * K)).astype(bf16)
    for to in peers:
        remote(part, tops.at[place], 10, to).start()
    own_part = pltpu.make_async_copy(part, tops.at[place], local.at[0])
    own_part.start()

    finish(every.at[0, pl.ds(0, 15)], 8)
    across = remote(every.at[core], every.at[core], 11, across_chip)
    across.start()
    own_part.wait()
    finish(tops.at[pl.ds(0, GROUP - 1)], 10)
    top_sum[...] = jnp.sum(tops[...].astype(f32), axis=0)
    finish(top_all.at[pl.ds(0, 15)], 9)
    across.wait()
    for copy in own:
        copy.wait()
    finish(r_blk.at[pl.ds(0, 15)], 14)
    finish(r_src.at[pl.ds(0, 15)], 15)
    swap.wait()


def exchange_call(blk, blk_src, top, top_idx, coords, charges, basis, transfers):
    inside = pl.BlockSpec(memory_space=pltpu.VMEM)
    anywhere = pl.BlockSpec(memory_space=pl.ANY)
    shape = jax.ShapeDtypeStruct
    return pl.pallas_call(
        functools.partial(exchange_kernel, math.sqrt(NNEAR * M)),
        out_shape=(
            shape((16, GROUP, *blk.shape[2:]), bf16),
            shape((16, GROUP, *blk_src.shape[2:]), jnp.int32),
            shape((2, 16, 4, K, RHS), bf16),
            shape((16, K, RHS), bf16),
            shape((16, K * K), f32),
            shape((POOL + 8, K, M), bf16),
            shape((LEAVES, K, M), bf16),
            shape((LEAVES, M, RHS), bf16),
        ),
        in_specs=[
            *[inside] * 5,
            anywhere,
            inside,
            inside,
        ],
        out_specs=(*[inside] * 7, anywhere),
        scratch_shapes=[
            pltpu.VMEM((LEAVES, M, RHS), bf16),
            pltpu.VMEM((3, LEAVES, M), f32),
            pltpu.VMEM(blk.shape, bf16),
            pltpu.VMEM(blk_src.shape, jnp.int32),
            pltpu.VMEM((GROUP, 16, K * K), bf16),
            pltpu.VMEM((16, 8, K * K), bf16),
            pltpu.VMEM((16, 1, N), jnp.int32),
            pltpu.VMEM((GROUP, K, RHS), bf16),
            pltpu.VMEM((2, K, RHS), bf16),
            pltpu.VMEM((K, RHS), bf16),
            pltpu.VMEM((GROUP * K, RHS), bf16),
            pltpu.VMEM((16, K * K), bf16),
            pltpu.VMEM((2, 3, LEAVES, M), f32),
            pltpu.VMEM((LEAVES * K, M), f32),
            pltpu.SemaphoreType.DMA((16,)),
            pltpu.SemaphoreType.DMA((16,)),
            pltpu.SemaphoreType.DMA((7,)),
        ],
        compiler_params=pltpu.CompilerParams(
            collective_id=0, has_side_effects=True, vmem_limit_bytes=63 * 1024 * 1024
        ),
        cost_estimate=pl.CostEstimate(flops=10**9, bytes_accessed=10**7, transcendentals=0),
        name="exchange",
    )(blk, blk_src, top, top_idx, coords, charges, basis, transfers)


def kernel_rows(slot, mine, one, two, j, source, kern):
    squares = dot(mine, jnp.concatenate([source[one], source[two]], axis=1))
    kern[slot, :, 2 * M * j : 2 * M * (j + 1)] = lax.rsqrt(squares.astype(bf16))


def charge_rows(slot, one, two, j, pool, gathered, last):
    gathered[slot, 2 * M * j : 2 * M * j + M] = pool[jnp.minimum(one, last)]
    gathered[slot, 2 * M * j + M : 2 * M * (j + 1)] = pool[jnp.minimum(two, last)]


def load_pool(refs, pool, sems, last):
    copies = [
        pltpu.make_async_copy(ref, pool.at[pl.ds(LEAVES * i, LEAVES)], sems.at[i])
        for i, ref in enumerate(refs)
    ]
    for copy in copies:
        copy.start()
    pool[last] = jnp.zeros((M, RHS), bf16)
    return copies


def close_kernel(near, source, target, here, partner, out, pool, kern, gathered, sems):
    step = pl.program_id(0)

    def entries(b):
        leaf = step * GROUP + b
        return [(near[leaf, 2 * j], near[leaf, 2 * j + 1], j) for j in range(HALF // 2)]

    def fill(b):
        mine = target[b].T
        for one, two, j in entries(b):
            kernel_rows(b, mine, one, two, j, source, kern)

    def group(filled):
        for b in range(GROUP):
            if not filled:
                fill(b)
            for one, two, j in entries(b):
                charge_rows(b, one, two, j, pool, gathered, 2 * LEAVES)
            out[b] = dot(kern[b], gathered[b])

    @pl.when(step == 0)
    def _():
        copies = load_pool((here, partner), pool, sems, 2 * LEAVES)
        for b in range(GROUP):
            fill(b)
        for copy in copies:
            copy.wait()
        group(True)

    pl.when(step > 0)(lambda: group(False))


def near_kernel(
    near,
    source,
    target,
    here,
    partner,
    other,
    partial,
    a_high,
    a_low,
    every,
    t_high,
    t_low,
    top_all,
    transfers,
    basis,
    out,
    pool,
    kern,
    gathered,
    base,
    extra,
    sems,
):
    step = pl.program_id(0)

    def entries(b):
        leaf = step * GROUP + b
        return [
            (near[leaf, HALF + 2 * j], near[leaf, HALF + 2 * j + 1], j)
            for j in range(HALF // 2)
        ]

    def fill(b):
        mine = target[b].T
        for one, two, j in entries(b):
            kernel_rows(b, mine, one, two, j, source, kern)

    @pl.when(step == 0)
    def _():
        copies = load_pool((here, partner, other), pool, sems, POOL)
        for b in range(GROUP):
            fill(b)
        extra[...] = jnp.zeros_like(extra)
        top_field = (dot(t_high[...], top_all[...]) + dot(t_low[...], top_all[...])).astype(bf16)
        coupled = dot(a_high[...], every[...]) + dot(a_low[...], every[...])
        base[...] = (coupled + dot(transfers[(LEAVES + GROUP) * K :, :], top_field)).astype(bf16)
        for copy in copies:
            copy.wait()

    late = jnp.int32(0)
    for b in range(GROUP):
        late += HALF - near[step * GROUP + b, 2 * HALF]

    @pl.when(late > 0)
    def _():
        def one_leaf(b, c):
            leaf = step * GROUP + b

            def one_entry(e, total):
                g = near[leaf, e]
                squares = dot_t(target[b], source[g])
                return total + dot(lax.rsqrt(squares.astype(bf16)), pool[g])

            extra[b] = lax.fori_loop(
                near[leaf, 2 * HALF], HALF, one_entry, jnp.zeros((M, RHS), f32)
            )
            return c

        lax.fori_loop(0, GROUP, one_leaf, 0)

    def group(filled):
        down = transfers[pl.ds(pl.multiple_of((LEAVES + step) * K, K), K), :]
        mid = dot(down, base[...]).astype(bf16)
        down = transfers[pl.ds(pl.multiple_of(step * GROUP * K, GROUP * K), GROUP * K), :]
        fields = dot(down, mid).astype(bf16)
        for b in range(GROUP):
            if not filled:
                fill(b)
            for one, two, j in entries(b):
                charge_rows(b, one, two, j, pool, gathered, POOL)
            far = dot_t(basis[b], fields[b * K : (b + 1) * K])
            total = dot(kern[b], gathered[b]) + far + (partial[b] + extra[b])
            out[pl.ds(b * M, M), :] = total.astype(bf16)

    pl.when(step == 0)(lambda: group(True))
    pl.when(step > 0)(lambda: group(False))

    @pl.when(late > 0)
    def _():
        extra[...] = jnp.zeros_like(extra)


def near_scratch(leaves):
    return [
        pltpu.VMEM((leaves, M, RHS), bf16),
        pltpu.VMEM((GROUP, M, M * HALF), bf16),
        pltpu.VMEM((GROUP, M * HALF, RHS), bf16),
    ]


NEAR_PARAMS = dict(
    compiler_params=pltpu.CompilerParams(
        vmem_limit_bytes=63 * 1024 * 1024, dimension_semantics=("arbitrary",)
    ),
    cost_estimate=pl.CostEstimate(
        flops=5 * 10**9, bytes_accessed=10**7, transcendentals=10**7
    ),
)


def close_call(near, source, target, here, partner):
    anywhere = pl.BlockSpec(memory_space=pl.ANY)
    grid_spec = pltpu.PrefetchScalarGridSpec(
        num_scalar_prefetch=1,
        grid=(LEAVES // GROUP,),
        in_specs=[
            vmem(*source.shape),
            pl.BlockSpec((GROUP, K, M), lambda i, _: (i, 0, 0)),
            anywhere,
            anywhere,
        ],
        out_specs=pl.BlockSpec((GROUP, M, RHS), lambda i, _: (i, 0, 0)),
        scratch_shapes=[*near_scratch(2 * LEAVES + 1), pltpu.SemaphoreType.DMA((2,))],
    )
    return pl.pallas_call(
        close_kernel,
        grid_spec=grid_spec,
        out_shape=jax.ShapeDtypeStruct((LEAVES, M, RHS), f32),
        name="close",
        **NEAR_PARAMS,
    )(near, source, target, here, partner)


def near_call(near, source, target, here, partner, other, partial, far, transfers, basis):
    anywhere = pl.BlockSpec(memory_space=pl.ANY)
    grid_spec = pltpu.PrefetchScalarGridSpec(
        num_scalar_prefetch=1,
        grid=(LEAVES // GROUP,),
        in_specs=[
            vmem(*source.shape),
            pl.BlockSpec((GROUP, K, M), lambda i, _: (i, 0, 0)),
            anywhere,
            anywhere,
            anywhere,
            pl.BlockSpec((GROUP, M, RHS), lambda i, _: (i, 0, 0)),
            *[vmem(*v.shape) for v in far],
            vmem(*transfers.shape),
            pl.BlockSpec((GROUP, K, M), lambda i, _: (i, 0, 0)),
        ],
        out_specs=pl.BlockSpec((GROUP * M, RHS), lambda i, _: (i, 0)),
        scratch_shapes=[
            *near_scratch(POOL + 1),
            pltpu.VMEM((K, RHS), bf16),
            pltpu.VMEM((GROUP, M, RHS), f32),
            pltpu.SemaphoreType.DMA((3,)),
        ],
    )
    return pl.pallas_call(
        near_kernel,
        grid_spec=grid_spec,
        out_shape=jax.ShapeDtypeStruct((LEAVES * M, RHS), bf16),
        name="near",
        **NEAR_PARAMS,
    )(near, source, target, here, partner, other, partial, *far, transfers, basis)


def near_lists(near_leaves, core):
    block, inside = near_leaves // LEAVES, near_leaves % LEAVES
    moved = jnp.where(block == 1, 0, jnp.where((block == 0) == (core == 0), 2, 1))
    place = moved * LEAVES + inside
    away = place >= 2 * LEAVES
    column = jnp.arange(NNEAR)
    key = jnp.where(away, NNEAR, 0) + column
    rank = jnp.sum(key[:, None, :] < key[:, :, None], axis=2)
    ordered = jnp.sum(
        jnp.where(rank[:, :, None] == jnp.arange(2 * HALF), place[:, :, None] + 1, 0), axis=1
    )
    ordered = jnp.where(ordered == 0, POOL, ordered - 1)
    ready = jnp.minimum(NNEAR - jnp.sum(away, axis=1, keepdims=True), HALF)
    return jnp.concatenate([ordered, ready], axis=1)


def high_low(v):
    high = v.astype(bf16)
    return high, (v - high.astype(f32)).astype(bf16)


def per_device(
    coords,
    charges,
    near_leaves,
    leaf_basis,
    leaf_transfer,
    mid_transfer,
    base_transfer,
    base_coupling,
    base_target,
    base_source,
    top_coupling,
    top_target,
    top_source,
):
    me = lax.axis_index(AXIS)
    rows = charges.reshape(LEAVES, M, RHS)
    targets = base_target[:, 0]
    count = targets.shape[0]
    earlier = jnp.arange(count)[:, None] > jnp.arange(count)[None, :]
    rank = jnp.sum((targets[:, None] == targets[None, :]) & earlier, axis=1)
    slots = jnp.arange(2 * N)
    places = (targets % GROUP) * 16 + targets // GROUP
    chosen = (slots[:, None] == (2 * places + rank)[None, :]).astype(bf16)
    blk = dot(chosen, base_coupling).astype(bf16).reshape(GROUP, 16, 16, 128)
    order = (base_source % 2) * 64 + (base_source // 8) * 4 + (base_source // 2) % 4
    slot_source = jnp.sum(chosen.astype(jnp.int32) * (order + 1)[None, :], axis=1) - 1
    blk_src = jnp.pad(slot_source.reshape(GROUP, 16, 1, 2), ((0, 0),) * 3 + ((0, 126),))
    lane = jnp.arange(N)
    top_idx = jnp.tile(top_target * 16 + top_source, 16)
    top_idx = jnp.where(lane // 8 == me // GROUP, top_idx, 0).reshape(1, N)

    basis = leaf_basis.reshape(LEAVES, K, M)
    transfers = jnp.concatenate([leaf_transfer, mid_transfer, base_transfer], axis=0)
    transfers = transfers.reshape((LEAVES + GROUP + 1) * K, K)
    r_blk, r_src, every, top_all, t, source, target, partner = exchange_call(
        blk, blk_src, top_coupling, top_idx, coords, rows, basis, transfers
    )
    outward = [(i, i + 1) for i in range(1, N - 1, 2)] + [(i, i - 1) for i in range(2, N, 2)]
    sent, partner, listed = lax.optimization_barrier((rows, partner, near_leaves))
    other = lax.ppermute(sent, AXIS, outward)
    near = near_lists(listed, me % 2)
    partial = close_call(near, source, target, rows, partner)
    by_source = (lane[:, None] == r_src[:, :, 0, :2].reshape(1, 2 * N)).astype(bf16)
    a = dot(by_source, r_blk.reshape(2 * N, K * K))
    a = a.reshape(N, K, K).transpose(1, 0, 2).reshape(K, N * K)
    t = t.reshape(16, K, K).transpose(1, 0, 2).reshape(K, 16 * K)
    far = (
        *high_low(a),
        every.reshape(N * K, RHS),
        *high_low(t),
        top_all.reshape(16 * K, RHS),
    )
    return near_call(
        near, source, target, rows, partner, other, partial, far, transfers, basis
    )


def solution(mesh):
    lead = P(AXIS, None)
    in_specs = (
        P(None, AXIS),
        lead,
        lead,
        lead,
        lead,
        lead,
        lead,
        lead,
        lead,
        P(AXIS),
        lead,
        P(AXIS),
        P(AXIS),
    )
    return jax.shard_map(
        per_device, mesh=mesh, in_specs=in_specs, out_specs=lead, check_vma=False
    )
```

```python
import functools
import math

import jax
import jax.numpy as jnp
from jax import lax
from jax.experimental import pallas as pl
from jax.experimental.pallas import tpu as pltpu
from jax.sharding import PartitionSpec as P

K = 32
RHS = 128
M = 128
N = 128
LEAVES = 64
POOL = 3 * LEAVES
NNEAR = 27
HALF = (NNEAR + 1) // 2
GROUP = 8
DELTA_SQ = 0.0025
AXIS = "leaf"
MESH = pl.DeviceIdType.MESH
bf16 = jnp.bfloat16
f32 = jnp.float32


def dot(a, b):
    return jnp.dot(a, b, preferred_element_type=f32)


def dot_t(a, b):
    return lax.dot_general(a, b, (((0,), (0,)), ((), ())), preferred_element_type=f32)


def vmem(*shape):
    return pl.BlockSpec(shape, lambda *_: (0,) * len(shape))


def split3(v):
    high = v.astype(bf16).astype(f32)
    rest = v - high
    mid = rest.astype(bf16).astype(f32)
    return high, mid, rest - mid


def features(scale, points, target):
    centred = [(p - 0.5) * scale for p in points]
    norm = centred[0] * centred[0] + centred[1] * centred[1] + centred[2] * centred[2]
    one = jnp.ones_like(norm)
    rows = []
    for c in centred:
        h, m, l = split3(c)
        if target:
            h, m, l = -2.0 * h, -2.0 * m, -2.0 * l
            rows += [h, h, m, m, h, l]
        else:
            rows += [h, m, h, m, l, h]
    if target:
        rows += [*split3(norm + scale * scale * DELTA_SQ), one, one, one]
    else:
        rows += [one, one, one, *split3(norm)]
    return rows


def exchange_kernel(
    scale,
    blk,
    blk_src,
    top,
    top_idx,
    coords,
    charges,
    basis,
    transfers,
    r_blk,
    r_src,
    every,
    top_all,
    top_sum,
    source,
    target,
    partner,
    held,
    points,
    half,
    half_src,
    tops,
    r_top,
    r_idx,
    lifted,
    coeffs,
    mine,
    mids,
    part,
    others,
    lines,
    send,
    recv,
    local,
):
    me = lax.axis_index(AXIS)
    plane, place = me // GROUP, me % GROUP
    core, y = place % 2, place // 2
    fetch = pltpu.make_async_copy(charges, held, local.at[0])
    fetch.start()
    barrier = pltpu.get_barrier_semaphore()

    across_chip, next_chip = me + 1 - 2 * core, lax.rem(me - 1 + 2 * core + N, N)
    peers = [plane * GROUP + lax.rem(place + o, GROUP) for o in range(1, GROUP)]
    planes = [lax.rem(plane + o, 16) for o in range(1, 16)]
    greeted = [*peers, *[p * GROUP + place for p in planes], next_chip]
    for to in greeted:
        pl.semaphore_signal(barrier, inc=1, device_id=(to,), device_id_type=MESH)
    for i in range(3):
        for l in range(LEAVES):
            points[i, l : l + 1, :] = coords[i : i + 1, l * M : (l + 1) * M]

    lines[...] = jnp.zeros_like(lines)

    fetch.wait()

    def one_mid(m, c):
        rows = []
        for b in range(GROUP):
            rows.append(dot(basis[m * GROUP + b], held[m * GROUP + b]).astype(bf16))
        first = pl.multiple_of(m * GROUP * K, GROUP * K)
        rows = dot_t(transfers[pl.ds(first, GROUP * K), :], jnp.concatenate(rows, axis=0))
        mids[pl.ds(pl.multiple_of(m * K, K), K), :] = rows.astype(bf16)
        return c

    lax.fori_loop(0, GROUP, one_mid, 0, unroll=2)
    base = dot_t(transfers[LEAVES * K : LEAVES * K + GROUP * K, :], mids[...]).astype(bf16)
    coeffs[0] = base
    coeffs[1] = dot_t(transfers[LEAVES * K + GROUP * K :, :], base).astype(bf16)
    pl.semaphore_wait(barrier, len(greeted))

    def remote(src, dst, k, to):
        return pltpu.make_async_remote_copy(
            src_ref=src,
            dst_ref=dst,
            send_sem=send.at[k],
            recv_sem=recv.at[k],
            device_id=(to,),
            device_id_type=MESH,
        )

    def finish(ref, k):
        whole = remote(ref, ref, k, me)
        whole.wait_send()
        whole.wait_recv()

    for o in range(1, 4):
        to = plane * GROUP + lax.rem(y + o, 4) * 2 + core
        remote(coeffs.at[0], every.at[core, plane, y], 6, to).start()
    for to in peers:
        remote(coeffs.at[1], lifted.at[place], 7, to).start()
    for to in peers:
        remote(blk.at[to % GROUP], half.at[place], 4, to).start()
        remote(blk_src.at[to % GROUP], half_src.at[place], 5, to).start()
    to_partner = remote(points, others.at[0], 0, across_chip)
    to_other = remote(points, others.at[1], 1, next_chip)
    to_partner.start()
    to_other.start()
    swap = remote(held, partner, 12, across_chip)
    swap.start()
    for p in planes:
        to = p * GROUP + place
        remote(top, r_top.at[plane], 2, to).start()
        remote(top_idx, r_idx.at[plane], 3, to).start()
    own = [
        pltpu.make_async_copy(blk.at[place], half.at[place], local.at[1]),
        pltpu.make_async_copy(blk_src.at[place], half_src.at[place], local.at[2]),
        pltpu.make_async_copy(top, r_top.at[plane], local.at[3]),
        pltpu.make_async_copy(top_idx, r_idx.at[plane], local.at[4]),
        pltpu.make_async_copy(coeffs.at[0], every.at[core, plane, y], local.at[5]),
        pltpu.make_async_copy(coeffs.at[1], lifted.at[place], local.at[6]),
    ]
    for copy in own:
        copy.start()

    def side(rows, put, count):
        for r, row in enumerate(rows):
            lines[pl.ds(r, LEAVES, stride=K), :] = row
        lax.fori_loop(0, count, put, 0, unroll=4)

    def line(l):
        return lines[pl.ds(pl.multiple_of(l * K, K), K), :]

    def put_target(l, c):
        target[l] = line(l).T.astype(bf16)
        return c

    def put_source(block):
        def put(l, c):
            source[block * LEAVES + l] = line(l).astype(bf16)
            return c

        return put

    here = [points[i] for i in range(3)]
    side(features(scale, here, True), put_target, LEAVES)
    for copy in own:
        copy.wait()
    finish(lifted.at[pl.ds(0, 3)], 6)
    for p in planes:
        to = p * GROUP + place
        remote(every.at[core, plane], every.at[core, plane], 8, to).start()
    finish(lifted.at[pl.ds(0, GROUP - 1)], 7)
    mine[...] = jnp.sum(lifted[...].astype(f32), axis=0).astype(bf16)
    for p in planes:
        remote(mine, top_all.at[plane], 9, p * GROUP + place).start()
    own_top = pltpu.make_async_copy(mine, top_all.at[plane], local.at[0])
    own_top.start()
    side(features(scale, here, False), put_source(0), LEAVES)
    own_top.wait()

    finish(half.at[pl.ds(0, GROUP - 1)], 4)
    finish(half_src.at[pl.ds(0, GROUP - 1)], 5)
    for p in planes:
        to = p * GROUP + place
        remote(half.at[:, p], r_blk.at[plane], 14, to).start()
        remote(half_src.at[:, p], r_src.at[plane], 15, to).start()
    own = [
        pltpu.make_async_copy(half.at[:, plane], r_blk.at[plane], local.at[2]),
        pltpu.make_async_copy(half_src.at[:, plane], r_src.at[plane], local.at[3]),
    ]
    for copy in own:
        copy.start()
    to_partner.wait()
    to_other.wait()
    spare = source[0]
    for l in range(8):
        source[POOL + l] = spare
    for i in range(2):
        side(features(scale, [others[i, j] for j in range(3)], False), put_source(i + 1), LEAVES)

    finish(r_top.at[pl.ds(0, 15)], 2)
    finish(r_idx.at[pl.ds(0, 15)], 3)
    named = jnp.sum(r_idx[...], axis=0)
    wanted = plane * 16 + lax.broadcasted_iota(jnp.int32, (16, N), 0)
    chosen = jnp.where(wanted == named, 1.0, 0.0).astype(bf16)
    part[...] = dot(chosen, r_top[...].reshape(N, K * K)).astype(bf16)
    for to in peers:
        remote(part, tops.at[place], 10, to).start()
    own_part = pltpu.make_async_copy(part, tops.at[place], local.at[0])
    own_part.start()

    finish(every.at[0, pl.ds(0, 15)], 8)
    across = remote(every.at[core], every.at[core], 11, across_chip)
    across.start()
    own_part.wait()
    finish(tops.at[pl.ds(0, GROUP - 1)], 10)
    top_sum[...] = jnp.sum(tops[...].astype(f32), axis=0)
    finish(top_all.at[pl.ds(0, 15)], 9)
    across.wait()
    for copy in own:
        copy.wait()
    finish(r_blk.at[pl.ds(0, 15)], 14)
    finish(r_src.at[pl.ds(0, 15)], 15)
    swap.wait()


def exchange_call(blk, blk_src, top, top_idx, coords, charges, basis, transfers):
    inside = pl.BlockSpec(memory_space=pltpu.VMEM)
    anywhere = pl.BlockSpec(memory_space=pl.ANY)
    shape = jax.ShapeDtypeStruct
    return pl.pallas_call(
        functools.partial(exchange_kernel, math.sqrt(NNEAR * M)),
        out_shape=(
            shape((16, GROUP, *blk.shape[2:]), bf16),
            shape((16, GROUP, *blk_src.shape[2:]), jnp.int32),
            shape((2, 16, 4, K, RHS), bf16),
            shape((16, K, RHS), bf16),
            shape((16, K * K), f32),
            shape((POOL + 8, K, M), bf16),
            shape((LEAVES, M, K), bf16),
            shape((LEAVES, M, RHS), bf16),
        ),
        in_specs=[
            *[inside] * 5,
            anywhere,
            inside,
            inside,
        ],
        out_specs=(*[inside] * 7, anywhere),
        scratch_shapes=[
            pltpu.VMEM((LEAVES, M, RHS), bf16),
            pltpu.VMEM((3, LEAVES, M), f32),
            pltpu.VMEM(blk.shape, bf16),
            pltpu.VMEM(blk_src.shape, jnp.int32),
            pltpu.VMEM((GROUP, 16, K * K), bf16),
            pltpu.VMEM((16, 8, K * K), bf16),
            pltpu.VMEM((16, 1, N), jnp.int32),
            pltpu.VMEM((GROUP, K, RHS), bf16),
            pltpu.VMEM((2, K, RHS), bf16),
            pltpu.VMEM((K, RHS), bf16),
            pltpu.VMEM((GROUP * K, RHS), bf16),
            pltpu.VMEM((16, K * K), bf16),
            pltpu.VMEM((2, 3, LEAVES, M), f32),
            pltpu.VMEM((LEAVES * K, M), f32),
            pltpu.SemaphoreType.DMA((16,)),
            pltpu.SemaphoreType.DMA((16,)),
            pltpu.SemaphoreType.DMA((7,)),
        ],
        compiler_params=pltpu.CompilerParams(
            collective_id=0, has_side_effects=True, vmem_limit_bytes=63 * 1024 * 1024
        ),
        cost_estimate=pl.CostEstimate(flops=10**9, bytes_accessed=10**7, transcendentals=0),
        name="exchange",
    )(blk, blk_src, top, top_idx, coords, charges, basis, transfers)


def kernel_rows(slot, mine, one, two, j, source, kern):
    squares = dot(mine, jnp.concatenate([source[one], source[two]], axis=1))
    kern[slot, :, 2 * M * j : 2 * M * (j + 1)] = lax.rsqrt(squares.astype(bf16))


def charge_rows(slot, one, two, j, pool, gathered, last):
    gathered[slot, 2 * M * j : 2 * M * j + M] = pool[jnp.minimum(one, last)]
    gathered[slot, 2 * M * j + M : 2 * M * (j + 1)] = pool[jnp.minimum(two, last)]


def load_pool(refs, pool, sems, last):
    copies = [
        pltpu.make_async_copy(ref, pool.at[pl.ds(LEAVES * i, LEAVES)], sems.at[i])
        for i, ref in enumerate(refs)
    ]
    for copy in copies:
        copy.start()
    pool[last] = jnp.zeros((M, RHS), bf16)
    return copies


def close_kernel(near, source, target, here, partner, out, pool, kern, gathered, sems):
    step = pl.program_id(0)

    def entries(b):
        leaf = step * GROUP + b
        return [(near[leaf, 2 * j], near[leaf, 2 * j + 1], j) for j in range(HALF // 2)]

    @pl.when(step == 0)
    def _():
        for copy in load_pool((here, partner), pool, sems, 2 * LEAVES):
            copy.wait()

    for b in range(GROUP):
        mine = target[b]
        for one, two, j in entries(b):
            kernel_rows(b, mine, one, two, j, source, kern)
            charge_rows(b, one, two, j, pool, gathered, 2 * LEAVES)
        out[b] = dot(kern[b], gathered[b])


def near_kernel(
    near,
    source,
    target,
    here,
    partner,
    other,
    partial,
    a_high,
    a_low,
    every,
    t_high,
    t_low,
    top_all,
    transfers,
    basis,
    out,
    pool,
    kern,
    gathered,
    base,
    extra,
    sems,
):
    step = pl.program_id(0)

    def entries(b):
        leaf = step * GROUP + b
        return [
            (near[leaf, HALF + 2 * j], near[leaf, HALF + 2 * j + 1], j)
            for j in range(HALF // 2)
        ]

    @pl.when(step == 0)
    def _():
        copies = load_pool((here, partner, other), pool, sems, POOL)
        extra[...] = jnp.zeros_like(extra)
        top_field = (dot(t_high[...], top_all[...]) + dot(t_low[...], top_all[...])).astype(bf16)
        coupled = dot(a_high[...], every[...]) + dot(a_low[...], every[...])
        base[...] = (coupled + dot(transfers[(LEAVES + GROUP) * K :, :], top_field)).astype(bf16)
        for copy in copies:
            copy.wait()

    late = jnp.int32(0)
    for b in range(GROUP):
        late += HALF - near[step * GROUP + b, 2 * HALF]

    @pl.when(late > 0)
    def _():
        def one_leaf(b, c):
            leaf = step * GROUP + b

            def one_entry(e, total):
                g = near[leaf, e]
                squares = dot(target[b], source[g])
                return total + dot(lax.rsqrt(squares.astype(bf16)), pool[g])

            extra[b] = lax.fori_loop(
                near[leaf, 2 * HALF], HALF, one_entry, jnp.zeros((M, RHS), f32)
            )
            return c

        lax.fori_loop(0, GROUP, one_leaf, 0)

    down = transfers[pl.ds(pl.multiple_of((LEAVES + step) * K, K), K), :]
    mid = dot(down, base[...]).astype(bf16)
    down = transfers[pl.ds(pl.multiple_of(step * GROUP * K, GROUP * K), GROUP * K), :]
    fields = dot(down, mid).astype(bf16)
    for b in range(GROUP):
        mine = target[b]
        for one, two, j in entries(b):
            kernel_rows(b, mine, one, two, j, source, kern)
            charge_rows(b, one, two, j, pool, gathered, POOL)
        far = dot_t(basis[b], fields[b * K : (b + 1) * K])
        total = dot(kern[b], gathered[b]) + far + (partial[b] + extra[b])
        out[pl.ds(b * M, M), :] = total.astype(bf16)

    @pl.when(late > 0)
    def _():
        extra[...] = jnp.zeros_like(extra)


def near_scratch(leaves):
    return [
        pltpu.VMEM((leaves, M, RHS), bf16),
        pltpu.VMEM((GROUP, M, M * HALF), bf16),
        pltpu.VMEM((GROUP, M * HALF, RHS), bf16),
    ]


NEAR_PARAMS = dict(
    compiler_params=pltpu.CompilerParams(
        vmem_limit_bytes=63 * 1024 * 1024, dimension_semantics=("arbitrary",)
    ),
    cost_estimate=pl.CostEstimate(
        flops=5 * 10**9, bytes_accessed=10**7, transcendentals=10**7
    ),
)


def close_call(near, source, target, here, partner):
    anywhere = pl.BlockSpec(memory_space=pl.ANY)
    grid_spec = pltpu.PrefetchScalarGridSpec(
        num_scalar_prefetch=1,
        grid=(LEAVES // GROUP,),
        in_specs=[
            vmem(*source.shape),
            pl.BlockSpec((GROUP, M, K), lambda i, _: (i, 0, 0)),
            anywhere,
            anywhere,
        ],
        out_specs=pl.BlockSpec((GROUP, M, RHS), lambda i, _: (i, 0, 0)),
        scratch_shapes=[*near_scratch(2 * LEAVES + 1), pltpu.SemaphoreType.DMA((2,))],
    )
    return pl.pallas_call(
        close_kernel,
        grid_spec=grid_spec,
        out_shape=jax.ShapeDtypeStruct((LEAVES, M, RHS), f32),
        name="close",
        **NEAR_PARAMS,
    )(near, source, target, here, partner)


def near_call(near, source, target, here, partner, other, partial, far, transfers, basis):
    anywhere = pl.BlockSpec(memory_space=pl.ANY)
    grid_spec = pltpu.PrefetchScalarGridSpec(
        num_scalar_prefetch=1,
        grid=(LEAVES // GROUP,),
        in_specs=[
            vmem(*source.shape),
            pl.BlockSpec((GROUP, M, K), lambda i, _: (i, 0, 0)),
            anywhere,
            anywhere,
            anywhere,
            pl.BlockSpec((GROUP, M, RHS), lambda i, _: (i, 0, 0)),
            *[vmem(*v.shape) for v in far],
            vmem(*transfers.shape),
            pl.BlockSpec((GROUP, K, M), lambda i, _: (i, 0, 0)),
        ],
        out_specs=pl.BlockSpec((GROUP * M, RHS), lambda i, _: (i, 0)),
        scratch_shapes=[
            *near_scratch(POOL + 1),
            pltpu.VMEM((K, RHS), bf16),
            pltpu.VMEM((GROUP, M, RHS), f32),
            pltpu.SemaphoreType.DMA((3,)),
        ],
    )
    return pl.pallas_call(
        near_kernel,
        grid_spec=grid_spec,
        out_shape=jax.ShapeDtypeStruct((LEAVES * M, RHS), bf16),
        name="near",
        **NEAR_PARAMS,
    )(near, source, target, here, partner, other, partial, *far, transfers, basis)


def near_lists(near_leaves, core):
    block, inside = near_leaves // LEAVES, near_leaves % LEAVES
    moved = jnp.where(block == 1, 0, jnp.where((block == 0) == (core == 0), 2, 1))
    place = moved * LEAVES + inside
    away = place >= 2 * LEAVES
    column = jnp.arange(NNEAR)
    key = jnp.where(away, NNEAR, 0) + column
    rank = jnp.sum(key[:, None, :] < key[:, :, None], axis=2)
    ordered = jnp.sum(
        jnp.where(rank[:, :, None] == jnp.arange(2 * HALF), place[:, :, None] + 1, 0), axis=1
    )
    ordered = jnp.where(ordered == 0, POOL, ordered - 1)
    ready = jnp.minimum(NNEAR - jnp.sum(away, axis=1, keepdims=True), HALF)
    return jnp.concatenate([ordered, ready], axis=1)


def high_low(v):
    high = v.astype(bf16)
    return high, (v - high.astype(f32)).astype(bf16)


def per_device(
    coords,
    charges,
    near_leaves,
    leaf_basis,
    leaf_transfer,
    mid_transfer,
    base_transfer,
    base_coupling,
    base_target,
    base_source,
    top_coupling,
    top_target,
    top_source,
):
    me = lax.axis_index(AXIS)
    rows = charges.reshape(LEAVES, M, RHS)
    targets = base_target[:, 0]
    count = targets.shape[0]
    earlier = jnp.arange(count)[:, None] > jnp.arange(count)[None, :]
    rank = jnp.sum((targets[:, None] == targets[None, :]) & earlier, axis=1)
    slots = jnp.arange(2 * N)
    places = (targets % GROUP) * 16 + targets // GROUP
    chosen = (slots[:, None] == (2 * places + rank)[None, :]).astype(bf16)
    blk = dot(chosen, base_coupling).astype(bf16).reshape(GROUP, 16, 16, 128)
    order = (base_source % 2) * 64 + (base_source // 8) * 4 + (base_source // 2) % 4
    slot_source = jnp.sum(chosen.astype(jnp.int32) * (order + 1)[None, :], axis=1) - 1
    blk_src = jnp.pad(slot_source.reshape(GROUP, 16, 1, 2), ((0, 0),) * 3 + ((0, 126),))
    lane = jnp.arange(N)
    top_idx = jnp.tile(top_target * 16 + top_source, 16)
    top_idx = jnp.where(lane // 8 == me // GROUP, top_idx, 0).reshape(1, N)

    basis = leaf_basis.reshape(LEAVES, K, M)
    transfers = jnp.concatenate([leaf_transfer, mid_transfer, base_transfer], axis=0)
    transfers = transfers.reshape((LEAVES + GROUP + 1) * K, K)
    r_blk, r_src, every, top_all, t, source, target, partner = exchange_call(
        blk, blk_src, top_coupling, top_idx, coords, rows, basis, transfers
    )
    outward = [(i, i + 1) for i in range(1, N - 1, 2)] + [(i, i - 1) for i in range(2, N, 2)]
    sent, partner, listed = lax.optimization_barrier((rows, partner, near_leaves))
    other = lax.ppermute(sent, AXIS, outward)
    near = near_lists(listed, me % 2)
    partial = close_call(near, source, target, rows, partner)
    by_source = (lane[:, None] == r_src[:, :, 0, :2].reshape(1, 2 * N)).astype(bf16)
    a = dot(by_source, r_blk.reshape(2 * N, K * K))
    a = a.reshape(N, K, K).transpose(1, 0, 2).reshape(K, N * K)
    t = t.reshape(16, K, K).transpose(1, 0, 2).reshape(K, 16 * K)
    far = (
        *high_low(a),
        every.reshape(N * K, RHS),
        *high_low(t),
        top_all.reshape(16 * K, RHS),
    )
    return near_call(
        near, source, target, rows, partner, other, partial, far, transfers, basis
    )


def solution(mesh):
    lead = P(AXIS, None)
    in_specs = (
        P(None, AXIS),
        lead,
        lead,
        lead,
        lead,
        lead,
        lead,
        lead,
        lead,
        P(AXIS),
        lead,
        P(AXIS),
        P(AXIS),
    )
    return jax.shard_map(
        per_device, mesh=mesh, in_specs=in_specs, out_specs=lead, check_vma=False
    )
```

```python
import functools
import math

import jax
import jax.numpy as jnp
from jax import lax
from jax.experimental import pallas as pl
from jax.experimental.pallas import tpu as pltpu
from jax.sharding import PartitionSpec as P

K = 32
RHS = 128
M = 128
N = 128
LEAVES = 64
POOL = 3 * LEAVES
NNEAR = 27
HALF = (NNEAR + 1) // 2
GROUP = 8
WIDE = 16
DELTA_SQ = 0.0025
AXIS = "leaf"
MESH = pl.DeviceIdType.MESH
bf16 = jnp.bfloat16
f32 = jnp.float32


def dot(a, b):
    return jnp.dot(a, b, preferred_element_type=f32)


def dot_t(a, b):
    return lax.dot_general(a, b, (((0,), (0,)), ((), ())), preferred_element_type=f32)


def vmem(*shape):
    return pl.BlockSpec(shape, lambda *_: (0,) * len(shape))


def split3(v):
    high = v.astype(bf16).astype(f32)
    rest = v - high
    mid = rest.astype(bf16).astype(f32)
    return high, mid, rest - mid


def features(scale, points, target):
    centred = [(p - 0.5) * scale for p in points]
    norm = centred[0] * centred[0] + centred[1] * centred[1] + centred[2] * centred[2]
    one = jnp.ones_like(norm)
    rows = []
    for c in centred:
        h, m, l = split3(c)
        if target:
            h, m, l = -2.0 * h, -2.0 * m, -2.0 * l
            rows += [h, h, m, m, h, l]
        else:
            rows += [h, m, h, m, l, h]
    if target:
        rows += [*split3(norm + scale * scale * DELTA_SQ), one, one, one]
    else:
        rows += [one, one, one, *split3(norm)]
    return rows


def exchange_kernel(
    scale,
    blk,
    blk_src,
    top,
    top_idx,
    coords,
    charges,
    basis,
    transfers,
    r_blk,
    r_src,
    every,
    top_all,
    top_sum,
    source,
    target,
    partner,
    held,
    points,
    half,
    half_src,
    tops,
    r_top,
    r_idx,
    lifted,
    coeffs,
    mine,
    mids,
    part,
    others,
    lines,
    send,
    recv,
    local,
):
    me = lax.axis_index(AXIS)
    plane, place = me // GROUP, me % GROUP
    core, y = place % 2, place // 2
    fetch = pltpu.make_async_copy(charges, held, local.at[0])
    fetch.start()
    barrier = pltpu.get_barrier_semaphore()

    across_chip, next_chip = me + 1 - 2 * core, lax.rem(me - 1 + 2 * core + N, N)
    peers = [plane * GROUP + lax.rem(place + o, GROUP) for o in range(1, GROUP)]
    planes = [lax.rem(plane + o, 16) for o in range(1, 16)]
    greeted = [*peers, *[p * GROUP + place for p in planes], next_chip]
    for to in greeted:
        pl.semaphore_signal(barrier, inc=1, device_id=(to,), device_id_type=MESH)
    for i in range(3):
        for l in range(LEAVES):
            points[i, l : l + 1, :] = coords[i : i + 1, l * M : (l + 1) * M]

    lines[...] = jnp.zeros_like(lines)

    fetch.wait()

    def one_mid(m, c):
        rows = []
        for b in range(GROUP):
            rows.append(dot(basis[m * GROUP + b], held[m * GROUP + b]).astype(bf16))
        first = pl.multiple_of(m * GROUP * K, GROUP * K)
        rows = dot_t(transfers[pl.ds(first, GROUP * K), :], jnp.concatenate(rows, axis=0))
        mids[pl.ds(pl.multiple_of(m * K, K), K), :] = rows.astype(bf16)
        return c

    lax.fori_loop(0, GROUP, one_mid, 0, unroll=2)
    base = dot_t(transfers[LEAVES * K : LEAVES * K + GROUP * K, :], mids[...]).astype(bf16)
    coeffs[0] = base
    coeffs[1] = dot_t(transfers[LEAVES * K + GROUP * K :, :], base).astype(bf16)
    pl.semaphore_wait(barrier, len(greeted))

    def remote(src, dst, k, to):
        return pltpu.make_async_remote_copy(
            src_ref=src,
            dst_ref=dst,
            send_sem=send.at[k],
            recv_sem=recv.at[k],
            device_id=(to,),
            device_id_type=MESH,
        )

    def finish(ref, k):
        whole = remote(ref, ref, k, me)
        whole.wait_send()
        whole.wait_recv()

    for o in range(1, 4):
        to = plane * GROUP + lax.rem(y + o, 4) * 2 + core
        remote(coeffs.at[0], every.at[core, plane, y], 6, to).start()
    for to in peers:
        remote(coeffs.at[1], lifted.at[place], 7, to).start()
    for to in peers:
        remote(blk.at[to % GROUP], half.at[place], 4, to).start()
        remote(blk_src.at[to % GROUP], half_src.at[place], 5, to).start()
    to_partner = remote(points, others.at[0], 0, across_chip)
    to_other = remote(points, others.at[1], 1, next_chip)
    to_partner.start()
    to_other.start()
    swap = remote(held, partner, 12, across_chip)
    swap.start()
    for p in planes:
        to = p * GROUP + place
        remote(top, r_top.at[plane], 2, to).start()
        remote(top_idx, r_idx.at[plane], 3, to).start()
    own = [
        pltpu.make_async_copy(blk.at[place], half.at[place], local.at[1]),
        pltpu.make_async_copy(blk_src.at[place], half_src.at[place], local.at[2]),
        pltpu.make_async_copy(top, r_top.at[plane], local.at[3]),
        pltpu.make_async_copy(top_idx, r_idx.at[plane], local.at[4]),
        pltpu.make_async_copy(coeffs.at[0], every.at[core, plane, y], local.at[5]),
        pltpu.make_async_copy(coeffs.at[1], lifted.at[place], local.at[6]),
    ]
    for copy in own:
        copy.start()

    def side(rows, put, count):
        for r, row in enumerate(rows):
            lines[pl.ds(r, LEAVES, stride=K), :] = row
        lax.fori_loop(0, count, put, 0, unroll=4)

    def line(l):
        return lines[pl.ds(pl.multiple_of(l * K, K), K), :]

    def put_target(l, c):
        target[l] = line(l).T.astype(bf16)
        return c

    def put_source(block):
        def put(l, c):
            source[block * LEAVES + l] = line(l).astype(bf16)
            return c

        return put

    here = [points[i] for i in range(3)]
    side(features(scale, here, True), put_target, LEAVES)
    for copy in own:
        copy.wait()
    finish(lifted.at[pl.ds(0, 3)], 6)
    for p in planes:
        to = p * GROUP + place
        remote(every.at[core, plane], every.at[core, plane], 8, to).start()
    finish(lifted.at[pl.ds(0, GROUP - 1)], 7)
    mine[...] = jnp.sum(lifted[...].astype(f32), axis=0).astype(bf16)
    for p in planes:
        remote(mine, top_all.at[plane], 9, p * GROUP + place).start()
    own_top = pltpu.make_async_copy(mine, top_all.at[plane], local.at[0])
    own_top.start()
    side(features(scale, here, False), put_source(0), LEAVES)
    own_top.wait()

    finish(half.at[pl.ds(0, GROUP - 1)], 4)
    finish(half_src.at[pl.ds(0, GROUP - 1)], 5)
    for p in planes:
        to = p * GROUP + place
        remote(half.at[:, p], r_blk.at[plane], 14, to).start()
        remote(half_src.at[:, p], r_src.at[plane], 15, to).start()
    own = [
        pltpu.make_async_copy(half.at[:, plane], r_blk.at[plane], local.at[2]),
        pltpu.make_async_copy(half_src.at[:, plane], r_src.at[plane], local.at[3]),
    ]
    for copy in own:
        copy.start()
    to_partner.wait()
    to_other.wait()
    spare = source[0]
    for l in range(8):
        source[POOL + l] = spare
    for i in range(2):
        side(features(scale, [others[i, j] for j in range(3)], False), put_source(i + 1), LEAVES)

    finish(r_top.at[pl.ds(0, 15)], 2)
    finish(r_idx.at[pl.ds(0, 15)], 3)
    named = jnp.sum(r_idx[...], axis=0)
    wanted = plane * 16 + lax.broadcasted_iota(jnp.int32, (16, N), 0)
    chosen = jnp.where(wanted == named, 1.0, 0.0).astype(bf16)
    part[...] = dot(chosen, r_top[...].reshape(N, K * K)).astype(bf16)
    for to in peers:
        remote(part, tops.at[place], 10, to).start()
    own_part = pltpu.make_async_copy(part, tops.at[place], local.at[0])
    own_part.start()

    finish(every.at[0, pl.ds(0, 15)], 8)
    across = remote(every.at[core], every.at[core], 11, across_chip)
    across.start()
    own_part.wait()
    finish(tops.at[pl.ds(0, GROUP - 1)], 10)
    top_sum[...] = jnp.sum(tops[...].astype(f32), axis=0)
    finish(top_all.at[pl.ds(0, 15)], 9)
    across.wait()
    for copy in own:
        copy.wait()
    finish(r_blk.at[pl.ds(0, 15)], 14)
    finish(r_src.at[pl.ds(0, 15)], 15)
    swap.wait()


def exchange_call(blk, blk_src, top, top_idx, coords, charges, basis, transfers):
    inside = pl.BlockSpec(memory_space=pltpu.VMEM)
    anywhere = pl.BlockSpec(memory_space=pl.ANY)
    shape = jax.ShapeDtypeStruct
    return pl.pallas_call(
        functools.partial(exchange_kernel, math.sqrt(NNEAR * M)),
        out_shape=(
            shape((16, GROUP, *blk.shape[2:]), bf16),
            shape((16, GROUP, *blk_src.shape[2:]), jnp.int32),
            shape((2, 16, 4, K, RHS), bf16),
            shape((16, K, RHS), bf16),
            shape((16, K * K), f32),
            shape((POOL + 8, K, M), bf16),
            shape((LEAVES, M, K), bf16),
            shape((LEAVES, M, RHS), bf16),
        ),
        in_specs=[
            *[inside] * 5,
            anywhere,
            inside,
            inside,
        ],
        out_specs=(*[inside] * 7, anywhere),
        scratch_shapes=[
            pltpu.VMEM((LEAVES, M, RHS), bf16),
            pltpu.VMEM((3, LEAVES, M), f32),
            pltpu.VMEM(blk.shape, bf16),
            pltpu.VMEM(blk_src.shape, jnp.int32),
            pltpu.VMEM((GROUP, 16, K * K), bf16),
            pltpu.VMEM((16, 8, K * K), bf16),
            pltpu.VMEM((16, 1, N), jnp.int32),
            pltpu.VMEM((GROUP, K, RHS), bf16),
            pltpu.VMEM((2, K, RHS), bf16),
            pltpu.VMEM((K, RHS), bf16),
            pltpu.VMEM((GROUP * K, RHS), bf16),
            pltpu.VMEM((16, K * K), bf16),
            pltpu.VMEM((2, 3, LEAVES, M), f32),
            pltpu.VMEM((LEAVES * K, M), f32),
            pltpu.SemaphoreType.DMA((16,)),
            pltpu.SemaphoreType.DMA((16,)),
            pltpu.SemaphoreType.DMA((7,)),
        ],
        compiler_params=pltpu.CompilerParams(
            collective_id=0, has_side_effects=True, vmem_limit_bytes=63 * 1024 * 1024
        ),
        cost_estimate=pl.CostEstimate(flops=10**9, bytes_accessed=10**7, transcendentals=0),
        name="exchange",
    )(blk, blk_src, top, top_idx, coords, charges, basis, transfers)


def kernel_rows(slot, mine, one, two, j, source, kern):
    squares = dot(mine, jnp.concatenate([source[one], source[two]], axis=1))
    kern[slot, :, 2 * M * j : 2 * M * (j + 1)] = lax.rsqrt(squares.astype(bf16))


def charge_rows(slot, one, two, j, pool, gathered, last):
    gathered[slot, 2 * M * j : 2 * M * j + M] = pool[jnp.minimum(one, last)]
    gathered[slot, 2 * M * j + M : 2 * M * (j + 1)] = pool[jnp.minimum(two, last)]


def load_pool(refs, pool, sems, last):
    copies = [
        pltpu.make_async_copy(ref, pool.at[pl.ds(LEAVES * i, LEAVES)], sems.at[i])
        for i, ref in enumerate(refs)
    ]
    for copy in copies:
        copy.start()
    pool[last] = jnp.zeros((M, RHS), bf16)
    return copies


def close_kernel(near, source, target, here, partner, out, pool, kern, gathered, sems):
    step = pl.program_id(0)

    def entries(b):
        leaf = step * WIDE + b
        return [(near[leaf, 2 * j], near[leaf, 2 * j + 1], j) for j in range(HALF // 2)]

    @pl.when(step == 0)
    def _():
        for copy in load_pool((here, partner), pool, sems, 2 * LEAVES):
            copy.wait()

    for b in range(WIDE):
        mine = target[b]
        for one, two, j in entries(b):
            kernel_rows(b, mine, one, two, j, source, kern)
            charge_rows(b, one, two, j, pool, gathered, 2 * LEAVES)
        out[b] = dot(kern[b], gathered[b])


def near_kernel(
    near,
    source,
    target,
    here,
    partner,
    other,
    partial,
    a_high,
    a_low,
    every,
    t_high,
    t_low,
    top_all,
    transfers,
    basis,
    out,
    pool,
    kern,
    gathered,
    base,
    extra,
    sems,
):
    step = pl.program_id(0)

    def entries(b):
        leaf = step * GROUP + b
        return [
            (near[leaf, HALF + 2 * j], near[leaf, HALF + 2 * j + 1], j)
            for j in range(HALF // 2)
        ]

    @pl.when(step == 0)
    def _():
        copies = load_pool((here, partner, other), pool, sems, POOL)
        extra[...] = jnp.zeros_like(extra)
        top_field = (dot(t_high[...], top_all[...]) + dot(t_low[...], top_all[...])).astype(bf16)
        coupled = dot(a_high[...], every[...]) + dot(a_low[...], every[...])
        base[...] = (coupled + dot(transfers[(LEAVES + GROUP) * K :, :], top_field)).astype(bf16)
        for copy in copies:
            copy.wait()

    late = jnp.int32(0)
    for b in range(GROUP):
        late += HALF - near[step * GROUP + b, 2 * HALF]

    @pl.when(late > 0)
    def _():
        def one_leaf(b, c):
            leaf = step * GROUP + b

            def one_entry(e, total):
                g = near[leaf, e]
                squares = dot(target[b], source[g])
                return total + dot(lax.rsqrt(squares.astype(bf16)), pool[g])

            extra[b] = lax.fori_loop(
                near[leaf, 2 * HALF], HALF, one_entry, jnp.zeros((M, RHS), f32)
            )
            return c

        lax.fori_loop(0, GROUP, one_leaf, 0)

    down = transfers[pl.ds(pl.multiple_of((LEAVES + step) * K, K), K), :]
    mid = dot(down, base[...]).astype(bf16)
    down = transfers[pl.ds(pl.multiple_of(step * GROUP * K, GROUP * K), GROUP * K), :]
    fields = dot(down, mid).astype(bf16)
    for b in range(GROUP):
        mine = target[b]
        for one, two, j in entries(b):
            kernel_rows(b, mine, one, two, j, source, kern)
            charge_rows(b, one, two, j, pool, gathered, POOL)
        far = dot_t(basis[b], fields[b * K : (b + 1) * K])
        total = dot(kern[b], gathered[b]) + far + (partial[b] + extra[b])
        out[pl.ds(b * M, M), :] = total.astype(bf16)

    @pl.when(late > 0)
    def _():
        extra[...] = jnp.zeros_like(extra)


def near_scratch(leaves, group):
    return [
        pltpu.VMEM((leaves, M, RHS), bf16),
        pltpu.VMEM((group, M, M * HALF), bf16),
        pltpu.VMEM((group, M * HALF, RHS), bf16),
    ]


NEAR_PARAMS = dict(
    compiler_params=pltpu.CompilerParams(
        vmem_limit_bytes=63 * 1024 * 1024, dimension_semantics=("arbitrary",)
    ),
    cost_estimate=pl.CostEstimate(
        flops=5 * 10**9, bytes_accessed=10**7, transcendentals=10**7
    ),
)


def close_call(near, source, target, here, partner):
    anywhere = pl.BlockSpec(memory_space=pl.ANY)
    grid_spec = pltpu.PrefetchScalarGridSpec(
        num_scalar_prefetch=1,
        grid=(LEAVES // WIDE,),
        in_specs=[
            vmem(*source.shape),
            pl.BlockSpec((WIDE, M, K), lambda i, _: (i, 0, 0)),
            anywhere,
            anywhere,
        ],
        out_specs=pl.BlockSpec((WIDE, M, RHS), lambda i, _: (i, 0, 0)),
        scratch_shapes=[*near_scratch(2 * LEAVES + 1, WIDE), pltpu.SemaphoreType.DMA((2,))],
    )
    return pl.pallas_call(
        close_kernel,
        grid_spec=grid_spec,
        out_shape=jax.ShapeDtypeStruct((LEAVES, M, RHS), f32),
        name="close",
        **NEAR_PARAMS,
    )(near, source, target, here, partner)


def near_call(near, source, target, here, partner, other, partial, far, transfers, basis):
    anywhere = pl.BlockSpec(memory_space=pl.ANY)
    grid_spec = pltpu.PrefetchScalarGridSpec(
        num_scalar_prefetch=1,
        grid=(LEAVES // GROUP,),
        in_specs=[
            vmem(*source.shape),
            pl.BlockSpec((GROUP, M, K), lambda i, _: (i, 0, 0)),
            anywhere,
            anywhere,
            anywhere,
            pl.BlockSpec((GROUP, M, RHS), lambda i, _: (i, 0, 0)),
            *[vmem(*v.shape) for v in far],
            vmem(*transfers.shape),
            pl.BlockSpec((GROUP, K, M), lambda i, _: (i, 0, 0)),
        ],
        out_specs=pl.BlockSpec((GROUP * M, RHS), lambda i, _: (i, 0)),
        scratch_shapes=[
            *near_scratch(POOL + 1, GROUP),
            pltpu.VMEM((K, RHS), bf16),
            pltpu.VMEM((GROUP, M, RHS), f32),
            pltpu.SemaphoreType.DMA((3,)),
        ],
    )
    return pl.pallas_call(
        near_kernel,
        grid_spec=grid_spec,
        out_shape=jax.ShapeDtypeStruct((LEAVES * M, RHS), bf16),
        name="near",
        **NEAR_PARAMS,
    )(near, source, target, here, partner, other, partial, *far, transfers, basis)


def near_lists(near_leaves, core):
    block, inside = near_leaves // LEAVES, near_leaves % LEAVES
    moved = jnp.where(block == 1, 0, jnp.where((block == 0) == (core == 0), 2, 1))
    place = moved * LEAVES + inside
    away = place >= 2 * LEAVES
    column = jnp.arange(NNEAR)
    key = jnp.where(away, NNEAR, 0) + column
    rank = jnp.sum(key[:, None, :] < key[:, :, None], axis=2)
    ordered = jnp.sum(
        jnp.where(rank[:, :, None] == jnp.arange(2 * HALF), place[:, :, None] + 1, 0), axis=1
    )
    ordered = jnp.where(ordered == 0, POOL, ordered - 1)
    ready = jnp.minimum(NNEAR - jnp.sum(away, axis=1, keepdims=True), HALF)
    return jnp.concatenate([ordered, ready], axis=1)


def high_low(v):
    high = v.astype(bf16)
    return high, (v - high.astype(f32)).astype(bf16)


def per_device(
    coords,
    charges,
    near_leaves,
    leaf_basis,
    leaf_transfer,
    mid_transfer,
    base_transfer,
    base_coupling,
    base_target,
    base_source,
    top_coupling,
    top_target,
    top_source,
):
    me = lax.axis_index(AXIS)
    rows = charges.reshape(LEAVES, M, RHS)
    targets = base_target[:, 0]
    count = targets.shape[0]
    earlier = jnp.arange(count)[:, None] > jnp.arange(count)[None, :]
    rank = jnp.sum((targets[:, None] == targets[None, :]) & earlier, axis=1)
    slots = jnp.arange(2 * N)
    places = (targets % GROUP) * 16 + targets // GROUP
    chosen = (slots[:, None] == (2 * places + rank)[None, :]).astype(bf16)
    blk = dot(chosen, base_coupling).astype(bf16).reshape(GROUP, 16, 16, 128)
    order = (base_source % 2) * 64 + (base_source // 8) * 4 + (base_source // 2) % 4
    slot_source = jnp.sum(chosen.astype(jnp.int32) * (order + 1)[None, :], axis=1) - 1
    blk_src = jnp.pad(slot_source.reshape(GROUP, 16, 1, 2), ((0, 0),) * 3 + ((0, 126),))
    lane = jnp.arange(N)
    top_idx = jnp.tile(top_target * 16 + top_source, 16)
    top_idx = jnp.where(lane // 8 == me // GROUP, top_idx, 0).reshape(1, N)

    basis = leaf_basis.reshape(LEAVES, K, M)
    transfers = jnp.concatenate([leaf_transfer, mid_transfer, base_transfer], axis=0)
    transfers = transfers.reshape((LEAVES + GROUP + 1) * K, K)
    r_blk, r_src, every, top_all, t, source, target, partner = exchange_call(
        blk, blk_src, top_coupling, top_idx, coords, rows, basis, transfers
    )
    outward = [(i, i + 1) for i in range(1, N - 1, 2)] + [(i, i - 1) for i in range(2, N, 2)]
    sent, partner, listed = lax.optimization_barrier((rows, partner, near_leaves))
    other = lax.ppermute(sent, AXIS, outward)
    near = near_lists(listed, me % 2)
    partial = close_call(near, source, target, rows, partner)
    by_source = (lane[:, None] == r_src[:, :, 0, :2].reshape(1, 2 * N)).astype(bf16)
    a = dot(by_source, r_blk.reshape(2 * N, K * K))
    a = a.reshape(N, K, K).transpose(1, 0, 2).reshape(K, N * K)
    t = t.reshape(16, K, K).transpose(1, 0, 2).reshape(K, 16 * K)
    far = (
        *high_low(a),
        every.reshape(N * K, RHS),
        *high_low(t),
        top_all.reshape(16 * K, RHS),
    )
    return near_call(
        near, source, target, rows, partner, other, partial, far, transfers, basis
    )


def solution(mesh):
    lead = P(AXIS, None)
    in_specs = (
        P(None, AXIS),
        lead,
        lead,
        lead,
        lead,
        lead,
        lead,
        lead,
        lead,
        P(AXIS),
        lead,
        P(AXIS),
        P(AXIS),
    )
    return jax.shard_map(
        per_device, mesh=mesh, in_specs=in_specs, out_specs=lead, check_vma=False
    )
```
